32 devices in a mesh: gz: 8 (over z, y), gy: 4 (over x, core).
Axes of the slice: x: 2, y: 2, z: 4, core: 2. Of those that a mesh axis runs over, the one named last changes fastest.
Arguments:
- right_side: float32 [8, 16, 256, 512], P(None, 'gz', 'gy'), may hold values from -8 to 8
- diagonal: float32 [16, 256, 512], P('gz', 'gy'), may hold values from 0.1 to 4
Outputs:
- solution: float32 [8, 16, 256, 512], P(None, 'gz', 'gy')
- hessenberg: float32 [24, 32], replicated
The draws below stay inside these ranges and needn't reach their ends.
All inputs are finite; a program needn't handle non-finite values.
Results may differ from the reference program's by a relative error of at most 0.0003.
Values sent between devices are 32-bit elements; how exact they have to be, the bound alone decides.
A program may use at most 64 MiB of HBM per device.

```python
import math
import jax
import jax.numpy as jnp
from jax import lax

BLK = 8
ITERS = 3
NX = 512
NZ = 16
NY = 256


def level_of(rng, dims, shards, smallest, top_value):
    gain = 1.0
    for axis_at, shards_of in shards:
        draws = jax.random.uniform(jax.random.fold_in(jax.random.fold_in(rng, 6), axis_at), (shards_of,), jnp.float32, smallest / len(shards), top_value / len(shards))
        gain = gain * jnp.repeat(jnp.exp(draws), dims[axis_at] // shards_of).reshape((-1,) + (1,) * (len(dims) - 1 - axis_at))
    return gain


def gaussian(key, shape, deviation, most, split=(), dtype=jnp.bfloat16):
    level = level_of(key, shape, split, -0.22, 0.18) if split else 1.0
    drawn = jax.random.normal(key, shape, jnp.float32) * deviation * level
    return jnp.minimum(jnp.maximum(drawn, -most), most).astype(dtype)


def setup_inputs(seed: int = 0) -> dict:
    streams_of = jax.random.split(jax.random.key(seed), 3)
    return {
        "right_side": gaussian(streams_of[0], (BLK, NZ, NY, NX), 1.0, 8.0, ((1, 8), (2, 4)), jnp.float32),
        "diagonal": jnp.clip(jnp.exp(math.log(4.0) - 3.6888794 * jax.random.uniform(streams_of[1], (NZ, NY, NX), jnp.float32) ** level_of(streams_of[1], (NZ, NY, NX), ((0, 8), (1, 4)), -0.2, 0.2)), 0.1, 4.0),
    }


def apply_op(field, diagonal):
    padded = jnp.pad(field, ((0, 0), (1, 1), (1, 1), (1, 1)))
    beside = padded[:, 2:, 1:-1, 1:-1] + padded[:, :-2, 1:-1, 1:-1]
    beside = beside + padded[:, 1:-1, 2:, 1:-1] + padded[:, 1:-1, :-2, 1:-1]
    beside = beside + padded[:, 1:-1, 1:-1, 2:] + padded[:, 1:-1, 1:-1, :-2]
    return (6.0 + diagonal)[None] * field - beside

def inner(left, right):
    return jnp.dot(left, right.T, precision=lax.Precision.HIGHEST)

def reference(right_side, diagonal):
    shape = right_side.shape
    flat_rhs = right_side.reshape(BLK, -1)
    lower0 = jnp.linalg.cholesky(inner(flat_rhs, flat_rhs))
    basis = [jax.scipy.linalg.solve_triangular(lower0, flat_rhs, lower=True)]
    blocks = []
    for step in range(ITERS):
        work = apply_op(basis[step].reshape(shape), diagonal).reshape(BLK, -1)
        coeff = [inner(work, vec) for vec in basis]
        reduced = work
        for index in range(step + 1):
            reduced = reduced - jnp.dot(coeff[index], basis[index], precision=lax.Precision.HIGHEST)
        lower = jnp.linalg.cholesky(inner(reduced, reduced))
        basis.append(jax.scipy.linalg.solve_triangular(lower, reduced, lower=True))
        row = coeff + [lower] + [jnp.zeros((BLK, BLK), jnp.float32)] * (ITERS - 1 - step)
        blocks.append(jnp.concatenate(row, axis=1))
    hessenberg = jnp.concatenate(blocks, axis=0)
    normal = jnp.dot(hessenberg, hessenberg.T, precision=lax.Precision.HIGHEST)
    factor = jnp.linalg.cholesky(normal)
    target = jnp.dot(hessenberg[:, :BLK], lower0.T, precision=lax.Precision.HIGHEST)
    coeffs = jax.scipy.linalg.cho_solve((factor, True), target)
    stacked = jnp.concatenate(basis[:ITERS], axis=0)
    solution = jnp.dot(coeffs.T, stacked, precision=lax.Precision.HIGHEST)
    return (solution.reshape(shape), hessenberg)
```

```python
import functools

import jax
import jax.numpy as jnp
from jax import lax
from jax.experimental import pallas as pl
from jax.experimental.pallas import tpu as pltpu
from jax.sharding import PartitionSpec as P

ITERS = 3
CENTRE = 7.5
SCALE = 0.25
CHUNKS = 4
EARLY = 2
BACK = {
    (0, 3): ((1, 0), (1, 1)), (1, 0): ((1, 2),), (1, 1): ((1, 3),), (1, 2): ((2, 0),),
    (1, 3): ((2, 1),), (2, 0): ((2, 2),), "reduce": ((2, 3),),
}
MESH = pl.DeviceIdType.MESH
HIGH = lax.Precision.HIGHEST


def SC(name, f):
    with jax.named_scope(name):
        return f()


def nt_dot(left, right):
    return lax.dot_general(
        left, right, (((1,), (1,)), ((), ())), precision=HIGH, preferred_element_type=jnp.float32
    )


def dot(left, right):
    return jnp.dot(left, right, precision=HIGH, preferred_element_type=jnp.float32)


def kernel(
    r_hbm, d_hbm, out_ref, hess_ref,
    r_ref, d_ref, k0, k1, k2, k3, diag, ret1, ret2, held, ys, yh, rows_out, rows_in,
    acc, mine, slots, splat, i_s,
    x_s, x_r, d_s, d_r, z_s, z_r, y_s, y_r, e_s, e_r, b_s, b_r, l_s, l_r, g_s, g_r,
):
    blk, lay, rows, nx = r_ref.shape
    half, group_lay = rows // 2, 2 * lay
    vc = blk // CHUNKS
    n_z, n_y = lax.axis_size("gz"), lax.axis_size("gy")
    gz, gy = lax.axis_index("gz"), lax.axis_index("gy")
    n_dev = n_z * n_y
    me = gz * n_y + gy
    p, group = gz % 2, gz // 2
    h = (p + gy) % 2
    partner = gz + 1 - 2 * p
    hs = pl.multiple_of(h * half, half)
    os = pl.multiple_of((1 - h) * half, half)
    mine_at = p * lay
    theirs_at = (1 - p) * lay
    below, above = group > 0, group < n_z // 2 - 1
    place = 2 * gy + h
    before, after = place > 0, place < 2 * n_y - 1
    prev_dev = (gz + h * (partner - gz), gy - (1 - h))
    next_dev = (gz + (1 - h) * (partner - gz), gy + h)
    basis = (k0, k1, k2, k3)
    edge = (lay - 1) * p

    def remote(src, dst, send, recv, dev):
        return pltpu.make_async_remote_copy(
            src_ref=src, dst_ref=dst, send_sem=send, recv_sem=recv, device_id=dev,
            device_id_type=MESH,
        )

    def device(i):
        return (i // n_y, i % n_y)

    load_r = pltpu.make_async_copy(r_hbm, r_ref, i_s.at[0])
    load_d = pltpu.make_async_copy(d_hbm, d_ref, i_s.at[1])
    load_r.start()
    load_d.start()

    barrier = pltpu.get_barrier_semaphore()

    def greet(off, carry):
        pl.semaphore_signal(
            barrier, inc=1, device_id=device((me + off) % n_dev), device_id_type=MESH
        )
        return carry

    lax.fori_loop(1, n_dev, greet, 0)

    @pl.when(jnp.logical_not(below))
    def _():
        for k in (k0, k1, k2):
            k[:, 0] = jnp.zeros((blk, half, nx), jnp.float32)

    @pl.when(jnp.logical_not(above))
    def _():
        for k in (k0, k1, k2):
            k[:, group_lay + 1] = jnp.zeros((blk, half, nx), jnp.float32)

    @pl.when(jnp.logical_not(before))
    def _():
        yh[:, 0] = jnp.zeros((ITERS,) + yh.shape[2:], jnp.float32)

    @pl.when(jnp.logical_not(after))
    def _():
        yh[:, 1] = jnp.zeros((ITERS,) + yh.shape[2:], jnp.float32)

    load_r.wait()
    for v in range(blk):
        rows_out[v] = jnp.where(
            h == 0, r_ref[v, :, half - 1:half], r_ref[v, :, half:half + 1]
        )
    SC("barrier", lambda: pl.semaphore_wait(barrier, n_dev - 1))

    rows_copy = remote(rows_out, rows_in, e_s, e_r, (partner, gy))
    rows_copy.start()

    def exchange(which, ch):
        layer = edge + which * (1 - 2 * p)
        vs = pl.ds(ch * vc, vc)
        return remote(
            r_ref.at[vs, pl.ds(layer, 1), pl.ds(os, half)],
            k0.at[vs, pl.ds(1 + mine_at + layer, 1)],
            x_s.at[which, ch], x_r.at[which, ch], (partner, gy),
        )

    def z_from_rhs(ch, direction):
        vs = pl.ds(ch * vc, vc)
        if direction == 0:
            dst, dev = k0.at[vs, pl.ds(group_lay + 1, 1)], (gz - 2, gy)
        else:
            dst, dev = k0.at[vs, pl.ds(0, 1)], (gz + 2, gy)
        return remote(
            r_ref.at[vs, pl.ds(edge, 1), pl.ds(hs, half)], dst,
            z_s.at[0, direction, ch], z_r.at[0, direction, ch], dev,
        )

    def z_copy(j, ch, direction):
        vs = pl.ds(ch * vc, vc)
        k = basis[j]
        if direction == 0:
            src, dst, dev = k.at[vs, pl.ds(1, 1)], k.at[vs, pl.ds(group_lay + 1, 1)], (gz - 2, gy)
        else:
            src, dst, dev = k.at[vs, pl.ds(group_lay, 1)], k.at[vs, pl.ds(0, 1)], (gz + 2, gy)
        return remote(src, dst, z_s.at[j, direction, ch], z_r.at[j, direction, ch], dev)

    def y_copy(j, ch, side):
        vs = pl.ds(ch * vc, vc)
        dev = prev_dev if side == 0 else next_dev
        return remote(
            ys.at[j, side, vs], yh.at[j, 1 - side, vs],
            y_s.at[j, side, ch], y_r.at[j, 1 - side, ch], dev,
        )

    def y_wait_recv(j, ch, side):
        vs = pl.ds(ch * vc, vc)
        remote(
            ys.at[j, side, vs], yh.at[j, side, vs], y_s.at[j, side, ch], y_r.at[j, side, ch],
            (partner, gy),
        ).wait_recv()

    def has(j, side):
        if side == 0:
            return before if j else before & (h == 0)
        return after if j else after & (h == 1)

    early = ret1.shape[2]
    late = half - early

    def back_copy(j, ch):
        vs = pl.ds(ch * vc, vc)
        dst = (ret1, ret2)[j - 1]
        return remote(
            basis[j].at[vs, pl.ds(1 + theirs_at, lay), pl.ds(0, early)],
            dst.at[vs], b_s.at[j - 1, ch], b_r.at[j - 1, ch], (partner, gy),
        )

    def late_copy(layer):
        return remote(
            held.at[:, pl.ds(layer, 1)],
            out_ref.at[:, pl.ds(layer, 1), pl.ds(pl.multiple_of(hs + early, 8), late)],
            l_s.at[layer], l_r.at[layer], (partner, gy),
        )

    diag_copy = remote(
        d_ref.at[:, pl.ds(os, half)], diag.at[pl.ds(mine_at, lay)], d_s, d_r, (partner, gy)
    )

    for ch in range(CHUNKS):
        exchange(0, ch).start()

        @pl.when((p == 0) & below)
        def _():
            z_from_rhs(ch, 0).start()

        @pl.when((p == 1) & above)
        def _():
            z_from_rhs(ch, 1).start()

    load_d.wait()
    diag_copy.start()
    for ch in range(CHUNKS):
        exchange(1, ch).start()

    def own(v, carry):
        k0[v, pl.ds(1 + mine_at, lay)] = r_ref[v, :, pl.ds(hs, half)]
        return carry

    lax.fori_loop(0, blk, own, 0)
    diag[pl.ds(mine_at, lay)] = d_ref[:, pl.ds(hs, half)]

    lanes = nx // 128

    def add_up(sums, tiles):
        def run(i, carry):
            layer, at = i // tiles, pl.multiple_of((i % tiles) * 8, 8)
            for lane in range(lanes):
                carry = sums(carry, layer, at, pl.ds(lane * 128, 128))
            return carry
        return run

    def keep_sum(moment, a, b, s):
        line = jnp.sum(s, axis=0, keepdims=True)
        at = (moment * blk + a) * blk + b
        acc[at:at + 1] = line
        if a != b:
            at = (moment * blk + b) * blk + a
            acc[at:at + 1] = line

    zero = jnp.zeros((8, 128), jnp.float32)

    def gram_rhs():
        pairs = [(a, b) for a in range(blk) for b in range(a, blk)]

        def body(sums, layer, at, cols):
            x = [r_ref[v, layer, pl.ds(at, 8), cols] for v in range(blk)]
            return tuple(s + x[a] * x[b] for s, (a, b) in zip(sums, pairs))

        sums = lax.fori_loop(
            0, lay * (rows // 8), add_up(body, rows // 8), (zero,) * len(pairs)
        )
        for s, (a, b) in zip(sums, pairs):
            keep_sum(0, a, b, s)

    def gram(j, ch):
        src, dst = basis[j], basis[j + 1]
        shift = 0 if j == ITERS - 1 else 1
        top = (ch + 1) * vc
        pairs = [(a, b) for b in range(ch * vc, top) for a in range(b + 1)]

        def body(sums, layer, at, cols):
            x = [src[v, 1 + layer, pl.ds(at, 8), cols] for v in range(top)]
            y = [dst[v, shift + layer, pl.ds(at, 8), cols] for v in range(top)]
            first, second = sums[:len(pairs)], sums[len(pairs):]
            first = tuple(s + x[a] * y[b] for s, (a, b) in zip(first, pairs))
            second = tuple(s + y[a] * y[b] for s, (a, b) in zip(second, pairs))
            return first + second

        sums = lax.fori_loop(
            0, group_lay * (half // 8), add_up(body, half // 8), (zero,) * (2 * len(pairs))
        )
        for i, (a, b) in enumerate(pairs):
            keep_sum(2 * j + 1, a, b, sums[i])
            keep_sum(2 * j + 2, a, b, sums[len(pairs) + i])

    acc[7 * blk * blk:] = jnp.zeros((acc.shape[0] - 7 * blk * blk, 128), jnp.float32)
    SC("gram0", gram_rhs)

    def relay(ch):
        remote(
            r_ref.at[pl.ds(0, vc), pl.ds(0, 1), pl.ds(os, half)],
            k0.at[pl.ds(ch * vc, vc), pl.ds(1 + (group_lay - 1) * (1 - p), 1)],
            x_s.at[0, ch], x_r.at[0, ch], (partner, gy),
        ).wait_recv()

        @pl.when((p == 0) & above)
        def _():
            z_copy(0, ch, 1).start()

        @pl.when((p == 1) & below)
        def _():
            z_copy(0, ch, 0).start()

    def stage_rows(j, v, layer, value):
        ys[j, 0, v, layer:layer + 1] = value[:1]
        ys[j, 1, v, layer:layer + 1] = value[half - 1:]

    def start_rows(j, ch):
        for side in range(2):
            @pl.when(has(j, side))
            def _():
                y_copy(j, ch, side).start()

    def arrived(ch):
        remote(
            r_ref.at[pl.ds(0, vc), pl.ds(0, 1), pl.ds(os, half)],
            k0.at[pl.ds(ch * vc, vc), pl.ds(1 + lay - p, 1)],
            x_s.at[1, ch], x_r.at[1, ch], (partner, gy),
        ).wait_recv()

        def run(v, carry):
            for layer in range(group_lay):
                stage_rows(0, v, layer, k0[v, 1 + layer])
            return carry

        lax.fori_loop(ch * vc, (ch + 1) * vc, run, 0)
        start_rows(0, ch)

    for ch in range(CHUNKS):
        SC(f"relay#{ch}", lambda: relay(ch))

    def rows_arrived():
        rows_copy.wait()
        for v in range(blk):
            near = jnp.where(
                h == 0, r_ref[v, :, half:half + 1], r_ref[v, :, half - 1:half]
            ).reshape(lay, nx)
            far = rows_in[v].reshape(lay, nx)
            yh[0, 1 - h, v] = jnp.where(
                p == 0,
                jnp.concatenate([near, far], axis=0),
                jnp.concatenate([far, near], axis=0),
            )
        remote(
            d_ref.at[:, pl.ds(os, half)], diag.at[pl.ds(theirs_at, lay)], d_s, d_r, (partner, gy)
        ).wait_recv()

    SC("rows_diag", rows_arrived)

    row_at = lax.broadcasted_iota(jnp.int32, (half, nx), 0)
    col_at = lax.broadcasted_iota(jnp.int32, (half, nx), 1)

    def apply(j, ch):
        src, dst = basis[j], basis[j + 1]
        shift = 0 if j == ITERS - 1 else 1
        vs = pl.ds(ch * vc, vc)

        def waits():
            @pl.when(below)
            def _():
                remote(
                    src.at[vs, pl.ds(1, 1)], src.at[vs, pl.ds(0, 1)],
                    z_s.at[j, 1, ch], z_r.at[j, 1, ch], (partner, gy),
                ).wait_recv()

            @pl.when(above)
            def _():
                remote(
                    src.at[vs, pl.ds(1, 1)], src.at[vs, pl.ds(group_lay + 1, 1)],
                    z_s.at[j, 0, ch], z_r.at[j, 0, ch], (partner, gy),
                ).wait_recv()

        def row_waits():
            for side in range(2):
                @pl.when(has(j, side))
                def _():
                    y_wait_recv(j, ch, side)

        SC(f"z_wait{j}#{ch}", waits)
        SC(f"y_wait{j}#{ch}", row_waits)

        def run(v, carry):
            for layer in range(group_lay):
                here = src[v, 1 + layer]
                near = src[v, layer] + src[v, 2 + layer]
                up = jnp.where(
                    row_at == 0, yh[j, 0, v, layer:layer + 1], pltpu.roll(here, 1, 0)
                )
                down = jnp.where(
                    row_at == half - 1, yh[j, 1, v, layer:layer + 1],
                    pltpu.roll(here, half - 1, 0),
                )
                left = jnp.where(col_at == 0, 0.0, pltpu.roll(here, 1, 1))
                right = jnp.where(col_at == nx - 1, 0.0, pltpu.roll(here, nx - 1, 1))
                near = near + (up + down) + (left + right)
                centre = (6.0 - CENTRE) + diag[layer]
                value = SCALE * (centre * here - near)
                dst[v, shift + layer] = value
                if j < ITERS - 1:
                    stage_rows(j + 1, v, layer, value)
            return carry

        SC(f"apply{j}#{ch}", lambda: lax.fori_loop(ch * vc, (ch + 1) * vc, run, 0))
        if j < ITERS - 1:
            @pl.when(below)
            def _():
                z_copy(j + 1, ch, 0).start()

            @pl.when(above)
            def _():
                z_copy(j + 1, ch, 1).start()

            start_rows(j + 1, ch)
        for item in BACK.get((j, ch), ()):
            back_copy(*item).start()
        SC(f"gram{j}#{ch}", lambda: gram(j, ch))

    for ch in range(CHUNKS):
        SC(f"arrived#{ch}", lambda: arrived(ch))
        apply(0, ch)
    for j in range(1, ITERS):
        for ch in range(CHUNKS):
            apply(j, ch)

    def reduce():
        count = acc.shape[0]
        sums = nt_dot(jnp.ones((8, 128), jnp.float32), acc[...])
        lane_q = lax.broadcasted_iota(jnp.int32, (8, count), 1)
        row_q = lax.broadcasted_iota(jnp.int32, (8, count), 0)
        q = lax.broadcasted_iota(jnp.int32, (count, 128), 0)
        c = lax.broadcasted_iota(jnp.int32, (count, 128), 1)
        pick = (q // (blk * blk) == c // blk) & (q % blk == c % blk)
        kept = jnp.where((lane_q // blk) % blk == row_q, sums, 0.0)
        local = dot(kept, jnp.where(pick, 1.0, 0.0))
        packed = local[:4] + pltpu.roll(local, 64, 1)[4:]
        mine[...] = packed
        slots[me] = packed

        def send(off, carry):
            to = (me + off) % n_dev
            remote(mine, slots.at[me], g_s.at[to], g_r.at[me], device(to)).start()
            return carry

        lax.fori_loop(1, n_dev, send, 0)
        for item in BACK.get("reduce", ()):
            back_copy(*item).start()

    SC("red_send", reduce)

    def collect():
        def take(off, carry):
            frm = (me + off) % n_dev
            remote(mine, slots.at[frm], g_s.at[frm], g_r.at[frm], device(frm)).wait()
            return carry

        lax.fori_loop(1, n_dev, take, 0)

    SC("red_wait", collect)
    packed = jnp.sum(slots[...], axis=0)

    lane = lax.broadcasted_iota(jnp.int32, (8, 128), 1)
    keep = lambda x, low, high: jnp.where((lane >= low) & (lane < high), x, 0.0)
    left_by = lambda x, n: x if n == 0 else pltpu.roll(x, 128 - n, 1)
    moments = keep(
        jnp.concatenate([packed, pltpu.roll(packed, 64, 1)], axis=0), 0, 64
    )
    def solve():
        order = (ITERS + 1) * blk
        lane32 = lax.broadcasted_iota(jnp.int32, (order, 128), 1)
        row32 = lax.broadcasted_iota(jnp.int32, (order, 128), 0)
        full = jnp.concatenate(
            [keep(left_by(moments, blk * i), 0, order) for i in range(ITERS + 1)], axis=0
        )
        full = full + jnp.where(lane32 == row32 + order, 1.0, 0.0)
        inv = 1.0 / SCALE
        second = (
            (inv * inv) * left_by(moments, 2 * blk)
            + (2.0 * CENTRE * inv) * left_by(moments, blk)
            + (CENTRE * CENTRE) * moments
        )
        target = inv * left_by(moments, blk) + CENTRE * moments
        small = ITERS * blk
        normal = jnp.concatenate(
            [
                keep(left_by(second, blk * i), 0, small)
                + keep(pltpu.roll(target, small - blk * i, 1) if i < ITERS else target, small, order)
                for i in range(ITERS)
            ],
            axis=0,
        )
        rows_small = lax.broadcasted_iota(jnp.int32, (small, 1), 0)
        rows_full = lax.broadcasted_iota(jnp.int32, (order, 1), 0)
        for k in range(order):
            if k < small:
                row = normal[k:k + 1] / normal[k:k + 1, k:k + 1]
                column = jnp.where(rows_small == k, 0.0, normal[:, k:k + 1])
                normal = jnp.where(rows_small == k, row, normal - column * row)
            row = full[k:k + 1] / full[k:k + 1, k:k + 1]
            column = jnp.where(rows_full <= k, 0.0, full[:, k:k + 1])
            full = full - column * row
        pivots = jnp.sum(jnp.where(lane32 == row32, full, 0.0), axis=1, keepdims=True)
        full = full / jnp.sqrt(pivots)
        upper = jnp.where((lane32 < order) & (lane32 >= row32), full, 0.0)
        lower_inv = left_by(full, order)
        lower_inv = jnp.where(lane32 < small, lower_inv, 0.0)[:small]
        hess = inv * nt_dot(pltpu.roll(lower_inv, blk, 1), upper)
        eye = lax.broadcasted_iota(jnp.int32, (small, order), 0) == lax.broadcasted_iota(
            jnp.int32, (small, order), 1
        )
        row_b = lax.broadcasted_iota(jnp.int32, (small, order), 0) // blk
        col_b = lax.broadcasted_iota(jnp.int32, (small, order), 1) // blk
        hess = hess + jnp.where(eye, CENTRE, 0.0)
        hess_ref[...] = jnp.where(col_b <= row_b + 1, hess, 0.0)
        return normal

    normal = SC("solve", solve)
    small = ITERS * blk

    def spread():
        for k in range(small):
            for u in range(blk):
                splat[k * blk + u] = jnp.broadcast_to(
                    normal[k:k + 1, small + u:small + u + 1], (8, 128)
                )

    SC("splat", spread)

    def combine(dst, layers, row_start, height, sources):
        tiles = height // 8

        def run(i, carry):
            layer, t = layers[0] + i // tiles, i % tiles
            at = pl.multiple_of(row_start + t * 8, 8)
            for lane_at in range(lanes):
                cols = pl.ds(lane_at * 128, 128)
                vals = []
                for ref, l_at, base in sources:
                    first_row = pl.multiple_of(base + t * 8, 8)
                    vals += [ref[v, l_at + layer, pl.ds(first_row, 8), cols] for v in range(blk)]
                for u in range(blk):
                    total = splat[u] * vals[0]
                    for k in range(1, small):
                        total = total + splat[k * blk + u] * vals[k]
                    dst[u, layer, pl.ds(at, 8), cols] = total
            return carry

        lax.fori_loop(0, (layers[1] - layers[0]) * tiles, run, 0)

    def send_late():
        for layer in range(lay):
            combine(held, (layer, layer + 1), 0, late, [(k, 1 + theirs_at, early) for k in basis[:ITERS]])
            late_copy(layer).start()

    SC("comb_late", send_late)
    SC("comb_own", lambda: combine(
        out_ref, (0, lay), hs, half, ((r_ref, 0, hs), (k1, 1 + mine_at, 0), (k2, 1 + mine_at, 0))
    ))

    def back_wait():
        for j in (1, 2):
            for ch in range(CHUNKS):
                back_copy(j, ch).wait()

    SC("back_wait", back_wait)
    SC("comb_other", lambda: combine(
        out_ref, (0, lay), os, early, ((r_ref, 0, os), (ret1, 0, 0), (ret2, 0, 0))
    ))

    def late_wait():
        for layer in range(lay):
            late_copy(layer).wait_send()
            remote(
                held.at[:, pl.ds(layer, 1)],
                out_ref.at[:, pl.ds(layer, 1), pl.ds(pl.multiple_of(os + early, 8), late)],
                l_s.at[layer], l_r.at[layer], (partner, gy),
            ).wait_recv()

    SC("late_wait", late_wait)

    for ch in range(CHUNKS):
        for which in (0, 1):
            exchange(which, ch).wait_send()

        @pl.when(below)
        def _():
            z_copy(0, ch, 0).wait_send()

        @pl.when(above)
        def _():
            z_copy(0, ch, 1).wait_send()

        for j in range(1, ITERS):
            @pl.when(below)
            def _():
                z_copy(j, ch, 0).wait_send()

            @pl.when(above)
            def _():
                z_copy(j, ch, 1).wait_send()

        for j in range(ITERS):
            for side in range(2):
                @pl.when(has(j, side))
                def _():
                    y_copy(j, ch, side).wait_send()

    diag_copy.wait_send()


def body(right_side, diagonal):
    blk, lay, rows, nx = right_side.shape
    half, group_lay = rows // 2, 2 * lay
    early = half * EARLY // 32 * 8
    n_z, n_y = lax.axis_size("gz"), lax.axis_size("gy")
    vmem = lambda *shape: pltpu.VMEM(shape, jnp.float32)
    dma = lambda *shape: pltpu.SemaphoreType.DMA(shape)
    small, order = ITERS * blk, (ITERS + 1) * blk
    in_hbm = lambda x: pltpu.with_memory_space_constraint(x, pltpu.HBM)
    return pl.pallas_call(
        kernel,
        out_shape=(vmem(*right_side.shape), vmem(small, order)),
        in_specs=[pl.BlockSpec(memory_space=pltpu.HBM)] * 2,
        out_specs=(pl.BlockSpec(memory_space=pltpu.VMEM),) * 2,
        scratch_shapes=[
            vmem(*right_side.shape),
            vmem(*diagonal.shape),
            vmem(blk, group_lay + 2, half, nx),
            vmem(blk, group_lay + 2, half, nx),
            vmem(blk, group_lay + 2, half, nx),
            vmem(blk, group_lay, half, nx),
            vmem(group_lay, half, nx),
            vmem(blk, lay, early, nx),
            vmem(blk, lay, early, nx),
            vmem(blk, lay, half - early, nx),
            vmem(ITERS, 2, blk, group_lay, nx),
            vmem(ITERS, 2, blk, group_lay, nx),
            vmem(blk, lay, 1, nx),
            vmem(blk, lay, 1, nx),
            vmem(8 * blk * blk, 128),
            vmem(4, 128),
            vmem(n_z * n_y, 4, 128),
            vmem(small * blk, 8, 128),
            dma(2),
            dma(2, CHUNKS), dma(2, CHUNKS),
            pltpu.SemaphoreType.DMA, pltpu.SemaphoreType.DMA,
            dma(ITERS, 2, CHUNKS), dma(ITERS, 2, CHUNKS),
            dma(ITERS, 2, CHUNKS), dma(ITERS, 2, CHUNKS),
            pltpu.SemaphoreType.DMA, pltpu.SemaphoreType.DMA,
            dma(2, CHUNKS), dma(2, CHUNKS), dma(lay), dma(lay),
            dma(n_z * n_y), dma(n_z * n_y),
        ],
        compiler_params=pltpu.CompilerParams(
            collective_id=0, has_side_effects=True, vmem_limit_bytes=40 * 1024 * 1024
        ),
        name="gmres",
    )(in_hbm(right_side), in_hbm(diagonal))


def solution(mesh):
    in_specs = (P(None, "gz", "gy", None), P("gz", "gy", None))
    out_specs = (P(None, "gz", "gy", None), P())
    return jax.shard_map(body, mesh=mesh, in_specs=in_specs, out_specs=out_specs, check_vma=False)
```

```python
import functools

import jax
import jax.numpy as jnp
from jax import lax
from jax.experimental import pallas as pl
from jax.experimental.pallas import tpu as pltpu
from jax.sharding import PartitionSpec as P

ITERS = 3
CENTRE = 7.5
SCALE = 0.25
CHUNKS = 4
EARLY = (3, 2)
BACK = {
    (0, 1): ((1, 0, 0),), (0, 2): ((1, 0, 1), (1, 1, 0)), (0, 3): ((1, 1, 1), (1, 2, 0)),
    (1, 0): ((1, 2, 1),), (1, 2): ((1, 3, 0),), (1, 3): ((1, 3, 1),),
    (2, 0): ((2, 0, 0), (2, 0, 1)), (2, 1): ((2, 1, 0),),
    "reduce": ((2, 1, 1), (2, 2, 0), (2, 2, 1), (2, 3, 0), (2, 3, 1)),
}
MESH = pl.DeviceIdType.MESH
HIGH = lax.Precision.HIGHEST


def SC(name, f):
    with jax.named_scope(name):
        return f()


def nt_dot(left, right):
    return lax.dot_general(
        left, right, (((1,), (1,)), ((), ())), precision=HIGH, preferred_element_type=jnp.float32
    )


def dot(left, right):
    return jnp.dot(left, right, precision=HIGH, preferred_element_type=jnp.float32)


def kernel(
    r_hbm, d_hbm, out_ref, hess_ref,
    r_ref, d_ref, k0, k1, k2, k3, diag, ret, held, ys, yh, rows_out, rows_in,
    acc, mine, slots, splat, i_s, met,
    x_s, x_r, d_s, d_r, z_s, z_r, y_s, y_r, e_s, e_r, b_s, b_r, l_s, l_r, g_s, g_r,
):
    blk, lay, rows, nx = r_ref.shape
    half, group_lay = rows // 2, 2 * lay
    vc = blk // CHUNKS
    n_z, n_y = lax.axis_size("gz"), lax.axis_size("gy")
    gz, gy = lax.axis_index("gz"), lax.axis_index("gy")
    n_dev = n_z * n_y
    me = gz * n_y + gy
    p, group = gz % 2, gz // 2
    h = (p + gy) % 2
    partner = gz + 1 - 2 * p
    hs = pl.multiple_of(h * half, half)
    os = pl.multiple_of((1 - h) * half, half)
    mine_at = p * lay
    theirs_at = (1 - p) * lay
    below, above = group > 0, group < n_z // 2 - 1
    place = 2 * gy + h
    before, after = place > 0, place < 2 * n_y - 1
    prev_dev = (gz + h * (partner - gz), gy - (1 - h))
    next_dev = (gz + (1 - h) * (partner - gz), gy + h)
    basis = (k0, k1, k2, k3)
    edge = (lay - 1) * p

    def remote(src, dst, send, recv, dev):
        return pltpu.make_async_remote_copy(
            src_ref=src, dst_ref=dst, send_sem=send, recv_sem=recv, device_id=dev,
            device_id_type=MESH,
        )

    def device(i):
        return (i // n_y, i % n_y)

    def load_r(ch):
        vs = pl.ds(ch * vc, vc)
        return pltpu.make_async_copy(r_hbm.at[vs], r_ref.at[vs], i_s.at[ch])

    load_d = pltpu.make_async_copy(d_hbm, d_ref, i_s.at[CHUNKS])
    for ch in range(CHUNKS):
        load_r(ch).start()
    load_d.start()

    def signal(semaphore, dev):
        pl.semaphore_signal(semaphore, inc=1, device_id=dev, device_id_type=MESH)

    barrier = pltpu.get_barrier_semaphore()
    left, right = gy > 0, gy < n_y - 1
    sides = (
        (below, (gz - 2, gy)), (above, (gz + 2, gy)), (left, (gz, gy - 1)), (right, (gz, gy + 1)),
    )
    signal(barrier, (partner, gy))
    for there, dev in sides:
        @pl.when(there)
        def _():
            signal(barrier, dev)

    def wave(which):
        there, back = sides[which], sides[which ^ 1]

        @pl.when(back[0])
        def _():
            pl.semaphore_wait(met.at[which], 1)

        @pl.when(there[0])
        def _():
            signal(met.at[which], there[1])

    @pl.when(jnp.logical_not(below))
    def _():
        for k in (k0, k1, k2):
            k[:, 0] = jnp.zeros((blk, half, nx), jnp.float32)

    @pl.when(jnp.logical_not(above))
    def _():
        for k in (k0, k1, k2):
            k[:, group_lay + 1] = jnp.zeros((blk, half, nx), jnp.float32)

    @pl.when(jnp.logical_not(before))
    def _():
        yh[:, 0] = jnp.zeros((ITERS,) + yh.shape[2:], jnp.float32)

    @pl.when(jnp.logical_not(after))
    def _():
        yh[:, 1] = jnp.zeros((ITERS,) + yh.shape[2:], jnp.float32)

    load_r(0).wait()
    SC("barrier", lambda: pl.semaphore_wait(
        barrier, 1 + sum(jnp.where(there, 1, 0) for there, _ in sides)
    ))
    rows_copy = remote(rows_out, rows_in, e_s, e_r, (partner, gy))

    def exchange(which, ch):
        layer = edge + which * (1 - 2 * p)
        vs = pl.ds(ch * vc, vc)
        return remote(
            r_ref.at[vs, pl.ds(layer, 1), pl.ds(os, half)],
            k0.at[vs, pl.ds(1 + mine_at + layer, 1)],
            x_s, x_r.at[which, ch], (partner, gy),
        )

    def z_from_rhs(ch, direction):
        vs = pl.ds(ch * vc, vc)
        if direction == 0:
            dst, dev = k0.at[vs, pl.ds(group_lay + 1, 1)], (gz - 2, gy)
        else:
            dst, dev = k0.at[vs, pl.ds(0, 1)], (gz + 2, gy)
        return remote(
            r_ref.at[vs, pl.ds(edge, 1), pl.ds(hs, half)], dst,
            z_s.at[0, direction], z_r.at[0, direction, ch], dev,
        )

    def z_copy(j, ch, direction):
        vs = pl.ds(ch * vc, vc)
        k = basis[j]
        if direction == 0:
            src, dst, dev = k.at[vs, pl.ds(1, 1)], k.at[vs, pl.ds(group_lay + 1, 1)], (gz - 2, gy)
        else:
            src, dst, dev = k.at[vs, pl.ds(group_lay, 1)], k.at[vs, pl.ds(0, 1)], (gz + 2, gy)
        return remote(src, dst, z_s.at[j, direction], z_r.at[j, direction, ch], dev)

    def y_copy(j, ch, side):
        vs = pl.ds(ch * vc, vc)
        dev = prev_dev if side == 0 else next_dev
        return remote(
            ys.at[j, side, vs], yh.at[j, 1 - side, vs],
            y_s.at[j, side], y_r.at[j, 1 - side, ch], dev,
        )

    def y_wait_recv(j, ch, side):
        vs = pl.ds(ch * vc, vc)
        remote(
            ys.at[j, side, vs], yh.at[j, side, vs], y_s.at[j, side], y_r.at[j, side, ch],
            (partner, gy),
        ).wait_recv()

    def has(j, side):
        if side == 0:
            return before if j else before & (h == 0)
        return after if j else after & (h == 1)

    early = [half * EARLY[layer % len(EARLY)] // 32 * 8 for layer in range(lay)]
    late = [half - e for e in early]

    def back_copy(j, ch, layer):
        vs = pl.ds(ch * vc, vc)
        return remote(
            basis[j].at[vs, 1 + theirs_at + layer, pl.ds(0, early[layer])],
            ret.at[j - 1, layer, vs, pl.ds(0, early[layer])],
            b_s.at[layer], b_r.at[layer], (partner, gy),
        )

    def all_back(layer):
        every = ret.at[:, layer, :, pl.ds(0, early[layer])]
        return remote(every, every, b_s.at[layer], b_r.at[layer], (partner, gy))

    def late_copy(layer, at):
        return remote(
            held.at[:, pl.ds(layer, 1), pl.ds(0, late[layer])],
            out_ref.at[
                :, pl.ds(layer, 1), pl.ds(pl.multiple_of(at + early[layer], 8), late[layer])
            ],
            l_s.at[layer], l_r.at[layer], (partner, gy),
        )

    diag_copy = remote(
        d_ref.at[:, pl.ds(os, half)], diag.at[pl.ds(mine_at, lay)], d_s, d_r, (partner, gy)
    )

    for ch in range(CHUNKS):
        if ch:
            load_r(ch).wait()
        exchange(0, ch).start()

        @pl.when((p == 0) & below)
        def _():
            z_from_rhs(ch, 0).start()

        @pl.when((p == 1) & above)
        def _():
            z_from_rhs(ch, 1).start()

    for v in range(blk):
        rows_out[v] = jnp.where(
            h == 0, r_ref[v, :, half - 1:half], r_ref[v, :, half:half + 1]
        )
    load_d.wait()
    rows_copy.start()
    diag_copy.start()
    for ch in range(CHUNKS):
        exchange(1, ch).start()

    def own(v, carry):
        k0[v, pl.ds(1 + mine_at, lay)] = r_ref[v, :, pl.ds(hs, half)]
        return carry

    lax.fori_loop(0, blk, own, 0)
    diag[pl.ds(mine_at, lay)] = d_ref[:, pl.ds(hs, half)]

    lanes = nx // 128

    def add_up(sums, tiles):
        def run(i, carry):
            layer, at = i // tiles, pl.multiple_of((i % tiles) * 8, 8)
            for lane in range(lanes):
                carry = sums(carry, layer, at, pl.ds(lane * 128, 128))
            return carry
        return run

    known = (2 * ITERS - 1) * blk * blk
    split = acc.shape[0] - 2 * blk * blk

    def keep_sum(moment, a, b, s):
        line = jnp.sum(s, axis=0, keepdims=True)
        first = moment * blk * blk + (split - known if moment >= 2 * ITERS - 1 else 0)
        at = first + a * blk + b
        acc[at:at + 1] = line
        if a != b:
            at = first + b * blk + a
            acc[at:at + 1] = line

    zero = jnp.zeros((8, 128), jnp.float32)

    def gram_rhs():
        pairs = [(a, b) for a in range(blk) for b in range(a, blk)]

        def body(sums, layer, at, cols):
            x = [r_ref[v, layer, pl.ds(at, 8), cols] for v in range(blk)]
            return tuple(s + x[a] * x[b] for s, (a, b) in zip(sums, pairs))

        sums = lax.fori_loop(
            0, lay * (rows // 8), add_up(body, rows // 8), (zero,) * len(pairs)
        )
        for s, (a, b) in zip(sums, pairs):
            keep_sum(0, a, b, s)

    def gram(j, ch):
        src, dst = basis[j], basis[j + 1]
        shift = 0 if j == ITERS - 1 else 1
        top = (ch + 1) * vc
        pairs = [(a, b) for b in range(ch * vc, top) for a in range(b + 1)]

        def body(sums, layer, at, cols):
            x = [src[v, 1 + layer, pl.ds(at, 8), cols] for v in range(top)]
            y = [dst[v, shift + layer, pl.ds(at, 8), cols] for v in range(top)]
            first, second = sums[:len(pairs)], sums[len(pairs):]
            first = tuple(s + x[a] * y[b] for s, (a, b) in zip(first, pairs))
            second = tuple(s + y[a] * y[b] for s, (a, b) in zip(second, pairs))
            return first + second

        sums = lax.fori_loop(
            0, group_lay * (half // 8), add_up(body, half // 8), (zero,) * (2 * len(pairs))
        )
        for i, (a, b) in enumerate(pairs):
            keep_sum(2 * j + 1, a, b, sums[i])
            keep_sum(2 * j + 2, a, b, sums[len(pairs) + i])

    acc[known:split] = jnp.zeros((split - known, 128), jnp.float32)
    SC("gram0", gram_rhs)

    def relay(ch):
        remote(
            r_ref.at[pl.ds(0, vc), pl.ds(0, 1), pl.ds(os, half)],
            k0.at[pl.ds(ch * vc, vc), pl.ds(1 + (group_lay - 1) * (1 - p), 1)],
            x_s, x_r.at[0, ch], (partner, gy),
        ).wait_recv()

        @pl.when((p == 0) & above)
        def _():
            z_copy(0, ch, 1).start()

        @pl.when((p == 1) & below)
        def _():
            z_copy(0, ch, 0).start()

    def stage_rows(j, v, layer, value):
        ys[j, 0, v, layer:layer + 1] = value[:1]
        ys[j, 1, v, layer:layer + 1] = value[half - 1:]

    def start_rows(j, ch):
        for side in range(2):
            @pl.when(has(j, side))
            def _():
                y_copy(j, ch, side).start()

    def arrived(ch):
        remote(
            r_ref.at[pl.ds(0, vc), pl.ds(0, 1), pl.ds(os, half)],
            k0.at[pl.ds(ch * vc, vc), pl.ds(1 + lay - p, 1)],
            x_s, x_r.at[1, ch], (partner, gy),
        ).wait_recv()

        def run(v, carry):
            for layer in range(group_lay):
                stage_rows(0, v, layer, k0[v, 1 + layer])
            return carry

        lax.fori_loop(ch * vc, (ch + 1) * vc, run, 0)
        start_rows(0, ch)

    for ch in range(CHUNKS):
        SC(f"wave#{ch}", lambda: wave(ch))
        SC(f"relay#{ch}", lambda: relay(ch))

    def rows_arrived():
        rows_copy.wait()
        for v in range(blk):
            near = jnp.where(
                h == 0, r_ref[v, :, half:half + 1], r_ref[v, :, half - 1:half]
            ).reshape(lay, nx)
            far = rows_in[v].reshape(lay, nx)
            yh[0, 1 - h, v] = jnp.where(
                p == 0,
                jnp.concatenate([near, far], axis=0),
                jnp.concatenate([far, near], axis=0),
            )
        remote(
            d_ref.at[:, pl.ds(os, half)], diag.at[pl.ds(theirs_at, lay)], d_s, d_r, (partner, gy)
        ).wait_recv()

    SC("rows_diag", rows_arrived)

    row_at = lax.broadcasted_iota(jnp.int32, (half, nx), 0)
    col_at = lax.broadcasted_iota(jnp.int32, (half, nx), 1)

    def apply(j, ch):
        src, dst = basis[j], basis[j + 1]
        shift = 0 if j == ITERS - 1 else 1
        vs = pl.ds(ch * vc, vc)

        def waits():
            @pl.when(below)
            def _():
                remote(
                    src.at[vs, pl.ds(1, 1)], src.at[vs, pl.ds(0, 1)],
                    z_s.at[j, 1], z_r.at[j, 1, ch], (partner, gy),
                ).wait_recv()

            @pl.when(above)
            def _():
                remote(
                    src.at[vs, pl.ds(1, 1)], src.at[vs, pl.ds(group_lay + 1, 1)],
                    z_s.at[j, 0], z_r.at[j, 0, ch], (partner, gy),
                ).wait_recv()

        def row_waits():
            for side in range(2):
                @pl.when(has(j, side))
                def _():
                    y_wait_recv(j, ch, side)

        SC(f"z_wait{j}#{ch}", waits)
        SC(f"y_wait{j}#{ch}", row_waits)

        def run(v, carry):
            for layer in range(group_lay):
                here = src[v, 1 + layer]
                near = src[v, layer] + src[v, 2 + layer]
                up = jnp.where(
                    row_at == 0, yh[j, 0, v, layer:layer + 1], pltpu.roll(here, 1, 0)
                )
                down = jnp.where(
                    row_at == half - 1, yh[j, 1, v, layer:layer + 1],
                    pltpu.roll(here, half - 1, 0),
                )
                left = jnp.where(col_at == 0, 0.0, pltpu.roll(here, 1, 1))
                right = jnp.where(col_at == nx - 1, 0.0, pltpu.roll(here, nx - 1, 1))
                near = near + (up + down) + (left + right)
                centre = (6.0 - CENTRE) + diag[layer]
                value = SCALE * (centre * here - near)
                dst[v, shift + layer] = value
                if j < ITERS - 1:
                    stage_rows(j + 1, v, layer, value)
            return carry

        SC(f"apply{j}#{ch}", lambda: lax.fori_loop(ch * vc, (ch + 1) * vc, run, 0))
        if j < ITERS - 1:
            @pl.when(below)
            def _():
                z_copy(j + 1, ch, 0).start()

            @pl.when(above)
            def _():
                z_copy(j + 1, ch, 1).start()

            start_rows(j + 1, ch)
        for item in BACK.get((j, ch), ()):
            back_copy(*item).start()
        SC(f"gram{j}#{ch}", lambda: gram(j, ch))

    def gather(first, last, skip):
        count = last - first
        sums = nt_dot(jnp.ones((8, 128), jnp.float32), acc[first:last])
        lane_q = lax.broadcasted_iota(jnp.int32, (8, count), 1)
        row_q = lax.broadcasted_iota(jnp.int32, (8, count), 0)
        q = lax.broadcasted_iota(jnp.int32, (count, 128), 0) + (first - skip)
        c = lax.broadcasted_iota(jnp.int32, (count, 128), 1)
        pick = (q // (blk * blk) == c // blk) & (q % blk == c % blk)
        kept = jnp.where((lane_q // blk) % blk == row_q, sums, 0.0)
        return dot(kept, jnp.where(pick, 1.0, 0.0))

    for ch in range(CHUNKS):
        SC(f"arrived#{ch}", lambda: arrived(ch))
        apply(0, ch)
    for ch in range(CHUNKS):
        apply(1, ch)

    def early_sums():
        local = gather(0, split, 0)
        mine[...] = local[:4] + pltpu.roll(local, 64, 1)[4:]

    SC("early_sums", early_sums)
    for ch in range(CHUNKS):
        apply(2, ch)

    def reduce():
        local = gather(split, acc.shape[0], split - known)
        packed = mine[...] + local[:4] + pltpu.roll(local, 64, 1)[4:]
        mine[...] = packed
        slots[me] = packed

        def send(off, carry):
            to = (me + off) % n_dev
            remote(mine, slots.at[me], g_s, g_r, device(to)).start()
            return carry

        lax.fori_loop(1, n_dev, send, 0)
        for item in BACK.get("reduce", ()):
            back_copy(*item).start()

    SC("red_send", reduce)

    def collect():
        others = slots.at[pl.ds(0, n_dev - 1)]
        remote(others, others, g_s, g_r, (partner, gy)).wait()

    SC("red_wait", collect)
    packed = jnp.sum(slots[...], axis=0)

    lane = lax.broadcasted_iota(jnp.int32, (8, 128), 1)
    keep = lambda x, low, high: jnp.where((lane >= low) & (lane < high), x, 0.0)
    left_by = lambda x, n: x if n == 0 else pltpu.roll(x, 128 - n, 1)
    moments = keep(
        jnp.concatenate([packed, pltpu.roll(packed, 64, 1)], axis=0), 0, 64
    )
    small, order = ITERS * blk, (ITERS + 1) * blk
    inv = 1.0 / SCALE

    def solve():
        second = (
            (inv * inv) * left_by(moments, 2 * blk)
            + (2.0 * CENTRE * inv) * left_by(moments, blk)
            + (CENTRE * CENTRE) * moments
        )
        target = inv * left_by(moments, blk) + CENTRE * moments
        normal = jnp.concatenate(
            [
                keep(left_by(second, blk * i), 0, small)
                + keep(pltpu.roll(target, small - blk * i, 1) if i < ITERS else target, small, order)
                for i in range(ITERS)
            ],
            axis=0,
        )
        rows_small = lax.broadcasted_iota(jnp.int32, (small, 1), 0)
        for k in range(small):
            row = normal[k:k + 1] / normal[k:k + 1, k:k + 1]
            column = jnp.where(rows_small == k, 0.0, normal[:, k:k + 1])
            normal = jnp.where(rows_small == k, row, normal - column * row)
        return normal

    normal = SC("solve", solve)

    def factor():
        lane32 = lax.broadcasted_iota(jnp.int32, (order, 128), 1)
        row32 = lax.broadcasted_iota(jnp.int32, (order, 128), 0)
        full = jnp.concatenate(
            [keep(left_by(moments, blk * i), 0, order) for i in range(ITERS + 1)], axis=0
        )
        full = full + jnp.where(lane32 == row32 + order, 1.0, 0.0)
        rows_full = lax.broadcasted_iota(jnp.int32, (order, 1), 0)
        for k in range(order):
            row = full[k:k + 1] / full[k:k + 1, k:k + 1]
            column = jnp.where(rows_full <= k, 0.0, full[:, k:k + 1])
            full = full - column * row
        pivots = jnp.sum(jnp.where(lane32 == row32, full, 0.0), axis=1, keepdims=True)
        full = full / jnp.sqrt(pivots)
        upper = jnp.where((lane32 < order) & (lane32 >= row32), full, 0.0)
        lower_inv = left_by(full, order)
        lower_inv = jnp.where(lane32 < small, lower_inv, 0.0)[:small]
        hess = inv * nt_dot(pltpu.roll(lower_inv, blk, 1), upper)
        row_h = lax.broadcasted_iota(jnp.int32, (small, order), 0)
        col_h = lax.broadcasted_iota(jnp.int32, (small, order), 1)
        hess = hess + jnp.where(row_h == col_h, CENTRE, 0.0)
        hess_ref[...] = jnp.where(col_h // blk <= row_h // blk + 1, hess, 0.0)

    def spread():
        for k in range(small):
            for u in range(blk):
                splat[k * blk + u] = jnp.broadcast_to(
                    normal[k:k + 1, small + u:small + u + 1], (8, 128)
                )

    SC("splat", spread)

    def combine(dst, layers, row_start, height, sources):
        tiles = height // 8

        def run(i, carry):
            layer, t = layers[0] + i // tiles, i % tiles
            at = pl.multiple_of(row_start + t * 8, 8)
            for lane_at in range(lanes):
                cols = pl.ds(lane_at * 128, 128)
                vals = []
                for ref, l_at, base in sources:
                    first_row = pl.multiple_of(base + t * 8, 8)
                    vals += [
                        ref[v, pl.ds(first_row, 8), cols] if l_at is None
                        else ref[v, l_at + layer, pl.ds(first_row, 8), cols]
                        for v in range(blk)
                    ]
                for u in range(blk):
                    total = splat[u] * vals[0]
                    for k in range(1, small):
                        total = total + splat[k * blk + u] * vals[k]
                    dst[u, layer, pl.ds(at, 8), cols] = total
            return carry

        lax.fori_loop(0, (layers[1] - layers[0]) * tiles, run, 0)

    def send_late():
        for layer in range(lay):
            combine(
                held, (layer, layer + 1), 0, late[layer],
                [(k, 1 + theirs_at, early[layer]) for k in basis[:ITERS]],
            )
            late_copy(layer, hs).start()

    SC("comb_late", send_late)
    SC("comb_own", lambda: combine(
        out_ref, (0, lay), hs, half, ((r_ref, 0, hs), (k1, 1 + mine_at, 0), (k2, 1 + mine_at, 0))
    ))

    def back_wait():
        for layer in range(lay):
            all_back(layer).wait()

    SC("back_wait", back_wait)

    def rest():
        for layer in range(lay):
            combine(
                out_ref, (layer, layer + 1), os, early[layer],
                ((r_ref, 0, os), (ret.at[0, layer], None, 0), (ret.at[1, layer], None, 0)),
            )

    SC("comb_other", rest)
    SC("factor", factor)

    def drain():
        whole = r_ref.at[:, :, pl.ds(os, half)]
        remote(whole, whole, x_s, x_r.at[0, 0], (partner, gy)).wait_send()
        for j in range(ITERS):
            for direction, there in ((0, below), (1, above)):
                @pl.when(there)
                def _():
                    every = basis[j].at[:, pl.ds(0, 1)]
                    remote(
                        every, every, z_s.at[j, direction], z_r.at[j, direction, 0], (partner, gy)
                    ).wait_send()

            for side in range(2):
                @pl.when(has(j, side))
                def _():
                    every = ys.at[j, side]
                    remote(
                        every, every, y_s.at[j, side], y_r.at[j, side, 0], (partner, gy)
                    ).wait_send()

        diag_copy.wait_send()

    SC("drain", drain)

    def late_wait():
        for layer in range(lay):
            late_copy(layer, hs).wait_send()
            late_copy(layer, os).wait_recv()

    SC("late_wait", late_wait)


def store(x_ref, h_ref, x_out, h_out, sems):
    copies = (
        pltpu.make_async_copy(x_ref, x_out, sems.at[0]),
        pltpu.make_async_copy(h_ref, h_out, sems.at[1]),
    )
    for copy in copies:
        copy.start()
    for copy in copies:
        copy.wait()


def body(right_side, diagonal):
    blk, lay, rows, nx = right_side.shape
    half, group_lay = rows // 2, 2 * lay
    early = [half * EARLY[layer % len(EARLY)] // 32 * 8 for layer in range(lay)]
    n_z, n_y = lax.axis_size("gz"), lax.axis_size("gy")
    vmem = lambda *shape: pltpu.VMEM(shape, jnp.float32)
    dma = lambda *shape: pltpu.SemaphoreType.DMA(shape) if shape else pltpu.SemaphoreType.DMA
    small, order = ITERS * blk, (ITERS + 1) * blk
    in_hbm = lambda x: pltpu.with_memory_space_constraint(x, pltpu.HBM)
    x, h = pl.pallas_call(
        kernel,
        out_shape=(vmem(*right_side.shape), vmem(small, order)),
        in_specs=[pl.BlockSpec(memory_space=pltpu.HBM)] * 2,
        out_specs=(pl.BlockSpec(memory_space=pltpu.VMEM),) * 2,
        scratch_shapes=[
            vmem(*right_side.shape),
            vmem(*diagonal.shape),
            vmem(blk, group_lay + 2, half, nx),
            vmem(blk, group_lay + 2, half, nx),
            vmem(blk, group_lay + 2, half, nx),
            vmem(blk, group_lay, half, nx),
            vmem(group_lay, half, nx),
            vmem(ITERS - 1, lay, blk, max(early), nx),
            vmem(blk, lay, half - min(early), nx),
            vmem(ITERS, 2, blk, group_lay, nx),
            vmem(ITERS, 2, blk, group_lay, nx),
            vmem(blk, lay, 1, nx),
            vmem(blk, lay, 1, nx),
            vmem(8 * blk * blk, 128),
            vmem(4, 128),
            vmem(n_z * n_y, 4, 128),
            vmem(small * blk, 8, 128),
            dma(CHUNKS + 1), pltpu.SemaphoreType.REGULAR((4,)),
            dma(), dma(2, CHUNKS),
            dma(), dma(),
            dma(ITERS, 2), dma(ITERS, 2, CHUNKS),
            dma(ITERS, 2), dma(ITERS, 2, CHUNKS),
            dma(), dma(),
            dma(lay), dma(lay), dma(lay), dma(lay),
            dma(), dma(),
        ],
        compiler_params=pltpu.CompilerParams(
            collective_id=0, has_side_effects=True, vmem_limit_bytes=40 * 1024 * 1024
        ),
        name="gmres",
    )(in_hbm(right_side), in_hbm(diagonal))
    in_vmem = lambda x: pltpu.with_memory_space_constraint(x, pltpu.VMEM)
    return pl.pallas_call(
        store,
        out_shape=(
            jax.ShapeDtypeStruct(x.shape, jnp.float32), jax.ShapeDtypeStruct(h.shape, jnp.float32),
        ),
        in_specs=[pl.BlockSpec(memory_space=pltpu.VMEM)] * 2,
        out_specs=(pl.BlockSpec(memory_space=pltpu.HBM),) * 2,
        scratch_shapes=[dma(2)],
        compiler_params=pltpu.CompilerParams(vmem_limit_bytes=4 * 1024 * 1024),
        name="store",
    )(in_vmem(x), in_vmem(h))


def solution(mesh):
    in_specs = (P(None, "gz", "gy", None), P("gz", "gy", None))
    out_specs = (P(None, "gz", "gy", None), P())
    return jax.shard_map(body, mesh=mesh, in_specs=in_specs, out_specs=out_specs, check_vma=False)
```

```python
import functools

import jax
import jax.numpy as jnp
from jax import lax
from jax.experimental import pallas as pl
from jax.experimental.pallas import tpu as pltpu
from jax.sharding import PartitionSpec as P

ITERS = 3
CENTRE = 7.5
SCALE = 0.25
CUTS = (0, 1, 3, 5, 7, 8)
CHUNKS = len(CUTS) - 1
EARLY = (1, 1)
BACK = {
    (0, 1): ("ghost",), (0, 2): ((0, 0),), (0, 3): ((0, 1),), (0, 4): ((0, 2),), (1, 1): ((0, 3),),
    (1, 4): ((0, 4), (1, 0)), (2, 0): ((1, 1),), (2, 1): ((1, 2),),
    "reduce": ((1, 3), (1, 4), (2, 0), (2, 1), (2, 2), (2, 3), (2, 4)),
}
RELAY = {(2, 1): (0,), "reduce": (1, 2, 3, 4)}
MESH = pl.DeviceIdType.MESH
HIGH = lax.Precision.HIGHEST


def SC(name, f):
    with jax.named_scope(name):
        return f()


def nt_dot(left, right):
    return lax.dot_general(
        left, right, (((1,), (1,)), ((), ())), precision=HIGH, preferred_element_type=jnp.float32
    )


def dot(left, right):
    return jnp.dot(left, right, precision=HIGH, preferred_element_type=jnp.float32)


def kernel(
    r_hbm, d_hbm, out_ref, hess_ref,
    r_ref, d_ref, k0, k1, k2, k3, diag, ret, held, ys, yh, rows_out, rows_in,
    deep, d_deep, g_out, g_in, kd1, kd2,
    acc, mine, slots, splat, i_s, met,
    x_s, x_r, d_s, d_r, z_s, z_r, y_s, y_r, e_s, e_r, b_s, b_r, l_s, l_r, g_s, g_r,
    q_s, q_r, qz_s, qz_r, w_s, w_r,
):
    blk, lay, rows, nx = r_ref.shape
    half, group_lay = rows // 2, 2 * lay
    starts = [blk * cut // CUTS[-1] for cut in CUTS]
    part = lambda ch: pl.ds(starts[ch], starts[ch + 1] - starts[ch])
    n_z, n_y = lax.axis_size("gz"), lax.axis_size("gy")
    gz, gy = lax.axis_index("gz"), lax.axis_index("gy")
    n_dev = n_z * n_y
    me = gz * n_y + gy
    p, group = gz % 2, gz // 2
    h = (p + gy) % 2
    partner = gz + 1 - 2 * p
    hs = pl.multiple_of(h * half, half)
    os = pl.multiple_of((1 - h) * half, half)
    mine_at = p * lay
    theirs_at = (1 - p) * lay
    below, above = group > 0, group < n_z // 2 - 1
    place = 2 * gy + h
    before, after = place > 0, place < 2 * n_y - 1
    prev_dev = (gz + h * (partner - gz), gy - (1 - h))
    next_dev = (gz + (1 - h) * (partner - gz), gy + h)
    basis = (k0, k1, k2, k3)
    edge = (lay - 1) * p
    inner = half // 2
    outer = half - inner
    early = [outer * EARLY[layer % len(EARLY)] // 16 * 8 for layer in range(lay)]
    late = [outer - e for e in early]
    theirs_out = pl.multiple_of(h * inner, 8)
    mine_out = pl.multiple_of((1 - h) * inner, 8)
    inner_at = pl.multiple_of(os + h * outer, 8)
    far, near_l = (lay - 1) * p, (lay - 1) * (1 - p)
    beyond = jnp.where(p == 0, below, above)
    onward = jnp.where(p == 0, above, below)
    onward_dev = (gz + 2 - 4 * p, gy)

    def remote(src, dst, send, recv, dev):
        return pltpu.make_async_remote_copy(
            src_ref=src, dst_ref=dst, send_sem=send, recv_sem=recv, device_id=dev,
            device_id_type=MESH,
        )

    def device(i):
        return (i // n_y, i % n_y)

    def load_r(ch):
        vs = part(ch)
        return pltpu.make_async_copy(r_hbm.at[vs], r_ref.at[vs], i_s.at[ch])

    load_d = pltpu.make_async_copy(d_hbm, d_ref, i_s.at[CHUNKS])
    for ch in range(CHUNKS):
        load_r(ch).start()
    load_d.start()

    def signal(semaphore, dev):
        pl.semaphore_signal(semaphore, inc=1, device_id=dev, device_id_type=MESH)

    barrier = pltpu.get_barrier_semaphore()
    left, right = gy > 0, gy < n_y - 1
    sides = (
        (below, (gz - 2, gy)), (above, (gz + 2, gy)), (left, (gz, gy - 1)), (right, (gz, gy + 1)),
    )
    signal(barrier, (partner, gy))
    for there, dev in sides:
        @pl.when(there)
        def _():
            signal(barrier, dev)

    def wave(which):
        there, back = sides[which], sides[which ^ 1]

        @pl.when(back[0])
        def _():
            pl.semaphore_wait(met.at[which], 1)

        @pl.when(there[0])
        def _():
            signal(met.at[which], there[1])

    @pl.when(jnp.logical_not(below))
    def _():
        for k in (k0, k1, k2):
            k[:, 0] = jnp.zeros((blk, half, nx), jnp.float32)

    @pl.when(jnp.logical_not(above))
    def _():
        for k in (k0, k1, k2):
            k[:, group_lay + 1] = jnp.zeros((blk, half, nx), jnp.float32)

    @pl.when(jnp.logical_not(before))
    def _():
        yh[:, 0] = jnp.zeros((ITERS,) + yh.shape[2:], jnp.float32)

    @pl.when(jnp.logical_not(after))
    def _():
        yh[:, 1] = jnp.zeros((ITERS,) + yh.shape[2:], jnp.float32)

    @pl.when(jnp.logical_not(beyond))
    def _():
        deep[0:2] = jnp.zeros((2,) + deep.shape[1:], jnp.float32)
        d_deep[0] = jnp.zeros(d_deep.shape[1:], jnp.float32)
        g_in[:, 0] = jnp.zeros((blk, 1, nx), jnp.float32)

    load_r(0).wait()
    SC("barrier", lambda: pl.semaphore_wait(
        barrier, 1 + sum(jnp.where(there, 1, 0) for there, _ in sides)
    ))
    rows_copy = remote(rows_out, rows_in, e_s, e_r, (partner, gy))

    def exchange(which, ch):
        layer = edge + which * (1 - 2 * p)
        vs = part(ch)
        return remote(
            r_ref.at[vs, pl.ds(layer, 1), pl.ds(os, half)],
            k0.at[vs, pl.ds(1 + mine_at + layer, 1)],
            x_s, x_r.at[which, ch], (partner, gy),
        )

    def z_from_rhs(ch, direction):
        vs = part(ch)
        if direction == 0:
            dst, dev = k0.at[vs, pl.ds(group_lay + 1, 1)], (gz - 2, gy)
        else:
            dst, dev = k0.at[vs, pl.ds(0, 1)], (gz + 2, gy)
        return remote(
            r_ref.at[vs, pl.ds(edge, 1), pl.ds(hs, half)], dst,
            z_s.at[direction], z_r.at[0, direction, ch], dev,
        )

    def z_copy(j, ch, direction):
        vs = part(ch)
        k = basis[j]
        if direction == 0:
            src, dst, dev = k.at[vs, pl.ds(1, 1)], k.at[vs, pl.ds(group_lay + 1, 1)], (gz - 2, gy)
        else:
            src, dst, dev = k.at[vs, pl.ds(group_lay, 1)], k.at[vs, pl.ds(0, 1)], (gz + 2, gy)
        return remote(src, dst, z_s.at[direction], z_r.at[j % 2, direction, ch], dev)

    def y_copy(j, ch, side):
        vs = part(ch)
        dev = prev_dev if side == 0 else next_dev
        return remote(
            ys.at[j, side, vs], yh.at[j, 1 - side, vs],
            y_s.at[side], y_r.at[j % 2, 1 - side, ch], dev,
        )

    def y_wait_recv(j, ch, side):
        vs = part(ch)
        remote(
            ys.at[j, side, vs], yh.at[j, side, vs], y_s.at[side], y_r.at[j % 2, side, ch],
            (partner, gy),
        ).wait_recv()

    def has(j, side):
        if side == 0:
            return before if j else before & (h == 0)
        return after if j else after & (h == 1)

    def back_copy(j, ch):
        vs = part(ch)
        return [
            remote(
                basis[j].at[vs, 1 + theirs_at + layer, pl.ds(theirs_out, early[layer])],
                ret.at[j - 1, layer, vs, pl.ds(0, early[layer])],
                b_s.at[layer], b_r.at[layer], (partner, gy),
            )
            for layer in range(lay)
        ]

    def all_back(layer):
        every = ret.at[:, layer, :, pl.ds(0, early[layer])]
        return remote(every, every, b_s.at[layer], b_r.at[layer], (partner, gy))

    def late_copy(layer, at, first, count):
        return remote(
            held.at[:, pl.ds(layer, 1), pl.ds(first, count)],
            out_ref.at[
                :, pl.ds(layer, 1), pl.ds(pl.multiple_of(at + early[layer] + first, 8), count)
            ],
            l_s.at[layer], l_r.at[layer], (partner, gy),
        )

    give_at = pl.multiple_of(hs + (1 - h) * outer, 8)

    def deep_copy(ch):
        vs = part(ch)
        return [
            remote(
                r_ref.at[vs, layer, pl.ds(give_at, inner)], deep.at[slot, vs],
                q_s, q_r.at[ch], (partner, gy),
            )
            for slot, layer in ((2, near_l), (3, far))
        ]

    def deep_recv(ch):
        every = deep.at[pl.ds(2, 2), part(ch)]
        return remote(every, every, q_s, q_r.at[ch], (partner, gy))

    def deep_relay(ch):
        vs = part(ch)
        return remote(
            deep.at[pl.ds(2, 2), vs], deep.at[pl.ds(0, 2), vs], qz_s, qz_r.at[ch], onward_dev
        )

    ghost_copies = [
        remote(g_out, g_in.at[:, pl.ds(1, 2)], w_s.at[0], w_r.at[0], (partner, gy))
    ] + [
        remote(
            d_ref.at[layer, pl.ds(give_at, inner)], d_deep.at[slot], w_s.at[1], w_r.at[1],
            (partner, gy),
        )
        for slot, layer in ((1, near_l), (2, far))
    ]
    both_diag = d_deep.at[pl.ds(1, 2)]
    ghost_diag = remote(both_diag, both_diag, w_s.at[1], w_r.at[1], (partner, gy))
    ghost_relays = (
        remote(g_in.at[:, pl.ds(2, 1)], g_in.at[:, pl.ds(0, 1)], w_s.at[2], w_r.at[2], onward_dev),
        remote(d_deep.at[pl.ds(2, 1)], d_deep.at[pl.ds(0, 1)], w_s.at[3], w_r.at[3], onward_dev),
    )

    def issue(items):
        for item in items:
            if item == "ghost":
                copies = ghost_copies
            else:
                copies = back_copy(*item) if item[0] else deep_copy(item[1])
            for copy in copies:
                copy.start()

    def relay_deep(ch):
        deep_recv(ch).wait_recv()
        if ch == 0:
            ghost_copies[0].wait_recv()
            ghost_diag.wait_recv()

        @pl.when(onward)
        def _():
            deep_relay(ch).start()
            if ch == 0:
                for copy in ghost_relays:
                    copy.start()

    diag_copy = remote(
        d_ref.at[:, pl.ds(os, half)], diag.at[pl.ds(mine_at, lay)], d_s, d_r, (partner, gy)
    )

    for ch in range(CHUNKS):
        if ch:
            load_r(ch).wait()
        exchange(0, ch).start()

        @pl.when((p == 0) & below)
        def _():
            z_from_rhs(ch, 0).start()

        @pl.when((p == 1) & above)
        def _():
            z_from_rhs(ch, 1).start()

    for v in range(blk):
        rows_out[v] = jnp.where(
            h == 0, r_ref[v, :, half - 1:half], r_ref[v, :, half:half + 1]
        )
        for slot, layer in ((0, near_l), (1, far)):
            g_out[v, slot] = jnp.where(
                h == 0, r_ref[v, layer, outer - 1:outer], r_ref[v, layer, half + inner:half + inner + 1]
            )
    load_d.wait()
    rows_copy.start()
    diag_copy.start()
    for ch in range(CHUNKS):
        exchange(1, ch).start()

    def own(v, carry):
        k0[v, pl.ds(1 + mine_at, lay)] = r_ref[v, :, pl.ds(hs, half)]
        return carry

    lax.fori_loop(0, blk, own, 0)
    diag[pl.ds(mine_at, lay)] = d_ref[:, pl.ds(hs, half)]

    lanes = nx // 128

    def add_up(sums, tiles):
        def run(i, carry):
            layer, at = i // tiles, pl.multiple_of((i % tiles) * 8, 8)
            for lane in range(lanes):
                carry = sums(carry, layer, at, pl.ds(lane * 128, 128))
            return carry
        return run

    known = (2 * ITERS - 1) * blk * blk
    split = acc.shape[0] - 2 * blk * blk

    def keep_sum(moment, a, b, s):
        line = jnp.sum(s, axis=0, keepdims=True)
        first = moment * blk * blk + (split - known if moment >= 2 * ITERS - 1 else 0)
        at = first + a * blk + b
        acc[at:at + 1] = line
        if a != b:
            at = first + b * blk + a
            acc[at:at + 1] = line

    zero = jnp.zeros((8, 128), jnp.float32)

    def gram_rhs():
        pairs = [(a, b) for a in range(blk) for b in range(a, blk)]

        def body(sums, layer, at, cols):
            x = [r_ref[v, layer, pl.ds(at, 8), cols] for v in range(blk)]
            return tuple(s + x[a] * x[b] for s, (a, b) in zip(sums, pairs))

        sums = lax.fori_loop(
            0, lay * (rows // 8), add_up(body, rows // 8), (zero,) * len(pairs)
        )
        for s, (a, b) in zip(sums, pairs):
            keep_sum(0, a, b, s)

    def gram(j, ch):
        src, dst = basis[j], basis[j + 1]
        shift = 0 if j == ITERS - 1 else 1
        top = starts[ch + 1]
        pairs = [(a, b) for b in range(starts[ch], top) for a in range(b + 1)]

        def body(sums, layer, at, cols):
            x = [src[v, 1 + layer, pl.ds(at, 8), cols] for v in range(top)]
            y = [dst[v, shift + layer, pl.ds(at, 8), cols] for v in range(top)]
            first, second = sums[:len(pairs)], sums[len(pairs):]
            first = tuple(s + x[a] * y[b] for s, (a, b) in zip(first, pairs))
            second = tuple(s + y[a] * y[b] for s, (a, b) in zip(second, pairs))
            return first + second

        sums = lax.fori_loop(
            0, group_lay * (half // 8), add_up(body, half // 8), (zero,) * (2 * len(pairs))
        )
        for i, (a, b) in enumerate(pairs):
            keep_sum(2 * j + 1, a, b, sums[i])
            keep_sum(2 * j + 2, a, b, sums[len(pairs) + i])

    acc[known:split] = jnp.zeros((split - known, 128), jnp.float32)
    SC("gram0", gram_rhs)

    def relay(ch):
        remote(
            r_ref.at[part(ch), pl.ds(0, 1), pl.ds(os, half)],
            k0.at[part(ch), pl.ds(1 + (group_lay - 1) * (1 - p), 1)],
            x_s, x_r.at[0, ch], (partner, gy),
        ).wait_recv()

        @pl.when((p == 0) & above)
        def _():
            z_copy(0, ch, 1).start()

        @pl.when((p == 1) & below)
        def _():
            z_copy(0, ch, 0).start()

    def stage_rows(j, v, layer, value):
        ys[j, 0, v, layer:layer + 1] = value[:1]
        ys[j, 1, v, layer:layer + 1] = value[half - 1:]

    def start_rows(j, ch):
        for side in range(2):
            @pl.when(has(j, side))
            def _():
                y_copy(j, ch, side).start()

    def arrived(ch):
        remote(
            r_ref.at[part(ch), pl.ds(0, 1), pl.ds(os, half)],
            k0.at[part(ch), pl.ds(1 + lay - p, 1)],
            x_s, x_r.at[1, ch], (partner, gy),
        ).wait_recv()

        def run(v, carry):
            for layer in range(group_lay):
                stage_rows(0, v, layer, k0[v, 1 + layer])
            return carry

        lax.fori_loop(starts[ch], starts[ch + 1], run, 0)
        start_rows(0, ch)

    for ch in range(CHUNKS):
        if ch < len(sides):
            SC(f"wave#{ch}", lambda: wave(ch))
        SC(f"relay#{ch}", lambda: relay(ch))

    def rows_arrived():
        rows_copy.wait()
        for v in range(blk):
            near = jnp.where(
                h == 0, r_ref[v, :, half:half + 1], r_ref[v, :, half - 1:half]
            ).reshape(lay, nx)
            far = rows_in[v].reshape(lay, nx)
            yh[0, 1 - h, v] = jnp.where(
                p == 0,
                jnp.concatenate([near, far], axis=0),
                jnp.concatenate([far, near], axis=0),
            )
        remote(
            d_ref.at[:, pl.ds(os, half)], diag.at[pl.ds(theirs_at, lay)], d_s, d_r, (partner, gy)
        ).wait_recv()

    SC("rows_diag", rows_arrived)

    row_at = lax.broadcasted_iota(jnp.int32, (half, nx), 0)
    col_at = lax.broadcasted_iota(jnp.int32, (half, nx), 1)

    def apply(j, ch):
        src, dst = basis[j], basis[j + 1]
        shift = 0 if j == ITERS - 1 else 1
        vs = part(ch)

        def waits():
            @pl.when(below)
            def _():
                remote(
                    src.at[vs, pl.ds(1, 1)], src.at[vs, pl.ds(0, 1)],
                    z_s.at[1], z_r.at[j % 2, 1, ch], (partner, gy),
                ).wait_recv()

            @pl.when(above)
            def _():
                remote(
                    src.at[vs, pl.ds(1, 1)], src.at[vs, pl.ds(group_lay + 1, 1)],
                    z_s.at[0], z_r.at[j % 2, 0, ch], (partner, gy),
                ).wait_recv()

        def row_waits():
            for side in range(2):
                @pl.when(has(j, side))
                def _():
                    y_wait_recv(j, ch, side)

        for which in RELAY.get((j, ch), ()):
            SC(f"drelay#{which}", lambda: relay_deep(which))
        SC(f"z_wait{j}#{ch}", waits)
        SC(f"y_wait{j}#{ch}", row_waits)

        def run(v, carry):
            for layer in range(group_lay):
                here = src[v, 1 + layer]
                near = src[v, layer] + src[v, 2 + layer]
                up = jnp.where(
                    row_at == 0, yh[j, 0, v, layer:layer + 1], pltpu.roll(here, 1, 0)
                )
                down = jnp.where(
                    row_at == half - 1, yh[j, 1, v, layer:layer + 1],
                    pltpu.roll(here, half - 1, 0),
                )
                left = jnp.where(col_at == 0, 0.0, pltpu.roll(here, 1, 1))
                right = jnp.where(col_at == nx - 1, 0.0, pltpu.roll(here, nx - 1, 1))
                near = near + (up + down) + (left + right)
                centre = (6.0 - CENTRE) + diag[layer]
                value = SCALE * (centre * here - near)
                dst[v, shift + layer] = value
                if j < ITERS - 1:
                    stage_rows(j + 1, v, layer, value)
            return carry

        SC(f"apply{j}#{ch}", lambda: lax.fori_loop(starts[ch], starts[ch + 1], run, 0))
        if j < ITERS - 1:
            @pl.when(below)
            def _():
                z_copy(j + 1, ch, 0).start()

            @pl.when(above)
            def _():
                z_copy(j + 1, ch, 1).start()

            start_rows(j + 1, ch)
        issue(BACK.get((j, ch), ()))
        SC(f"gram{j}#{ch}", lambda: gram(j, ch))

    def gather(first, last, skip):
        count = last - first
        sums = nt_dot(jnp.ones((8, 128), jnp.float32), acc[first:last])
        lane_q = lax.broadcasted_iota(jnp.int32, (8, count), 1)
        row_q = lax.broadcasted_iota(jnp.int32, (8, count), 0)
        q = lax.broadcasted_iota(jnp.int32, (count, 128), 0) + (first - skip)
        c = lax.broadcasted_iota(jnp.int32, (count, 128), 1)
        pick = (q // (blk * blk) == c // blk) & (q % blk == c % blk)
        kept = jnp.where((lane_q // blk) % blk == row_q, sums, 0.0)
        return dot(kept, jnp.where(pick, 1.0, 0.0))

    row_d = lax.broadcasted_iota(jnp.int32, (inner, nx), 0)
    col_d = lax.broadcasted_iota(jnp.int32, (inner, nx), 1)

    def sideways(here, col):
        return jnp.where(col == 0, 0.0, pltpu.roll(here, 1, 1)) + jnp.where(
            col == nx - 1, 0.0, pltpu.roll(here, nx - 1, 1)
        )

    def deepen(ch):
        @pl.when(beyond)
        def _():
            every = deep.at[pl.ds(0, 2), part(ch)]
            remote(every, every, qz_s, qz_r.at[ch], (partner, gy)).wait_recv()
            if ch == 0:
                for slot, ref in ((2, g_in.at[:, pl.ds(0, 1)]), (3, d_deep.at[pl.ds(0, 1)])):
                    remote(ref, ref, w_s.at[slot], w_r.at[slot], (partner, gy)).wait_recv()

        edge_of = lambda ref, v, slot: jnp.where(
            h == 0, ref[v, slot, half - 1:half], ref[v, slot, 0:1]
        )
        ghost_of = lambda row: jnp.where(
            h == 0, row(half + inner), row(outer - 1)
        )
        after_of = lambda row: jnp.where(
            h == 0, row(half + inner + 1), row(outer - 2)
        )
        slots = {
            "beyond": (group_lay + 1) * p, "far": 1 + (group_lay - 1) * p,
            "near": lay + p, "next": lay + 1 - p,
        }
        d_far, d_near = d_ref[far, pl.ds(inner_at, inner)], d_ref[near_l, pl.ds(inner_at, inner)]
        g_far = ghost_of(lambda i: d_ref[far, i:i + 1])
        g_near = ghost_of(lambda i: d_ref[near_l, i:i + 1])
        exists = jnp.where(beyond, 1.0, 0.0)
        one_col = lax.broadcasted_iota(jnp.int32, (1, nx), 1)

        def block(here, below_z, above_z, edge_row, ghost_row, extra):
            up = jnp.where(
                row_d == 0, jnp.where(h == 0, edge_row, ghost_row), pltpu.roll(here, 1, 0)
            )
            down = jnp.where(
                row_d == inner - 1, jnp.where(h == 0, ghost_row, edge_row),
                pltpu.roll(here, inner - 1, 0),
            )
            near = (below_z + above_z) + (up + down) + sideways(here, col_d)
            return SCALE * (((6.0 - CENTRE) + extra) * here - near)

        def run(v, carry):
            r_far = r_ref[v, far, pl.ds(inner_at, inner)]
            r_near = r_ref[v, near_l, pl.ds(inner_at, inner)]
            two, one, nxt, last = deep[0, v], deep[1, v], deep[2, v], deep[3, v]
            ghost_far = ghost_of(lambda i: r_ref[v, far, i:i + 1])
            ghost_near = ghost_of(lambda i: r_ref[v, near_l, i:i + 1])
            ghost_one, ghost_next = g_in[v, 0], g_in[v, 1]
            rows_of = lambda which: edge_of(k0, v, slots[which])
            k_one = exists * block(one, two, r_far, rows_of("beyond"), ghost_one, d_deep[0])
            k_far = block(r_far, one, r_near, rows_of("far"), ghost_far, d_far)
            k_near = block(r_near, r_far, nxt, rows_of("near"), ghost_near, d_near)
            k_next = block(nxt, r_near, last, rows_of("next"), ghost_next, d_deep[1])

            def line(here, inside, layer, beside, extra):
                outside = after_of(lambda i: r_ref[v, layer, i:i + 1])
                within = jnp.where(h == 0, inside[inner - 1:inner], inside[0:1])
                near = beside + (outside + within) + sideways(here, one_col)
                return SCALE * (((6.0 - CENTRE) + extra) * here - near)

            line_far = line(ghost_far, r_far, far, ghost_one + ghost_near, g_far)
            line_near = line(ghost_near, r_near, near_l, ghost_far + ghost_next, g_near)
            kd1[0, v], kd1[1, v] = k_far, k_near
            kd2[0, v] = block(
                k_far, k_one, k_near, edge_of(k1, v, slots["far"]), line_far, d_far
            )
            kd2[1, v] = block(
                k_near, k_far, k_next, edge_of(k1, v, slots["near"]), line_near, d_near
            )
            return carry

        lax.fori_loop(starts[ch], starts[ch + 1], run, 0)

    for ch in range(CHUNKS):
        SC(f"arrived#{ch}", lambda: arrived(ch))
        apply(0, ch)
    for ch in range(CHUNKS):
        apply(1, ch)

    def early_sums():
        local = gather(0, split, 0)
        mine[...] = local[:4] + pltpu.roll(local, 64, 1)[4:]

    SC("early_sums", early_sums)
    for ch in range(CHUNKS):
        apply(2, ch)

    def reduce():
        lane_s = lax.broadcasted_iota(jnp.int32, (8, 128), 1)
        local = jnp.zeros((8, 128), jnp.float32)
        for i in range(2 * blk):
            column = jnp.sum(acc[split + i * blk:split + (i + 1) * blk], axis=1, keepdims=True)
            local = local + jnp.where(lane_s == known // blk + i, column, 0.0)
        packed = mine[...] + local[:4] + pltpu.roll(local, 64, 1)[4:]
        mine[...] = packed
        slots[me] = packed

        def send(off, carry):
            to = (me + off) % n_dev
            remote(mine, slots.at[me], g_s, g_r, device(to)).start()
            return carry

        lax.fori_loop(1, n_dev, send, 0)
        issue(BACK.get("reduce", ()))
        for which in RELAY.get("reduce", ()):
            relay_deep(which)

    SC("red_send", reduce)

    def collect():
        others = slots.at[pl.ds(0, n_dev - 1)]
        remote(others, others, g_s, g_r, (partner, gy)).wait()

    SC("deepen#0", lambda: deepen(0))
    SC("red_wait", collect)
    packed = jnp.sum(slots[...], axis=0)

    lane = lax.broadcasted_iota(jnp.int32, (8, 128), 1)
    keep = lambda x, low, high: jnp.where((lane >= low) & (lane < high), x, 0.0)
    left_by = lambda x, n: x if n == 0 else pltpu.roll(x, 128 - n, 1)
    moments = keep(
        jnp.concatenate([packed, pltpu.roll(packed, 64, 1)], axis=0), 0, 64
    )
    small, order = ITERS * blk, (ITERS + 1) * blk
    inv = 1.0 / SCALE

    wide = lambda x: jnp.broadcast_to(x, (1, 128))

    def solve():
        second = (
            (inv * inv) * left_by(moments, 2 * blk)
            + (2.0 * CENTRE * inv) * left_by(moments, blk)
            + (CENTRE * CENTRE) * moments
        )
        target = inv * left_by(moments, blk) + CENTRE * moments
        normal = jnp.concatenate(
            [
                keep(left_by(second, blk * i), 0, small)
                + keep(pltpu.roll(target, small - blk * i, 1) if i < ITERS else target, small, order)
                for i in range(ITERS)
            ],
            axis=0,
        )
        rows_small = lax.broadcasted_iota(jnp.int32, (small, 1), 0)
        for k in range(0, small, 2):
            top, low = normal[k:k + 1], normal[k + 1:k + 2]
            top_k, top_l = wide(top[:, k:k + 1]), wide(top[:, k + 1:k + 2])
            low_k, low_l = wide(low[:, k:k + 1]), wide(low[:, k + 1:k + 2])
            inv_top = 1.0 / top_k
            ratio = low_k * inv_top
            inv_low = 1.0 / (low_l - ratio * top_l)
            second_row = (low - ratio * top) * inv_low
            first_row = (top - top_l * second_row) * inv_top
            pair = (rows_small == k) | (rows_small == k + 1)
            first_col = jnp.where(pair, 0.0, normal[:, k:k + 1])
            second_col = jnp.where(pair, 0.0, normal[:, k + 1:k + 2])
            rest = normal - first_col * first_row - second_col * second_row
            normal = jnp.where(
                rows_small == k, first_row, jnp.where(rows_small == k + 1, second_row, rest)
            )
        return normal

    normal = SC("solve", solve)

    def factor():
        lane32 = lax.broadcasted_iota(jnp.int32, (order, 128), 1)
        row32 = lax.broadcasted_iota(jnp.int32, (order, 128), 0)
        full = jnp.concatenate(
            [keep(left_by(moments, blk * i), 0, order) for i in range(ITERS + 1)], axis=0
        )
        full = full + jnp.where(lane32 == row32 + order, 1.0, 0.0)
        rows_full = lax.broadcasted_iota(jnp.int32, (order, 1), 0)
        for k in range(0, order, 2):
            top, low = full[k:k + 1], full[k + 1:k + 2]
            top_k, top_l = wide(top[:, k:k + 1]), wide(top[:, k + 1:k + 2])
            low_k, low_l = wide(low[:, k:k + 1]), wide(low[:, k + 1:k + 2])
            inv_top = 1.0 / top_k
            ratio = low_k * inv_top
            left_over = low - ratio * top
            second_row = left_over * (1.0 / (low_l - ratio * top_l))
            first_row = (top - top_l * second_row) * inv_top
            done = rows_full <= k + 1
            first_col = jnp.where(done, 0.0, full[:, k:k + 1])
            second_col = jnp.where(done, 0.0, full[:, k + 1:k + 2])
            rest = full - first_col * first_row - second_col * second_row
            full = jnp.where(rows_full == k + 1, left_over, rest)
        pivots = jnp.sum(jnp.where(lane32 == row32, full, 0.0), axis=1, keepdims=True)
        full = full / jnp.sqrt(pivots)
        upper = jnp.where((lane32 < order) & (lane32 >= row32), full, 0.0)
        lower_inv = left_by(full, order)
        lower_inv = jnp.where(lane32 < small, lower_inv, 0.0)[:small]
        hess = inv * nt_dot(pltpu.roll(lower_inv, blk, 1), upper)
        row_h = lax.broadcasted_iota(jnp.int32, (small, order), 0)
        col_h = lax.broadcasted_iota(jnp.int32, (small, order), 1)
        hess = hess + jnp.where(row_h == col_h, CENTRE, 0.0)
        hess_ref[...] = jnp.where(col_h // blk <= row_h // blk + 1, hess, 0.0)

    def spread():
        for k in range(small):
            for u in range(blk):
                splat[k * blk + u] = jnp.broadcast_to(
                    normal[k:k + 1, small + u:small + u + 1], (8, 128)
                )

    SC("splat", spread)

    def combine(dst, first_layer, count, row_start, height, sources):
        tiles = height // 8

        def run(i, carry):
            layer, t = first_layer + i // tiles, i % tiles
            at = pl.multiple_of(row_start + t * 8, 8)
            for lane_at in range(lanes):
                cols = pl.ds(lane_at * 128, 128)
                vals = []
                for ref, l_at, base in sources:
                    first_row = pl.multiple_of(base + t * 8, 8)
                    vals += [
                        ref[v, pl.ds(first_row, 8), cols] if l_at is None
                        else ref[v, l_at + layer, pl.ds(first_row, 8), cols]
                        for v in range(blk)
                    ]
                for u in range(blk):
                    total = splat[u] * vals[0]
                    for k in range(1, small):
                        total = total + splat[k * blk + u] * vals[k]
                    dst[u, layer, pl.ds(at, 8), cols] = total
            return carry

        lax.fori_loop(0, count * tiles, run, 0)

    def send_late():
        for layer in range(lay):
            for first in range(0, late[layer], 8):
                combine(
                    held, layer, 1, first, 8,
                    [
                        (k, 1 + theirs_at, theirs_out + early[layer] + first)
                        for k in basis[:ITERS]
                    ],
                )
                late_copy(layer, hs + theirs_out, first, 8).start()

    SC("comb_late", send_late)
    SC("deepen#1", lambda: deepen(1))
    SC("comb_own", lambda: combine(
        out_ref, 0, lay, hs, half, ((r_ref, 0, hs), (k1, 1 + mine_at, 0), (k2, 1 + mine_at, 0))
    ))
    SC("deepen#2", lambda: deepen(2))

    def back_wait():
        for layer in range(lay):
            all_back(layer).wait()

    SC("back_wait", back_wait)

    def rest():
        for layer in range(lay):
            combine(
                out_ref, layer, 1, os + mine_out, early[layer],
                (
                    (r_ref, 0, os + mine_out),
                    (ret.at[0, layer], None, 0), (ret.at[1, layer], None, 0),
                ),
            )

    SC("comb_other", rest)
    SC("deepen#3", lambda: deepen(3))
    SC("factor", factor)
    SC("deepen#4", lambda: deepen(4))

    def finish_inner():
        for slot, layer in ((0, far), (1, near_l)):
            combine(
                out_ref, layer, 1, inner_at, inner,
                ((r_ref, 0, inner_at), (kd1.at[slot], None, 0), (kd2.at[slot], None, 0)),
            )

    SC("comb_inner", finish_inner)

    def drain():
        whole = r_ref.at[:, :, pl.ds(os, half)]
        remote(whole, whole, x_s, x_r.at[0, 0], (partner, gy)).wait_send()
        for direction, there in ((0, below), (1, above)):
            @pl.when(there)
            def _():
                every = k0.at[:, pl.ds(0, ITERS)]
                remote(
                    every, every, z_s.at[direction], z_r.at[0, direction, 0], (partner, gy)
                ).wait_send()

        for side, there in ((0, before), (1, after)):
            first = has(0, side)

            @pl.when(first)
            def _():
                every = ys.at[:, side]
                remote(every, every, y_s.at[side], y_r.at[0, side, 0], (partner, gy)).wait_send()

            @pl.when(there & jnp.logical_not(first))
            def _():
                every = ys.at[pl.ds(1, ITERS - 1), side]
                remote(every, every, y_s.at[side], y_r.at[0, side, 0], (partner, gy)).wait_send()

        diag_copy.wait_send()
        every = deep.at[pl.ds(2, 2)]
        remote(every, every, q_s, q_r.at[0], (partner, gy)).wait_send()
        ghost_copies[0].wait_send()
        ghost_diag.wait_send()

        @pl.when(onward)
        def _():
            remote(every, every, qz_s, qz_r.at[0], (partner, gy)).wait_send()
            for copy in ghost_relays:
                copy.wait_send()

    SC("drain", drain)

    def late_wait():
        for layer in range(lay):
            late_copy(layer, hs + theirs_out, 0, late[layer]).wait_send()
            late_copy(layer, os + mine_out, 0, late[layer]).wait_recv()

    SC("late_wait", late_wait)


def store(x_ref, h_ref, x_out, h_out, sems):
    copies = (
        pltpu.make_async_copy(x_ref, x_out, sems.at[0]),
        pltpu.make_async_copy(h_ref, h_out, sems.at[1]),
    )
    for copy in copies:
        copy.start()
    for copy in copies:
        copy.wait()


def body(right_side, diagonal):
    blk, lay, rows, nx = right_side.shape
    half, group_lay = rows // 2, 2 * lay
    inner = half // 2
    outer = half - inner
    early = [outer * EARLY[layer % len(EARLY)] // 16 * 8 for layer in range(lay)]
    n_z, n_y = lax.axis_size("gz"), lax.axis_size("gy")
    vmem = lambda *shape: pltpu.VMEM(shape, jnp.float32)
    dma = lambda *shape: pltpu.SemaphoreType.DMA(shape) if shape else pltpu.SemaphoreType.DMA
    small, order = ITERS * blk, (ITERS + 1) * blk
    in_hbm = lambda x: pltpu.with_memory_space_constraint(x, pltpu.HBM)
    x, h = pl.pallas_call(
        kernel,
        out_shape=(vmem(*right_side.shape), vmem(small, order)),
        in_specs=[pl.BlockSpec(memory_space=pltpu.HBM)] * 2,
        out_specs=(pl.BlockSpec(memory_space=pltpu.VMEM),) * 2,
        scratch_shapes=[
            vmem(*right_side.shape),
            vmem(*diagonal.shape),
            vmem(blk, group_lay + 2, half, nx),
            vmem(blk, group_lay + 2, half, nx),
            vmem(blk, group_lay + 2, half, nx),
            vmem(blk, group_lay, half, nx),
            vmem(group_lay, half, nx),
            vmem(ITERS - 1, lay, blk, max(early), nx),
            vmem(blk, lay, outer - min(early), nx),
            vmem(ITERS, 2, blk, group_lay, nx),
            vmem(ITERS, 2, blk, group_lay, nx),
            vmem(blk, lay, 1, nx),
            vmem(blk, lay, 1, nx),
            vmem(4, blk, inner, nx),
            vmem(3, inner, nx),
            vmem(blk, 2, 1, nx),
            vmem(blk, 3, 1, nx),
            vmem(2, blk, inner, nx),
            vmem(2, blk, inner, nx),
            vmem(8 * blk * blk, 128),
            vmem(4, 128),
            vmem(n_z * n_y, 4, 128),
            vmem(small * blk, 8, 128),
            dma(CHUNKS + 1), pltpu.SemaphoreType.REGULAR((4,)),
            dma(), dma(2, CHUNKS),
            dma(), dma(),
            dma(2), dma(2, 2, CHUNKS),
            dma(2), dma(2, 2, CHUNKS),
            dma(), dma(),
            dma(lay), dma(lay), dma(lay), dma(lay),
            dma(), dma(),
            dma(), dma(CHUNKS), dma(), dma(CHUNKS), dma(4), dma(4),
        ],
        compiler_params=pltpu.CompilerParams(
            collective_id=0, has_side_effects=True, vmem_limit_bytes=40 * 1024 * 1024
        ),
        name="gmres",
    )(in_hbm(right_side), in_hbm(diagonal))
    in_vmem = lambda x: pltpu.with_memory_space_constraint(x, pltpu.VMEM)
    return pl.pallas_call(
        store,
        out_shape=(
            jax.ShapeDtypeStruct(x.shape, jnp.float32), jax.ShapeDtypeStruct(h.shape, jnp.float32),
        ),
        in_specs=[pl.BlockSpec(memory_space=pltpu.VMEM)] * 2,
        out_specs=(pl.BlockSpec(memory_space=pltpu.HBM),) * 2,
        scratch_shapes=[dma(2)],
        compiler_params=pltpu.CompilerParams(vmem_limit_bytes=4 * 1024 * 1024),
        name="store",
    )(in_vmem(x), in_vmem(h))


def solution(mesh):
    in_specs = (P(None, "gz", "gy", None), P("gz", "gy", None))
    out_specs = (P(None, "gz", "gy", None), P())
    return jax.shard_map(body, mesh=mesh, in_specs=in_specs, out_specs=out_specs, check_vma=False)
```

```python
import functools

import jax
import jax.numpy as jnp
from jax import lax
from jax.experimental import pallas as pl
from jax.experimental.pallas import tpu as pltpu
from jax.sharding import PartitionSpec as P

ITERS = 3
CENTRE = 7.5
SCALE = 0.25
CUTS = (0, 1, 3, 5, 7, 8)
CHUNKS = len(CUTS) - 1
EARLY = (1, 1)
BACK = {
    (0, 1): ("ghost",), (0, 2): ((0, 0),), (0, 3): ((0, 1),), (0, 4): ((0, 2),), (1, 1): ((0, 3),),
    (1, 4): ((0, 4), (1, 0)), (2, 0): ((1, 1),), (2, 1): ((1, 2),),
    "reduce": ((1, 3), (1, 4), (2, 0), (2, 1), (2, 2), (2, 3), (2, 4)),
}
RELAY = {(2, 1): (0,), "reduce": (1, 2, 3, 4)}
MESH = pl.DeviceIdType.MESH
HIGH = lax.Precision.HIGHEST


def SC(name, f):
    with jax.named_scope(name):
        return f()


def nt_dot(left, right):
    return lax.dot_general(
        left, right, (((1,), (1,)), ((), ())), precision=HIGH, preferred_element_type=jnp.float32
    )


def dot(left, right):
    return jnp.dot(left, right, precision=HIGH, preferred_element_type=jnp.float32)


def kernel(
    r_hbm, d_hbm, out_ref, hess_ref,
    r_ref, d_ref, k0, k1, k2, k3, diag, ret, held, ys, yh, rows_out, rows_in,
    deep, d_deep, g_out, g_in, kd1, kd2,
    acc, mine, slots, splat, i_s, met,
    x_s, x_r, d_s, d_r, z_s, z_r, y_s, y_r, e_s, e_r, b_s, b_r, l_s, l_r, g_s, g_r,
    q_s, q_r, qz_s, qz_r, w_s, w_r,
):
    blk, lay, rows, nx = r_ref.shape
    half, group_lay = rows // 2, 2 * lay
    starts = [blk * cut // CUTS[-1] for cut in CUTS]
    part = lambda ch: pl.ds(starts[ch], starts[ch + 1] - starts[ch])
    n_z, n_y = lax.axis_size("gz"), lax.axis_size("gy")
    gz, gy = lax.axis_index("gz"), lax.axis_index("gy")
    n_dev = n_z * n_y
    me = gz * n_y + gy
    p, group = gz % 2, gz // 2
    h = (p + gy) % 2
    partner = gz + 1 - 2 * p
    hs = pl.multiple_of(h * half, half)
    os = pl.multiple_of((1 - h) * half, half)
    mine_at = p * lay
    theirs_at = (1 - p) * lay
    below, above = group > 0, group < n_z // 2 - 1
    place = 2 * gy + h
    before, after = place > 0, place < 2 * n_y - 1
    prev_dev = (gz + h * (partner - gz), gy - (1 - h))
    next_dev = (gz + (1 - h) * (partner - gz), gy + h)
    basis = (k0, k1, k2, k3)
    edge = (lay - 1) * p
    inner = half // 2
    outer = half - inner
    early = [outer * EARLY[layer % len(EARLY)] // 16 * 8 for layer in range(lay)]
    late = [outer - e for e in early]
    theirs_out = pl.multiple_of(h * inner, 8)
    mine_out = pl.multiple_of((1 - h) * inner, 8)
    inner_at = pl.multiple_of(os + h * outer, 8)
    far, near_l = (lay - 1) * p, (lay - 1) * (1 - p)
    beyond = jnp.where(p == 0, below, above)
    onward = jnp.where(p == 0, above, below)
    onward_dev = (gz + 2 - 4 * p, gy)

    def remote(src, dst, send, recv, dev):
        return pltpu.make_async_remote_copy(
            src_ref=src, dst_ref=dst, send_sem=send, recv_sem=recv, device_id=dev,
            device_id_type=MESH,
        )

    def device(i):
        return (i // n_y, i % n_y)

    def load_r(ch):
        vs = part(ch)
        return pltpu.make_async_copy(r_hbm.at[vs], r_ref.at[vs], i_s.at[ch])

    load_d = pltpu.make_async_copy(d_hbm, d_ref, i_s.at[CHUNKS])
    for ch in range(CHUNKS):
        load_r(ch).start()
    load_d.start()

    def signal(semaphore, dev):
        pl.semaphore_signal(semaphore, inc=1, device_id=dev, device_id_type=MESH)

    barrier = pltpu.get_barrier_semaphore()
    left, right = gy > 0, gy < n_y - 1
    sides = (
        (below, (gz - 2, gy)), (above, (gz + 2, gy)), (left, (gz, gy - 1)), (right, (gz, gy + 1)),
    )
    signal(barrier, (partner, gy))
    for there, dev in sides:
        @pl.when(there)
        def _():
            signal(barrier, dev)

    def wave(which):
        there, back = sides[which], sides[which ^ 1]

        @pl.when(back[0])
        def _():
            pl.semaphore_wait(met.at[which], 1)

        @pl.when(there[0])
        def _():
            signal(met.at[which], there[1])

    @pl.when(jnp.logical_not(below))
    def _():
        for k in (k0, k1, k2):
            k[:, 0] = jnp.zeros((blk, half, nx), jnp.float32)

    @pl.when(jnp.logical_not(above))
    def _():
        for k in (k0, k1, k2):
            k[:, group_lay + 1] = jnp.zeros((blk, half, nx), jnp.float32)

    @pl.when(jnp.logical_not(before))
    def _():
        yh[:, 0] = jnp.zeros((ITERS,) + yh.shape[2:], jnp.float32)

    @pl.when(jnp.logical_not(after))
    def _():
        yh[:, 1] = jnp.zeros((ITERS,) + yh.shape[2:], jnp.float32)

    @pl.when(jnp.logical_not(beyond))
    def _():
        deep[0:2] = jnp.zeros((2,) + deep.shape[1:], jnp.float32)
        d_deep[0] = jnp.zeros(d_deep.shape[1:], jnp.float32)
        g_in[:, 0] = jnp.zeros((blk, 1, nx), jnp.float32)

    load_r(0).wait()
    SC("barrier", lambda: pl.semaphore_wait(
        barrier, 1 + sum(jnp.where(there, 1, 0) for there, _ in sides)
    ))
    rows_copy = remote(rows_out, rows_in, e_s, e_r, (partner, gy))

    def exchange(which, ch):
        layer = edge + which * (1 - 2 * p)
        vs = part(ch)
        return remote(
            r_ref.at[vs, pl.ds(layer, 1), pl.ds(os, half)],
            k0.at[vs, pl.ds(1 + mine_at + layer, 1)],
            x_s, x_r.at[which, ch], (partner, gy),
        )

    def z_from_rhs(ch, direction):
        vs = part(ch)
        if direction == 0:
            dst, dev = k0.at[vs, pl.ds(group_lay + 1, 1)], (gz - 2, gy)
        else:
            dst, dev = k0.at[vs, pl.ds(0, 1)], (gz + 2, gy)
        return remote(
            r_ref.at[vs, pl.ds(edge, 1), pl.ds(hs, half)], dst,
            z_s.at[direction], z_r.at[0, ch], dev,
        )

    def z_copy(j, ch, direction):
        vs = part(ch)
        k = basis[j]
        if direction == 0:
            src, dst, dev = k.at[vs, pl.ds(1, 1)], k.at[vs, pl.ds(group_lay + 1, 1)], (gz - 2, gy)
        else:
            src, dst, dev = k.at[vs, pl.ds(group_lay, 1)], k.at[vs, pl.ds(0, 1)], (gz + 2, gy)
        return remote(src, dst, z_s.at[direction], z_r.at[j % 2, ch], dev)

    def y_copy(j, ch, side):
        vs = part(ch)
        dev = prev_dev if side == 0 else next_dev
        return remote(
            ys.at[j, side, vs], yh.at[j, 1 - side, vs],
            y_s.at[side], y_r.at[j % 2, ch], dev,
        )

    def has(j, side):
        if side == 0:
            return before if j else before & (h == 0)
        return after if j else after & (h == 1)

    def back_copy(j, ch):
        vs = part(ch)
        return [
            remote(
                basis[j].at[vs, 1 + theirs_at + layer, pl.ds(theirs_out, early[layer])],
                ret.at[j - 1, layer, vs, pl.ds(0, early[layer])],
                b_s.at[layer], b_r.at[layer], (partner, gy),
            )
            for layer in range(lay)
        ]

    def all_back(layer):
        every = ret.at[:, layer, :, pl.ds(0, early[layer])]
        return remote(every, every, b_s.at[layer], b_r.at[layer], (partner, gy))

    def late_copy(layer, at, first, count):
        return remote(
            held.at[:, pl.ds(layer, 1), pl.ds(first, count)],
            out_ref.at[
                :, pl.ds(layer, 1), pl.ds(pl.multiple_of(at + early[layer] + first, 8), count)
            ],
            l_s.at[layer], l_r.at[layer], (partner, gy),
        )

    give_at = pl.multiple_of(hs + (1 - h) * outer, 8)

    def deep_copy(ch):
        vs = part(ch)
        return [
            remote(
                r_ref.at[vs, layer, pl.ds(give_at, inner)], deep.at[slot, vs],
                q_s, q_r.at[ch], (partner, gy),
            )
            for slot, layer in ((2, near_l), (3, far))
        ]

    def deep_recv(ch):
        every = deep.at[pl.ds(2, 2), part(ch)]
        return remote(every, every, q_s, q_r.at[ch], (partner, gy))

    def deep_relay(ch):
        vs = part(ch)
        return remote(
            deep.at[pl.ds(2, 2), vs], deep.at[pl.ds(0, 2), vs], qz_s, qz_r.at[ch], onward_dev
        )

    ghost_copies = [
        remote(g_out, g_in.at[:, pl.ds(1, 2)], w_s.at[0], w_r.at[0], (partner, gy))
    ] + [
        remote(
            d_ref.at[layer, pl.ds(give_at, inner)], d_deep.at[slot], w_s.at[1], w_r.at[1],
            (partner, gy),
        )
        for slot, layer in ((1, near_l), (2, far))
    ]
    both_diag = d_deep.at[pl.ds(1, 2)]
    ghost_diag = remote(both_diag, both_diag, w_s.at[1], w_r.at[1], (partner, gy))
    ghost_relays = (
        remote(g_in.at[:, pl.ds(2, 1)], g_in.at[:, pl.ds(0, 1)], w_s.at[2], w_r.at[2], onward_dev),
        remote(d_deep.at[pl.ds(2, 1)], d_deep.at[pl.ds(0, 1)], w_s.at[3], w_r.at[3], onward_dev),
    )

    def issue(items):
        for item in items:
            if item == "ghost":
                copies = ghost_copies
            else:
                copies = back_copy(*item) if item[0] else deep_copy(item[1])
            for copy in copies:
                copy.start()

    def relay_deep(ch):
        deep_recv(ch).wait_recv()
        if ch == 0:
            ghost_copies[0].wait_recv()
            ghost_diag.wait_recv()

        @pl.when(onward)
        def _():
            deep_relay(ch).start()
            if ch == 0:
                for copy in ghost_relays:
                    copy.start()

    diag_copy = remote(
        d_ref.at[:, pl.ds(os, half)], diag.at[pl.ds(mine_at, lay)], d_s, d_r, (partner, gy)
    )

    for ch in range(CHUNKS):
        if ch:
            load_r(ch).wait()
        exchange(0, ch).start()

        @pl.when((p == 0) & below)
        def _():
            z_from_rhs(ch, 0).start()

        @pl.when((p == 1) & above)
        def _():
            z_from_rhs(ch, 1).start()

    for v in range(blk):
        rows_out[v, :lay] = jnp.where(
            h == 0, r_ref[v, :, half - 1:half], r_ref[v, :, half:half + 1]
        )
        rows_out[v, lay] = jnp.where(
            h == 0, r_ref[v, near_l, rows - 1:rows], r_ref[v, near_l, 0:1]
        )
        for slot, layer in ((0, near_l), (1, far)):
            g_out[v, slot] = jnp.where(
                h == 0, r_ref[v, layer, outer - 1:outer], r_ref[v, layer, half + inner:half + inner + 1]
            )
    load_d.wait()
    rows_copy.start()
    diag_copy.start()
    for ch in range(CHUNKS):
        exchange(1, ch).start()

    def own(v, carry):
        k0[v, pl.ds(1 + mine_at, lay)] = r_ref[v, :, pl.ds(hs, half)]
        return carry

    lax.fori_loop(0, blk, own, 0)
    diag[pl.ds(mine_at, lay)] = d_ref[:, pl.ds(hs, half)]

    lanes = nx // 128

    def add_up(sums, tiles):
        def run(i, carry):
            layer, at = i // tiles, pl.multiple_of((i % tiles) * 8, 8)
            for lane in range(lanes):
                carry = sums(carry, layer, at, pl.ds(lane * 128, 128))
            return carry
        return run

    known = (2 * ITERS - 1) * blk * blk
    split = acc.shape[0] - 2 * blk * blk

    def keep_sum(moment, a, b, s):
        line = jnp.sum(s, axis=0, keepdims=True)
        first = moment * blk * blk + (split - known if moment >= 2 * ITERS - 1 else 0)
        at = first + a * blk + b
        acc[at:at + 1] = line
        if a != b:
            at = first + b * blk + a
            acc[at:at + 1] = line

    zero = jnp.zeros((8, 128), jnp.float32)

    def gram_rhs():
        pairs = [(a, b) for a in range(blk) for b in range(a, blk)]

        def body(sums, layer, at, cols):
            x = [r_ref[v, layer, pl.ds(at, 8), cols] for v in range(blk)]
            return tuple(s + x[a] * x[b] for s, (a, b) in zip(sums, pairs))

        sums = lax.fori_loop(
            0, lay * (rows // 8), add_up(body, rows // 8), (zero,) * len(pairs)
        )
        for s, (a, b) in zip(sums, pairs):
            keep_sum(0, a, b, s)

    def gram(j, ch):
        src, dst = basis[j], basis[j + 1]
        shift = 0 if j == ITERS - 1 else 1
        top = starts[ch + 1]
        pairs = [(a, b) for b in range(starts[ch], top) for a in range(b + 1)]

        def body(sums, layer, at, cols):
            x = [src[v, 1 + layer, pl.ds(at, 8), cols] for v in range(top)]
            y = [dst[v, shift + layer, pl.ds(at, 8), cols] for v in range(top)]
            first, second = sums[:len(pairs)], sums[len(pairs):]
            first = tuple(s + x[a] * y[b] for s, (a, b) in zip(first, pairs))
            second = tuple(s + y[a] * y[b] for s, (a, b) in zip(second, pairs))
            return first + second

        sums = lax.fori_loop(
            0, group_lay * (half // 8), add_up(body, half // 8), (zero,) * (2 * len(pairs))
        )
        for i, (a, b) in enumerate(pairs):
            keep_sum(2 * j + 1, a, b, sums[i])
            keep_sum(2 * j + 2, a, b, sums[len(pairs) + i])

    acc[known:split] = jnp.zeros((split - known, 128), jnp.float32)
    SC("gram0", gram_rhs)

    def relay(ch):
        remote(
            r_ref.at[part(ch), pl.ds(0, 1), pl.ds(os, half)],
            k0.at[part(ch), pl.ds(1 + (group_lay - 1) * (1 - p), 1)],
            x_s, x_r.at[0, ch], (partner, gy),
        ).wait_recv()

        @pl.when((p == 0) & above)
        def _():
            z_copy(0, ch, 1).start()

        @pl.when((p == 1) & below)
        def _():
            z_copy(0, ch, 0).start()

    def stage_rows(j, v, layer, value):
        ys[j, 0, v, layer:layer + 1] = value[:1]
        ys[j, 1, v, layer:layer + 1] = value[half - 1:]

    def start_rows(j, ch):
        for side in range(2):
            @pl.when(has(j, side))
            def _():
                y_copy(j, ch, side).start()

    def arrived(ch):
        remote(
            r_ref.at[part(ch), pl.ds(0, 1), pl.ds(os, half)],
            k0.at[part(ch), pl.ds(1 + lay - p, 1)],
            x_s, x_r.at[1, ch], (partner, gy),
        ).wait_recv()

    for ch in range(CHUNKS):
        if ch < len(sides):
            SC(f"wave#{ch}", lambda: wave(ch))
        SC(f"relay#{ch}", lambda: relay(ch))

    def rows_arrived():
        rows_copy.wait()
        for v in range(blk):
            near = jnp.where(
                h == 0, r_ref[v, :, half:half + 1], r_ref[v, :, half - 1:half]
            ).reshape(lay, nx)
            own_row = jnp.where(
                h == 0, r_ref[v, :, 0:1], r_ref[v, :, rows - 1:rows]
            ).reshape(lay, nx)
            both = lambda own, other: jnp.where(
                p == 0,
                jnp.concatenate([own, other], axis=0),
                jnp.concatenate([other, own], axis=0),
            )
            yh[0, 1 - h, v] = both(near, rows_in[v, :lay].reshape(lay, nx))
            last = 1 + (group_lay - 1) * (1 - p)
            edge_row = jnp.where(h == 0, k0[v, last, 0:1], k0[v, last, half - 1:half])
            next_row = rows_in[v, lay]
            ys[0, h, v] = both(own_row, jnp.where(
                p == 0,
                jnp.concatenate([next_row, edge_row], axis=0),
                jnp.concatenate([edge_row, next_row], axis=0),
            ))
        for ch in range(CHUNKS):
            start_rows(0, ch)
        remote(
            d_ref.at[:, pl.ds(os, half)], diag.at[pl.ds(theirs_at, lay)], d_s, d_r, (partner, gy)
        ).wait_recv()

    SC("rows_diag", rows_arrived)

    row_at = lax.broadcasted_iota(jnp.int32, (half, nx), 0)
    col_at = lax.broadcasted_iota(jnp.int32, (half, nx), 1)

    def apply(j, ch):
        src, dst = basis[j], basis[j + 1]
        shift = 0 if j == ITERS - 1 else 1
        vs = part(ch)

        def take(there, every, semaphore):
            for count in (1, 2):
                @pl.when(there[0].astype(jnp.int32) + there[1].astype(jnp.int32) == count)
                def _():
                    ref = every(count)
                    remote(ref, ref, z_s.at[0], semaphore, (partner, gy)).wait_recv()

        def waits():
            take((below, above), lambda n: src.at[vs, pl.ds(0, n)], z_r.at[j % 2, ch])

        def row_waits():
            take((has(j, 0), has(j, 1)), lambda n: yh.at[j, pl.ds(0, n), vs], y_r.at[j % 2, ch])

        for which in RELAY.get((j, ch), ()):
            SC(f"drelay#{which}", lambda: relay_deep(which))
        SC(f"z_wait{j}#{ch}", waits)
        SC(f"y_wait{j}#{ch}", row_waits)

        def run(v, carry):
            for layer in range(group_lay):
                here = src[v, 1 + layer]
                near = src[v, layer] + src[v, 2 + layer]
                up = jnp.where(
                    row_at == 0, yh[j, 0, v, layer:layer + 1], pltpu.roll(here, 1, 0)
                )
                down = jnp.where(
                    row_at == half - 1, yh[j, 1, v, layer:layer + 1],
                    pltpu.roll(here, half - 1, 0),
                )
                left = jnp.where(col_at == 0, 0.0, pltpu.roll(here, 1, 1))
                right = jnp.where(col_at == nx - 1, 0.0, pltpu.roll(here, nx - 1, 1))
                near = near + (up + down) + (left + right)
                centre = (6.0 - CENTRE) + diag[layer]
                value = SCALE * (centre * here - near)
                dst[v, shift + layer] = value
                if j < ITERS - 1:
                    stage_rows(j + 1, v, layer, value)
            return carry

        SC(f"apply{j}#{ch}", lambda: lax.fori_loop(starts[ch], starts[ch + 1], run, 0))
        if j < ITERS - 1:
            @pl.when(below)
            def _():
                z_copy(j + 1, ch, 0).start()

            @pl.when(above)
            def _():
                z_copy(j + 1, ch, 1).start()

            start_rows(j + 1, ch)
        issue(BACK.get((j, ch), ()))
        SC(f"gram{j}#{ch}", lambda: gram(j, ch))

    def gather(first, last, skip):
        count = last - first
        sums = nt_dot(jnp.ones((8, 128), jnp.float32), acc[first:last])
        lane_q = lax.broadcasted_iota(jnp.int32, (8, count), 1)
        row_q = lax.broadcasted_iota(jnp.int32, (8, count), 0)
        q = lax.broadcasted_iota(jnp.int32, (count, 128), 0) + (first - skip)
        c = lax.broadcasted_iota(jnp.int32, (count, 128), 1)
        pick = (q // (blk * blk) == c // blk) & (q % blk == c % blk)
        kept = jnp.where((lane_q // blk) % blk == row_q, sums, 0.0)
        return dot(kept, jnp.where(pick, 1.0, 0.0))

    row_d = lax.broadcasted_iota(jnp.int32, (inner, nx), 0)
    col_d = lax.broadcasted_iota(jnp.int32, (inner, nx), 1)

    def sideways(here, col):
        return jnp.where(col == 0, 0.0, pltpu.roll(here, 1, 1)) + jnp.where(
            col == nx - 1, 0.0, pltpu.roll(here, nx - 1, 1)
        )

    def deepen(ch):
        @pl.when(beyond)
        def _():
            every = deep.at[pl.ds(0, 2), part(ch)]
            remote(every, every, qz_s, qz_r.at[ch], (partner, gy)).wait_recv()
            if ch == 0:
                for slot, ref in ((2, g_in.at[:, pl.ds(0, 1)]), (3, d_deep.at[pl.ds(0, 1)])):
                    remote(ref, ref, w_s.at[slot], w_r.at[slot], (partner, gy)).wait_recv()

        edge_of = lambda ref, v, slot: jnp.where(
            h == 0, ref[v, slot, half - 1:half], ref[v, slot, 0:1]
        )
        ghost_of = lambda row: jnp.where(
            h == 0, row(half + inner), row(outer - 1)
        )
        after_of = lambda row: jnp.where(
            h == 0, row(half + inner + 1), row(outer - 2)
        )
        slots = {
            "beyond": (group_lay + 1) * p, "far": 1 + (group_lay - 1) * p,
            "near": lay + p, "next": lay + 1 - p,
        }
        d_far, d_near = d_ref[far, pl.ds(inner_at, inner)], d_ref[near_l, pl.ds(inner_at, inner)]
        g_far = ghost_of(lambda i: d_ref[far, i:i + 1])
        g_near = ghost_of(lambda i: d_ref[near_l, i:i + 1])
        exists = jnp.where(beyond, 1.0, 0.0)
        one_col = lax.broadcasted_iota(jnp.int32, (1, nx), 1)

        def block(here, below_z, above_z, edge_row, ghost_row, extra):
            up = jnp.where(
                row_d == 0, jnp.where(h == 0, edge_row, ghost_row), pltpu.roll(here, 1, 0)
            )
            down = jnp.where(
                row_d == inner - 1, jnp.where(h == 0, ghost_row, edge_row),
                pltpu.roll(here, inner - 1, 0),
            )
            near = (below_z + above_z) + (up + down) + sideways(here, col_d)
            return SCALE * (((6.0 - CENTRE) + extra) * here - near)

        def run(v, carry):
            r_far = r_ref[v, far, pl.ds(inner_at, inner)]
            r_near = r_ref[v, near_l, pl.ds(inner_at, inner)]
            two, one, nxt, last = deep[0, v], deep[1, v], deep[2, v], deep[3, v]
            ghost_far = ghost_of(lambda i: r_ref[v, far, i:i + 1])
            ghost_near = ghost_of(lambda i: r_ref[v, near_l, i:i + 1])
            ghost_one, ghost_next = g_in[v, 0], g_in[v, 1]
            rows_of = lambda which: edge_of(k0, v, slots[which])
            k_one = exists * block(one, two, r_far, rows_of("beyond"), ghost_one, d_deep[0])
            k_far = block(r_far, one, r_near, rows_of("far"), ghost_far, d_far)
            k_near = block(r_near, r_far, nxt, rows_of("near"), ghost_near, d_near)
            k_next = block(nxt, r_near, last, rows_of("next"), ghost_next, d_deep[1])

            def line(here, inside, layer, beside, extra):
                outside = after_of(lambda i: r_ref[v, layer, i:i + 1])
                within = jnp.where(h == 0, inside[inner - 1:inner], inside[0:1])
                near = beside + (outside + within) + sideways(here, one_col)
                return SCALE * (((6.0 - CENTRE) + extra) * here - near)

            line_far = line(ghost_far, r_far, far, ghost_one + ghost_near, g_far)
            line_near = line(ghost_near, r_near, near_l, ghost_far + ghost_next, g_near)
            kd1[0, v], kd1[1, v] = k_far, k_near
            kd2[0, v] = block(
                k_far, k_one, k_near, edge_of(k1, v, slots["far"]), line_far, d_far
            )
            kd2[1, v] = block(
                k_near, k_far, k_next, edge_of(k1, v, slots["near"]), line_near, d_near
            )
            return carry

        lax.fori_loop(starts[ch], starts[ch + 1], run, 0)

    for ch in range(CHUNKS):
        SC(f"arrived#{ch}", lambda: arrived(ch))
        apply(0, ch)
    for ch in range(CHUNKS):
        apply(1, ch)

    def early_sums():
        local = gather(0, split, 0)
        mine[...] = local[:4] + pltpu.roll(local, 64, 1)[4:]

    SC("early_sums", early_sums)
    for ch in range(CHUNKS):
        apply(2, ch)

    def reduce():
        lane_s = lax.broadcasted_iota(jnp.int32, (8, 128), 1)
        local = jnp.zeros((8, 128), jnp.float32)
        for i in range(2 * blk):
            column = jnp.sum(acc[split + i * blk:split + (i + 1) * blk], axis=1, keepdims=True)
            local = local + jnp.where(lane_s == known // blk + i, column, 0.0)
        packed = mine[...] + local[:4] + pltpu.roll(local, 64, 1)[4:]
        mine[...] = packed
        slots[me] = packed

        def send(off, carry):
            to = (me + off) % n_dev
            remote(mine, slots.at[me], g_s, g_r, device(to)).start()
            return carry

        lax.fori_loop(1, n_dev, send, 0)
        issue(BACK.get("reduce", ()))
        for which in RELAY.get("reduce", ()):
            relay_deep(which)

    SC("red_send", reduce)

    def collect():
        others = slots.at[pl.ds(0, n_dev - 1)]
        remote(others, others, g_s, g_r, (partner, gy)).wait()

    SC("deepen#0", lambda: deepen(0))
    SC("red_wait", collect)
    packed = jnp.sum(slots[...], axis=0)

    lane = lax.broadcasted_iota(jnp.int32, (8, 128), 1)
    keep = lambda x, low, high: jnp.where((lane >= low) & (lane < high), x, 0.0)
    left_by = lambda x, n: x if n == 0 else pltpu.roll(x, 128 - n, 1)
    moments = keep(
        jnp.concatenate([packed, pltpu.roll(packed, 64, 1)], axis=0), 0, 64
    )
    small, order = ITERS * blk, (ITERS + 1) * blk
    inv = 1.0 / SCALE

    wide = lambda x: jnp.broadcast_to(x, (1, 128))

    def solve():
        second = (
            (inv * inv) * left_by(moments, 2 * blk)
            + (2.0 * CENTRE * inv) * left_by(moments, blk)
            + (CENTRE * CENTRE) * moments
        )
        target = inv * left_by(moments, blk) + CENTRE * moments
        normal = jnp.concatenate(
            [
                keep(left_by(second, blk * i), 0, small)
                + keep(pltpu.roll(target, small - blk * i, 1) if i < ITERS else target, small, order)
                for i in range(ITERS)
            ],
            axis=0,
        )
        rows_small = lax.broadcasted_iota(jnp.int32, (small, 1), 0)
        for k in range(0, small, 2):
            top, low = normal[k:k + 1], normal[k + 1:k + 2]
            top_k, top_l = wide(top[:, k:k + 1]), wide(top[:, k + 1:k + 2])
            low_k, low_l = wide(low[:, k:k + 1]), wide(low[:, k + 1:k + 2])
            inv_top = 1.0 / top_k
            ratio = low_k * inv_top
            inv_low = 1.0 / (low_l - ratio * top_l)
            second_row = (low - ratio * top) * inv_low
            first_row = (top - top_l * second_row) * inv_top
            pair = (rows_small == k) | (rows_small == k + 1)
            first_col = jnp.where(pair, 0.0, normal[:, k:k + 1])
            second_col = jnp.where(pair, 0.0, normal[:, k + 1:k + 2])
            rest = normal - first_col * first_row - second_col * second_row
            normal = jnp.where(
                rows_small == k, first_row, jnp.where(rows_small == k + 1, second_row, rest)
            )
        return normal

    normal = SC("solve", solve)

    def factor():
        lane32 = lax.broadcasted_iota(jnp.int32, (order, 128), 1)
        row32 = lax.broadcasted_iota(jnp.int32, (order, 128), 0)
        full = jnp.concatenate(
            [keep(left_by(moments, blk * i), 0, order) for i in range(ITERS + 1)], axis=0
        )
        full = full + jnp.where(lane32 == row32 + order, 1.0, 0.0)
        rows_full = lax.broadcasted_iota(jnp.int32, (order, 1), 0)
        for k in range(0, order, 2):
            top, low = full[k:k + 1], full[k + 1:k + 2]
            top_k, top_l = wide(top[:, k:k + 1]), wide(top[:, k + 1:k + 2])
            low_k, low_l = wide(low[:, k:k + 1]), wide(low[:, k + 1:k + 2])
            inv_top = 1.0 / top_k
            ratio = low_k * inv_top
            left_over = low - ratio * top
            second_row = left_over * (1.0 / (low_l - ratio * top_l))
            first_row = (top - top_l * second_row) * inv_top
            done = rows_full <= k + 1
            first_col = jnp.where(done, 0.0, full[:, k:k + 1])
            second_col = jnp.where(done, 0.0, full[:, k + 1:k + 2])
            rest = full - first_col * first_row - second_col * second_row
            full = jnp.where(rows_full == k + 1, left_over, rest)
        pivots = jnp.sum(jnp.where(lane32 == row32, full, 0.0), axis=1, keepdims=True)
        full = full / jnp.sqrt(pivots)
        upper = jnp.where((lane32 < order) & (lane32 >= row32), full, 0.0)
        lower_inv = left_by(full, order)
        lower_inv = jnp.where(lane32 < small, lower_inv, 0.0)[:small]
        hess = inv * nt_dot(pltpu.roll(lower_inv, blk, 1), upper)
        row_h = lax.broadcasted_iota(jnp.int32, (small, order), 0)
        col_h = lax.broadcasted_iota(jnp.int32, (small, order), 1)
        hess = hess + jnp.where(row_h == col_h, CENTRE, 0.0)
        hess_ref[...] = jnp.where(col_h // blk <= row_h // blk + 1, hess, 0.0)

    def spread():
        for k in range(small):
            for u in range(blk):
                splat[k * blk + u] = jnp.broadcast_to(
                    normal[k:k + 1, small + u:small + u + 1], (8, 128)
                )

    SC("splat", spread)

    def combine(dst, first_layer, count, row_start, height, sources):
        tiles = height // 8

        def run(i, carry):
            layer, t = first_layer + i // tiles, i % tiles
            at = pl.multiple_of(row_start + t * 8, 8)
            for lane_at in range(lanes):
                cols = pl.ds(lane_at * 128, 128)
                vals = []
                for ref, l_at, base in sources:
                    first_row = pl.multiple_of(base + t * 8, 8)
                    vals += [
                        ref[v, pl.ds(first_row, 8), cols] if l_at is None
                        else ref[v, l_at + layer, pl.ds(first_row, 8), cols]
                        for v in range(blk)
                    ]
                for u in range(blk):
                    total = splat[u] * vals[0]
                    for k in range(1, small):
                        total = total + splat[k * blk + u] * vals[k]
                    dst[u, layer, pl.ds(at, 8), cols] = total
            return carry

        lax.fori_loop(0, count * tiles, run, 0)

    def send_late():
        for layer in range(lay):
            for first in range(0, late[layer], 8):
                combine(
                    held, layer, 1, first, 8,
                    [
                        (k, 1 + theirs_at, theirs_out + early[layer] + first)
                        for k in basis[:ITERS]
                    ],
                )
                late_copy(layer, hs + theirs_out, first, 8).start()

    SC("comb_late", send_late)
    SC("deepen#1", lambda: deepen(1))
    SC("comb_own", lambda: combine(
        out_ref, 0, lay, hs, half, ((r_ref, 0, hs), (k1, 1 + mine_at, 0), (k2, 1 + mine_at, 0))
    ))
    SC("deepen#2", lambda: deepen(2))

    def back_wait():
        for layer in range(lay):
            all_back(layer).wait()

    SC("back_wait", back_wait)

    def rest():
        for layer in range(lay):
            combine(
                out_ref, layer, 1, os + mine_out, early[layer],
                (
                    (r_ref, 0, os + mine_out),
                    (ret.at[0, layer], None, 0), (ret.at[1, layer], None, 0),
                ),
            )

    SC("comb_other", rest)
    SC("deepen#3", lambda: deepen(3))
    SC("factor", factor)
    SC("deepen#4", lambda: deepen(4))

    def finish_inner():
        for slot, layer in ((0, far), (1, near_l)):
            combine(
                out_ref, layer, 1, inner_at, inner,
                ((r_ref, 0, inner_at), (kd1.at[slot], None, 0), (kd2.at[slot], None, 0)),
            )

    SC("comb_inner", finish_inner)

    def drain():
        whole = r_ref.at[:, :, pl.ds(os, half)]
        remote(whole, whole, x_s, x_r.at[0, 0], (partner, gy)).wait_send()
        for direction, there in ((0, below), (1, above)):
            @pl.when(there)
            def _():
                every = k0.at[:, pl.ds(0, ITERS)]
                remote(
                    every, every, z_s.at[direction], z_r.at[0, 0], (partner, gy)
                ).wait_send()

        for side, there in ((0, before), (1, after)):
            first = has(0, side)

            @pl.when(first)
            def _():
                every = ys.at[:, side]
                remote(every, every, y_s.at[side], y_r.at[0, 0], (partner, gy)).wait_send()

            @pl.when(there & jnp.logical_not(first))
            def _():
                every = ys.at[pl.ds(1, ITERS - 1), side]
                remote(every, every, y_s.at[side], y_r.at[0, 0], (partner, gy)).wait_send()

        diag_copy.wait_send()
        every = deep.at[pl.ds(2, 2)]
        remote(every, every, q_s, q_r.at[0], (partner, gy)).wait_send()
        ghost_copies[0].wait_send()
        ghost_diag.wait_send()

        @pl.when(onward)
        def _():
            remote(every, every, qz_s, qz_r.at[0], (partner, gy)).wait_send()
            for copy in ghost_relays:
                copy.wait_send()

    SC("drain", drain)

    def late_wait():
        for layer in range(lay):
            late_copy(layer, hs + theirs_out, 0, late[layer]).wait_send()
            late_copy(layer, os + mine_out, 0, late[layer]).wait_recv()

    SC("late_wait", late_wait)


def store(x_ref, h_ref, x_out, h_out, sems):
    copies = (
        pltpu.make_async_copy(x_ref, x_out, sems.at[0]),
        pltpu.make_async_copy(h_ref, h_out, sems.at[1]),
    )
    for copy in copies:
        copy.start()
    for copy in copies:
        copy.wait()


def body(right_side, diagonal):
    blk, lay, rows, nx = right_side.shape
    half, group_lay = rows // 2, 2 * lay
    inner = half // 2
    outer = half - inner
    early = [outer * EARLY[layer % len(EARLY)] // 16 * 8 for layer in range(lay)]
    n_z, n_y = lax.axis_size("gz"), lax.axis_size("gy")
    vmem = lambda *shape: pltpu.VMEM(shape, jnp.float32)
    dma = lambda *shape: pltpu.SemaphoreType.DMA(shape) if shape else pltpu.SemaphoreType.DMA
    small, order = ITERS * blk, (ITERS + 1) * blk
    in_hbm = lambda x: pltpu.with_memory_space_constraint(x, pltpu.HBM)
    x, h = pl.pallas_call(
        kernel,
        out_shape=(vmem(*right_side.shape), vmem(small, order)),
        in_specs=[pl.BlockSpec(memory_space=pltpu.HBM)] * 2,
        out_specs=(pl.BlockSpec(memory_space=pltpu.VMEM),) * 2,
        scratch_shapes=[
            vmem(*right_side.shape),
            vmem(*diagonal.shape),
            vmem(blk, group_lay + 2, half, nx),
            vmem(blk, group_lay + 2, half, nx),
            vmem(blk, group_lay + 2, half, nx),
            vmem(blk, group_lay, half, nx),
            vmem(group_lay, half, nx),
            vmem(ITERS - 1, lay, blk, max(early), nx),
            vmem(blk, lay, outer - min(early), nx),
            vmem(ITERS, 2, blk, group_lay, nx),
            vmem(ITERS, 2, blk, group_lay, nx),
            vmem(blk, lay + 1, 1, nx),
            vmem(blk, lay + 1, 1, nx),
            vmem(4, blk, inner, nx),
            vmem(3, inner, nx),
            vmem(blk, 2, 1, nx),
            vmem(blk, 3, 1, nx),
            vmem(2, blk, inner, nx),
            vmem(2, blk, inner, nx),
            vmem(8 * blk * blk, 128),
            vmem(4, 128),
            vmem(n_z * n_y, 4, 128),
            vmem(small * blk, 8, 128),
            dma(CHUNKS + 1), pltpu.SemaphoreType.REGULAR((4,)),
            dma(), dma(2, CHUNKS),
            dma(), dma(),
            dma(2), dma(2, CHUNKS),
            dma(2), dma(2, CHUNKS),
            dma(), dma(),
            dma(lay), dma(lay), dma(lay), dma(lay),
            dma(), dma(),
            dma(), dma(CHUNKS), dma(), dma(CHUNKS), dma(4), dma(4),
        ],
        compiler_params=pltpu.CompilerParams(
            collective_id=0, has_side_effects=True, vmem_limit_bytes=40 * 1024 * 1024
        ),
        name="gmres",
    )(in_hbm(right_side), in_hbm(diagonal))
    in_vmem = lambda x: pltpu.with_memory_space_constraint(x, pltpu.VMEM)
    return pl.pallas_call(
        store,
        out_shape=(
            jax.ShapeDtypeStruct(x.shape, jnp.float32), jax.ShapeDtypeStruct(h.shape, jnp.float32),
        ),
        in_specs=[pl.BlockSpec(memory_space=pltpu.VMEM)] * 2,
        out_specs=(pl.BlockSpec(memory_space=pltpu.HBM),) * 2,
        scratch_shapes=[dma(2)],
        compiler_params=pltpu.CompilerParams(vmem_limit_bytes=4 * 1024 * 1024),
        name="store",
    )(in_vmem(x), in_vmem(h))


def solution(mesh):
    in_specs = (P(None, "gz", "gy", None), P("gz", "gy", None))
    out_specs = (P(None, "gz", "gy", None), P())
    return jax.shard_map(body, mesh=mesh, in_specs=in_specs, out_specs=out_specs, check_vma=False)
```

```python
import functools

import jax
import jax.numpy as jnp
from jax import lax
from jax.experimental import pallas as pl
from jax.experimental.pallas import tpu as pltpu
from jax.sharding import PartitionSpec as P

ITERS = 3
CENTRE = 7.5
SCALE = 0.25
CUTS = (0, 1, 3, 5, 7, 8)
CHUNKS = len(CUTS) - 1
EARLY = (1, 1)
WIDE = (4, 4)
BACK = {(0, 1): ("ghost",), (0, 2): ((0, 0),), (0, 3): ((0, 1),), (0, 4): ((0, 2),), (1, 1): ((0, 3),), (1, 4): ((0, 4), (1, 0)), (2, 0): ((1, 1),), (2, 1): ((1, 2),), "reduce": ((1, 3), (1, 4), (2, 0), (2, 1), (2, 2), (2, 3), (2, 4))}
RELAY = {"reduce": (0, 1, 2, 3, 4)}
MESH = pl.DeviceIdType.MESH
HIGH = lax.Precision.HIGHEST


def SC(name, f):
    with jax.named_scope(name):
        return f()


def nt_dot(left, right):
    return lax.dot_general(
        left, right, (((1,), (1,)), ((), ())), precision=HIGH, preferred_element_type=jnp.float32
    )


def dot(left, right):
    return jnp.dot(left, right, precision=HIGH, preferred_element_type=jnp.float32)


def kernel(
    r_hbm, d_hbm, out_ref, hess_ref,
    r_ref, d_ref, k0, k1, k2, k3, diag, ret, held, ys, yh, rows_out, rows_in,
    deep, d_deep, g_out, g_in, kd1, kd2,
    acc, mine, slots, splat, columns, i_s, met,
    x_s, x_r, d_s, d_r, z_s, z_r, y_s, y_r, e_s, e_r, b_s, b_r, l_s, l_r, g_s, g_r,
    q_s, q_r, qz_s, qz_r, w_s, w_r,
):
    blk, lay, rows, nx = r_ref.shape
    half, group_lay = rows // 2, 2 * lay
    starts = [blk * cut // CUTS[-1] for cut in CUTS]
    part = lambda ch: pl.ds(starts[ch], starts[ch + 1] - starts[ch])
    n_z, n_y = lax.axis_size("gz"), lax.axis_size("gy")
    gz, gy = lax.axis_index("gz"), lax.axis_index("gy")
    n_dev = n_z * n_y
    me = gz * n_y + gy
    p, group = gz % 2, gz // 2
    h = (p + gy) % 2
    partner = gz + 1 - 2 * p
    hs = pl.multiple_of(h * half, half)
    os = pl.multiple_of((1 - h) * half, half)
    mine_at = p * lay
    theirs_at = (1 - p) * lay
    below, above = group > 0, group < n_z // 2 - 1
    place = 2 * gy + h
    before, after = place > 0, place < 2 * n_y - 1
    prev_dev = (gz + h * (partner - gz), gy - (1 - h))
    next_dev = (gz + (1 - h) * (partner - gz), gy + h)
    basis = (k0, k1, k2, k3)
    edge = (lay - 1) * p
    inner = half // 2
    outer = half - inner
    early = [outer * EARLY[layer % len(EARLY)] // 16 * 8 for layer in range(lay)]
    late = [outer - e for e in early]
    width = [nx * WIDE[layer % len(WIDE)] // 4 for layer in range(lay)]
    theirs_out = pl.multiple_of(h * inner, 8)
    mine_out = pl.multiple_of((1 - h) * inner, 8)
    inner_at = pl.multiple_of(os + h * outer, 8)
    far, near_l = (lay - 1) * p, (lay - 1) * (1 - p)
    beyond = jnp.where(p == 0, below, above)
    onward = jnp.where(p == 0, above, below)
    onward_dev = (gz + 2 - 4 * p, gy)

    def remote(src, dst, send, recv, dev):
        return pltpu.make_async_remote_copy(
            src_ref=src, dst_ref=dst, send_sem=send, recv_sem=recv, device_id=dev,
            device_id_type=MESH,
        )

    def device(i):
        return (i // n_y, i % n_y)

    def load_r(ch):
        vs = part(ch)
        return pltpu.make_async_copy(r_hbm.at[vs], r_ref.at[vs], i_s.at[ch])

    load_d = pltpu.make_async_copy(d_hbm, d_ref, i_s.at[CHUNKS])
    for ch in range(CHUNKS):
        load_r(ch).start()
    load_d.start()

    def signal(semaphore, dev):
        pl.semaphore_signal(semaphore, inc=1, device_id=dev, device_id_type=MESH)

    barrier = pltpu.get_barrier_semaphore()
    left, right = gy > 0, gy < n_y - 1
    sides = (
        (below, (gz - 2, gy)), (above, (gz + 2, gy)), (left, (gz, gy - 1)), (right, (gz, gy + 1)),
    )
    signal(barrier, (partner, gy))
    for there, dev in sides:
        @pl.when(there)
        def _():
            signal(barrier, dev)

    def wave(which):
        there, back = sides[which], sides[which ^ 1]

        @pl.when(back[0])
        def _():
            pl.semaphore_wait(met.at[which], 1)

        @pl.when(there[0])
        def _():
            signal(met.at[which], there[1])

    @pl.when(jnp.logical_not(below))
    def _():
        for k in (k0, k1, k2):
            k[:, 0] = jnp.zeros((blk, half, nx), jnp.float32)

    @pl.when(jnp.logical_not(above))
    def _():
        for k in (k0, k1, k2):
            k[:, group_lay + 1] = jnp.zeros((blk, half, nx), jnp.float32)

    @pl.when(jnp.logical_not(before))
    def _():
        yh[:, 0] = jnp.zeros((ITERS,) + yh.shape[2:], jnp.float32)

    @pl.when(jnp.logical_not(after))
    def _():
        yh[:, 1] = jnp.zeros((ITERS,) + yh.shape[2:], jnp.float32)

    @pl.when(jnp.logical_not(beyond))
    def _():
        deep[0:2] = jnp.zeros((2,) + deep.shape[1:], jnp.float32)
        d_deep[0] = jnp.zeros(d_deep.shape[1:], jnp.float32)
        g_in[:, 0] = jnp.zeros((blk, 1, nx), jnp.float32)

    load_r(0).wait()
    SC("barrier", lambda: pl.semaphore_wait(
        barrier, 1 + sum(jnp.where(there, 1, 0) for there, _ in sides)
    ))
    rows_copy = remote(rows_out, rows_in, e_s, e_r, (partner, gy))

    def exchange(which, ch):
        layer = edge + which * (1 - 2 * p)
        vs = part(ch)
        return remote(
            r_ref.at[vs, pl.ds(layer, 1), pl.ds(os, half)],
            k0.at[vs, pl.ds(1 + mine_at + layer, 1)],
            x_s, x_r.at[which, ch], (partner, gy),
        )

    def z_from_rhs(ch, direction):
        vs = part(ch)
        if direction == 0:
            dst, dev = k0.at[vs, pl.ds(group_lay + 1, 1)], (gz - 2, gy)
        else:
            dst, dev = k0.at[vs, pl.ds(0, 1)], (gz + 2, gy)
        return remote(
            r_ref.at[vs, pl.ds(edge, 1), pl.ds(hs, half)], dst,
            z_s.at[direction], z_r.at[0, ch], dev,
        )

    def z_copy(j, ch, direction):
        vs = part(ch)
        k = basis[j]
        if direction == 0:
            src, dst, dev = k.at[vs, pl.ds(1, 1)], k.at[vs, pl.ds(group_lay + 1, 1)], (gz - 2, gy)
        else:
            src, dst, dev = k.at[vs, pl.ds(group_lay, 1)], k.at[vs, pl.ds(0, 1)], (gz + 2, gy)
        return remote(src, dst, z_s.at[direction], z_r.at[j % 2, ch], dev)

    def y_copy(j, ch, side):
        vs = part(ch)
        dev = prev_dev if side == 0 else next_dev
        return remote(
            ys.at[j, side, vs], yh.at[j, 1 - side, vs],
            y_s.at[side], y_r.at[j % 2, ch], dev,
        )

    def has(j, side):
        if side == 0:
            return before if j else before & (h == 0)
        return after if j else after & (h == 1)

    def back_copy(j, ch):
        vs = part(ch)
        return [
            remote(
                basis[j].at[vs, 1 + theirs_at + layer, pl.ds(theirs_out, early[layer]), pl.ds(0, width[layer])],
                ret.at[j - 1, layer, vs, pl.ds(0, early[layer]), pl.ds(0, width[layer])],
                b_s.at[layer], b_r.at[layer], (partner, gy),
            )
            for layer in range(lay)
        ]

    def all_back(layer):
        every = ret.at[:, layer, :, pl.ds(0, early[layer]), pl.ds(0, width[layer])]
        return remote(every, every, b_s.at[layer], b_r.at[layer], (partner, gy))

    def late_copy(layer, at, first, count, lane_at, sem):
        cols = pl.ds(lane_at, nx - lane_at)
        return remote(
            held.at[:, pl.ds(layer, 1), pl.ds(first, count), cols],
            out_ref.at[:, pl.ds(layer, 1), pl.ds(pl.multiple_of(at + first, 8), count), cols],
            l_s.at[sem], l_r.at[sem], (partner, gy),
        )

    late_parts = [
        (layer, 0, early[layer], width[layer], lay + layer)
        for layer in range(lay) if width[layer] < nx
    ] + [(layer, early[layer], late[layer], 0, layer) for layer in range(lay) if late[layer]]

    give_at = pl.multiple_of(hs + (1 - h) * outer, 8)

    def deep_copy(ch):
        vs = part(ch)
        return [
            remote(
                r_ref.at[vs, layer, pl.ds(give_at, inner)], deep.at[slot, vs],
                q_s, q_r.at[ch], (partner, gy),
            )
            for slot, layer in ((2, near_l), (3, far))
        ]

    def deep_recv(ch):
        every = deep.at[pl.ds(2, 2), part(ch)]
        return remote(every, every, q_s, q_r.at[ch], (partner, gy))

    def deep_relay(ch):
        vs = part(ch)
        return remote(
            deep.at[pl.ds(2, 2), vs], deep.at[pl.ds(0, 2), vs], qz_s, qz_r.at[ch], onward_dev
        )

    ghost_copies = [
        remote(g_out, g_in.at[:, pl.ds(1, 2)], w_s.at[0], w_r.at[0], (partner, gy))
    ] + [
        remote(
            d_ref.at[layer, pl.ds(give_at, inner)], d_deep.at[slot], w_s.at[1], w_r.at[1],
            (partner, gy),
        )
        for slot, layer in ((1, near_l), (2, far))
    ]
    both_diag = d_deep.at[pl.ds(1, 2)]
    ghost_diag = remote(both_diag, both_diag, w_s.at[1], w_r.at[1], (partner, gy))
    ghost_relays = (
        remote(g_in.at[:, pl.ds(2, 1)], g_in.at[:, pl.ds(0, 1)], w_s.at[2], w_r.at[2], onward_dev),
        remote(d_deep.at[pl.ds(2, 1)], d_deep.at[pl.ds(0, 1)], w_s.at[3], w_r.at[3], onward_dev),
    )

    def issue(items):
        for item in items:
            if item == "ghost":
                copies = ghost_copies
            else:
                copies = back_copy(*item) if item[0] else deep_copy(item[1])
            for copy in copies:
                copy.start()

    def relay_deep(ch):
        deep_recv(ch).wait_recv()
        if ch == 0:
            ghost_copies[0].wait_recv()
            ghost_diag.wait_recv()

        @pl.when(onward)
        def _():
            deep_relay(ch).start()
            if ch == 0:
                for copy in ghost_relays:
                    copy.start()

    diag_copy = remote(
        d_ref.at[:, pl.ds(os, half)], diag.at[pl.ds(mine_at, lay)], d_s, d_r, (partner, gy)
    )

    for ch in range(CHUNKS):
        if ch:
            load_r(ch).wait()
        exchange(0, ch).start()

        @pl.when((p == 0) & below)
        def _():
            z_from_rhs(ch, 0).start()

        @pl.when((p == 1) & above)
        def _():
            z_from_rhs(ch, 1).start()

    for v in range(blk):
        rows_out[v, :lay] = jnp.where(
            h == 0, r_ref[v, :, half - 1:half], r_ref[v, :, half:half + 1]
        )
        rows_out[v, lay] = jnp.where(
            h == 0, r_ref[v, near_l, rows - 1:rows], r_ref[v, near_l, 0:1]
        )
        for slot, layer in ((0, near_l), (1, far)):
            g_out[v, slot] = jnp.where(
                h == 0, r_ref[v, layer, outer - 1:outer], r_ref[v, layer, half + inner:half + inner + 1]
            )
    load_d.wait()
    rows_copy.start()
    diag_copy.start()
    for ch in range(CHUNKS):
        exchange(1, ch).start()

    def own(v, carry):
        k0[v, pl.ds(1 + mine_at, lay)] = r_ref[v, :, pl.ds(hs, half)]
        return carry

    lax.fori_loop(0, blk, own, 0)
    diag[pl.ds(mine_at, lay)] = d_ref[:, pl.ds(hs, half)]

    lanes = nx // 128

    def add_up(sums, tiles):
        def run(i, carry):
            layer, at = i // tiles, pl.multiple_of((i % tiles) * 8, 8)
            for lane in range(lanes):
                carry = sums(carry, layer, at, pl.ds(lane * 128, 128))
            return carry
        return run

    known = (2 * ITERS - 1) * blk * blk
    split = acc.shape[0] - 2 * blk * blk

    def keep_sum(moment, a, b, s):
        line = jnp.sum(s, axis=0, keepdims=True)
        first = moment * blk * blk + (split - known if moment >= 2 * ITERS - 1 else 0)
        at = first + a * blk + b
        acc[at:at + 1] = line
        if a != b:
            at = first + b * blk + a
            acc[at:at + 1] = line

    zero = jnp.zeros((8, 128), jnp.float32)

    def gram_rhs():
        pairs = [(a, b) for a in range(blk) for b in range(a, blk)]

        def body(sums, layer, at, cols):
            x = [r_ref[v, layer, pl.ds(at, 8), cols] for v in range(blk)]
            return tuple(s + x[a] * x[b] for s, (a, b) in zip(sums, pairs))

        sums = lax.fori_loop(
            0, lay * (rows // 8), add_up(body, rows // 8), (zero,) * len(pairs)
        )
        for s, (a, b) in zip(sums, pairs):
            keep_sum(0, a, b, s)

    def gram(j, ch):
        src, dst = basis[j], basis[j + 1]
        shift = 0 if j == ITERS - 1 else 1
        top = starts[ch + 1]
        pairs = [(a, b) for b in range(starts[ch], top) for a in range(b + 1)]

        def body(sums, layer, at, cols):
            x = [src[v, 1 + layer, pl.ds(at, 8), cols] for v in range(top)]
            y = [dst[v, shift + layer, pl.ds(at, 8), cols] for v in range(top)]
            first, second = sums[:len(pairs)], sums[len(pairs):]
            first = tuple(s + x[a] * y[b] for s, (a, b) in zip(first, pairs))
            second = tuple(s + y[a] * y[b] for s, (a, b) in zip(second, pairs))
            return first + second

        sums = lax.fori_loop(
            0, group_lay * (half // 8), add_up(body, half // 8), (zero,) * (2 * len(pairs))
        )
        for i, (a, b) in enumerate(pairs):
            keep_sum(2 * j + 1, a, b, sums[i])
            keep_sum(2 * j + 2, a, b, sums[len(pairs) + i])

    acc[known:split] = jnp.zeros((split - known, 128), jnp.float32)
    SC("gram0", gram_rhs)

    def relay(ch):
        remote(
            r_ref.at[part(ch), pl.ds(0, 1), pl.ds(os, half)],
            k0.at[part(ch), pl.ds(1 + (group_lay - 1) * (1 - p), 1)],
            x_s, x_r.at[0, ch], (partner, gy),
        ).wait_recv()

        @pl.when((p == 0) & above)
        def _():
            z_copy(0, ch, 1).start()

        @pl.when((p == 1) & below)
        def _():
            z_copy(0, ch, 0).start()

    def stage_rows(j, v, layer, value):
        ys[j, 0, v, layer:layer + 1] = value[:1]
        ys[j, 1, v, layer:layer + 1] = value[half - 1:]

    def start_rows(j, ch):
        for side in range(2):
            @pl.when(has(j, side))
            def _():
                y_copy(j, ch, side).start()

    def arrived(ch):
        remote(
            r_ref.at[part(ch), pl.ds(0, 1), pl.ds(os, half)],
            k0.at[part(ch), pl.ds(1 + lay - p, 1)],
            x_s, x_r.at[1, ch], (partner, gy),
        ).wait_recv()

    for ch in range(CHUNKS):
        if ch < len(sides):
            SC(f"wave#{ch}", lambda: wave(ch))
        SC(f"relay#{ch}", lambda: relay(ch))

    def rows_arrived():
        rows_copy.wait()
        for v in range(blk):
            near = jnp.where(
                h == 0, r_ref[v, :, half:half + 1], r_ref[v, :, half - 1:half]
            ).reshape(lay, nx)
            own_row = jnp.where(
                h == 0, r_ref[v, :, 0:1], r_ref[v, :, rows - 1:rows]
            ).reshape(lay, nx)
            both = lambda own, other: jnp.where(
                p == 0,
                jnp.concatenate([own, other], axis=0),
                jnp.concatenate([other, own], axis=0),
            )
            yh[0, 1 - h, v] = both(near, rows_in[v, :lay].reshape(lay, nx))
            last = 1 + (group_lay - 1) * (1 - p)
            edge_row = jnp.where(h == 0, k0[v, last, 0:1], k0[v, last, half - 1:half])
            next_row = rows_in[v, lay]
            ys[0, h, v] = both(own_row, jnp.where(
                p == 0,
                jnp.concatenate([next_row, edge_row], axis=0),
                jnp.concatenate([edge_row, next_row], axis=0),
            ))
        for ch in range(CHUNKS):
            start_rows(0, ch)
        remote(
            d_ref.at[:, pl.ds(os, half)], diag.at[pl.ds(theirs_at, lay)], d_s, d_r, (partner, gy)
        ).wait_recv()

    SC("rows_diag", rows_arrived)

    row_at = lax.broadcasted_iota(jnp.int32, (half, nx), 0)
    col_at = lax.broadcasted_iota(jnp.int32, (half, nx), 1)

    def apply(j, ch):
        src, dst = basis[j], basis[j + 1]
        shift = 0 if j == ITERS - 1 else 1
        vs = part(ch)

        def take(there, every, semaphore):
            for count in (1, 2):
                @pl.when(there[0].astype(jnp.int32) + there[1].astype(jnp.int32) == count)
                def _():
                    ref = every(count)
                    remote(ref, ref, z_s.at[0], semaphore, (partner, gy)).wait_recv()

        def waits():
            take((below, above), lambda n: src.at[vs, pl.ds(0, n)], z_r.at[j % 2, ch])

        def row_waits():
            take((has(j, 0), has(j, 1)), lambda n: yh.at[j, pl.ds(0, n), vs], y_r.at[j % 2, ch])

        for which in RELAY.get((j, ch), ()):
            SC(f"drelay#{which}", lambda: relay_deep(which))
        SC(f"z_wait{j}#{ch}", waits)
        SC(f"y_wait{j}#{ch}", row_waits)

        def run(v, carry):
            for layer in range(group_lay):
                here = src[v, 1 + layer]
                near = src[v, layer] + src[v, 2 + layer]
                up = jnp.where(
                    row_at == 0, yh[j, 0, v, layer:layer + 1], pltpu.roll(here, 1, 0)
                )
                down = jnp.where(
                    row_at == half - 1, yh[j, 1, v, layer:layer + 1],
                    pltpu.roll(here, half - 1, 0),
                )
                left = jnp.where(col_at == 0, 0.0, pltpu.roll(here, 1, 1))
                right = jnp.where(col_at == nx - 1, 0.0, pltpu.roll(here, nx - 1, 1))
                near = near + (up + down) + (left + right)
                centre = (6.0 - CENTRE) + diag[layer]
                value = SCALE * (centre * here - near)
                dst[v, shift + layer] = value
                if j < ITERS - 1:
                    stage_rows(j + 1, v, layer, value)
            return carry

        SC(f"apply{j}#{ch}", lambda: lax.fori_loop(starts[ch], starts[ch + 1], run, 0))
        if j < ITERS - 1:
            @pl.when(below)
            def _():
                z_copy(j + 1, ch, 0).start()

            @pl.when(above)
            def _():
                z_copy(j + 1, ch, 1).start()

            start_rows(j + 1, ch)
        issue(BACK.get((j, ch), ()))
        SC(f"gram{j}#{ch}", lambda: gram(j, ch))

    def gather(first, last, skip):
        count = last - first
        sums = nt_dot(jnp.ones((8, 128), jnp.float32), acc[first:last])
        lane_q = lax.broadcasted_iota(jnp.int32, (8, count), 1)
        row_q = lax.broadcasted_iota(jnp.int32, (8, count), 0)
        q = lax.broadcasted_iota(jnp.int32, (count, 128), 0) + (first - skip)
        c = lax.broadcasted_iota(jnp.int32, (count, 128), 1)
        pick = (q // (blk * blk) == c // blk) & (q % blk == c % blk)
        kept = jnp.where((lane_q // blk) % blk == row_q, sums, 0.0)
        return dot(kept, jnp.where(pick, 1.0, 0.0))

    row_d = lax.broadcasted_iota(jnp.int32, (inner, nx), 0)
    col_d = lax.broadcasted_iota(jnp.int32, (inner, nx), 1)

    def sideways(here, col):
        return jnp.where(col == 0, 0.0, pltpu.roll(here, 1, 1)) + jnp.where(
            col == nx - 1, 0.0, pltpu.roll(here, nx - 1, 1)
        )

    def deepen(ch):
        @pl.when(beyond)
        def _():
            every = deep.at[pl.ds(0, 2), part(ch)]
            remote(every, every, qz_s, qz_r.at[ch], (partner, gy)).wait_recv()
            if ch == 0:
                for slot, ref in ((2, g_in.at[:, pl.ds(0, 1)]), (3, d_deep.at[pl.ds(0, 1)])):
                    remote(ref, ref, w_s.at[slot], w_r.at[slot], (partner, gy)).wait_recv()

        edge_of = lambda ref, v, slot: jnp.where(
            h == 0, ref[v, slot, half - 1:half], ref[v, slot, 0:1]
        )
        ghost_of = lambda row: jnp.where(
            h == 0, row(half + inner), row(outer - 1)
        )
        after_of = lambda row: jnp.where(
            h == 0, row(half + inner + 1), row(outer - 2)
        )
        slots = {
            "beyond": (group_lay + 1) * p, "far": 1 + (group_lay - 1) * p,
            "near": lay + p, "next": lay + 1 - p,
        }
        d_far, d_near = d_ref[far, pl.ds(inner_at, inner)], d_ref[near_l, pl.ds(inner_at, inner)]
        g_far = ghost_of(lambda i: d_ref[far, i:i + 1])
        g_near = ghost_of(lambda i: d_ref[near_l, i:i + 1])
        exists = jnp.where(beyond, 1.0, 0.0)
        one_col = lax.broadcasted_iota(jnp.int32, (1, nx), 1)

        def block(here, below_z, above_z, edge_row, ghost_row, extra):
            up = jnp.where(
                row_d == 0, jnp.where(h == 0, edge_row, ghost_row), pltpu.roll(here, 1, 0)
            )
            down = jnp.where(
                row_d == inner - 1, jnp.where(h == 0, ghost_row, edge_row),
                pltpu.roll(here, inner - 1, 0),
            )
            near = (below_z + above_z) + (up + down) + sideways(here, col_d)
            return SCALE * (((6.0 - CENTRE) + extra) * here - near)

        def run(v, carry):
            r_far = r_ref[v, far, pl.ds(inner_at, inner)]
            r_near = r_ref[v, near_l, pl.ds(inner_at, inner)]
            two, one, nxt, last = deep[0, v], deep[1, v], deep[2, v], deep[3, v]
            ghost_far = ghost_of(lambda i: r_ref[v, far, i:i + 1])
            ghost_near = ghost_of(lambda i: r_ref[v, near_l, i:i + 1])
            ghost_one, ghost_next = g_in[v, 0], g_in[v, 1]
            rows_of = lambda which: edge_of(k0, v, slots[which])
            k_one = exists * block(one, two, r_far, rows_of("beyond"), ghost_one, d_deep[0])
            k_far = block(r_far, one, r_near, rows_of("far"), ghost_far, d_far)
            k_near = block(r_near, r_far, nxt, rows_of("near"), ghost_near, d_near)
            k_next = block(nxt, r_near, last, rows_of("next"), ghost_next, d_deep[1])

            def line(here, inside, layer, beside, extra):
                outside = after_of(lambda i: r_ref[v, layer, i:i + 1])
                within = jnp.where(h == 0, inside[inner - 1:inner], inside[0:1])
                near = beside + (outside + within) + sideways(here, one_col)
                return SCALE * (((6.0 - CENTRE) + extra) * here - near)

            line_far = line(ghost_far, r_far, far, ghost_one + ghost_near, g_far)
            line_near = line(ghost_near, r_near, near_l, ghost_far + ghost_next, g_near)
            kd1[0, v], kd1[1, v] = k_far, k_near
            kd2[0, v] = block(
                k_far, k_one, k_near, edge_of(k1, v, slots["far"]), line_far, d_far
            )
            kd2[1, v] = block(
                k_near, k_far, k_next, edge_of(k1, v, slots["near"]), line_near, d_near
            )
            return carry

        lax.fori_loop(starts[ch], starts[ch + 1], run, 0)

    for ch in range(CHUNKS):
        SC(f"arrived#{ch}", lambda: arrived(ch))
        apply(0, ch)
    for ch in range(CHUNKS):
        apply(1, ch)

    def early_sums():
        local = gather(0, split, 0)
        mine[...] = local[:4] + pltpu.roll(local, 64, 1)[4:]

    SC("early_sums", early_sums)
    for ch in range(CHUNKS):
        apply(2, ch)

    def reduce():
        lane_s = lax.broadcasted_iota(jnp.int32, (8, 128), 1)
        local = jnp.zeros((8, 128), jnp.float32)
        for i in range(2 * blk):
            column = jnp.sum(acc[split + i * blk:split + (i + 1) * blk], axis=1, keepdims=True)
            local = local + jnp.where(lane_s == known // blk + i, column, 0.0)
        packed = mine[...] + local[:4] + pltpu.roll(local, 64, 1)[4:]
        mine[...] = packed
        slots[me] = packed

        def send(i, carry):
            to = jnp.where(2 * gz < n_z, n_dev - 1 - i, i)

            @pl.when(to != me)
            def _():
                remote(mine, slots.at[me], g_s, g_r, device(to)).start()

            return carry

        lax.fori_loop(0, n_dev, send, 0)
        issue(BACK.get("reduce", ()))
        for which in RELAY.get("reduce", ()):
            relay_deep(which)

    SC("red_send", reduce)

    def collect():
        others = slots.at[pl.ds(0, n_dev - 1)]
        remote(others, others, g_s, g_r, (partner, gy)).wait()

    SC("red_wait", collect)
    packed = jnp.sum(slots[...], axis=0)

    lane = lax.broadcasted_iota(jnp.int32, (8, 128), 1)
    keep = lambda x, low, high: jnp.where((lane >= low) & (lane < high), x, 0.0)
    left_by = lambda x, n: x if n == 0 else pltpu.roll(x, 128 - n, 1)
    moments = keep(
        jnp.concatenate([packed, pltpu.roll(packed, 64, 1)], axis=0), 0, 64
    )
    small, order = ITERS * blk, (ITERS + 1) * blk
    inv = 1.0 / SCALE

    wide = lambda x: jnp.broadcast_to(x, (1, 128))

    def solve():
        second = (
            (inv * inv) * left_by(moments, 2 * blk)
            + (2.0 * CENTRE * inv) * left_by(moments, blk)
            + (CENTRE * CENTRE) * moments
        )
        target = inv * left_by(moments, blk) + CENTRE * moments
        normal = jnp.concatenate(
            [
                keep(left_by(second, blk * i), 0, small)
                + keep(pltpu.roll(target, small - blk * i, 1) if i < ITERS else target, small, order)
                for i in range(ITERS)
            ],
            axis=0,
        )
        rows_small = lax.broadcasted_iota(jnp.int32, (small, 1), 0)
        for k in range(0, small, 2):
            top, low = normal[k:k + 1], normal[k + 1:k + 2]
            top_k, top_l = wide(top[:, k:k + 1]), wide(top[:, k + 1:k + 2])
            low_k, low_l = wide(low[:, k:k + 1]), wide(low[:, k + 1:k + 2])
            inv_top = 1.0 / top_k
            ratio = low_k * inv_top
            inv_low = 1.0 / (low_l - ratio * top_l)
            second_row = (low - ratio * top) * inv_low
            first_row = (top - top_l * second_row) * inv_top
            pair = (rows_small == k) | (rows_small == k + 1)
            first_col = jnp.where(pair, 0.0, normal[:, k:k + 1])
            second_col = jnp.where(pair, 0.0, normal[:, k + 1:k + 2])
            rest = normal - first_col * first_row - second_col * second_row
            normal = jnp.where(
                rows_small == k, first_row, jnp.where(rows_small == k + 1, second_row, rest)
            )
        return normal

    normal = SC("solve", solve)

    def factor():
        lane32 = lax.broadcasted_iota(jnp.int32, (order, 128), 1)
        row32 = lax.broadcasted_iota(jnp.int32, (order, 128), 0)
        full = jnp.concatenate(
            [keep(left_by(moments, blk * i), 0, order) for i in range(ITERS + 1)], axis=0
        )
        full = full + jnp.where(lane32 == row32 + order, 1.0, 0.0)
        rows_full = lax.broadcasted_iota(jnp.int32, (order, 1), 0)
        for k in range(0, order, 2):
            top, low = full[k:k + 1], full[k + 1:k + 2]
            top_k, top_l = wide(top[:, k:k + 1]), wide(top[:, k + 1:k + 2])
            low_k, low_l = wide(low[:, k:k + 1]), wide(low[:, k + 1:k + 2])
            inv_top = 1.0 / top_k
            ratio = low_k * inv_top
            left_over = low - ratio * top
            second_row = left_over * (1.0 / (low_l - ratio * top_l))
            first_row = (top - top_l * second_row) * inv_top
            done = rows_full <= k + 1
            first_col = jnp.where(done, 0.0, full[:, k:k + 1])
            second_col = jnp.where(done, 0.0, full[:, k + 1:k + 2])
            rest = full - first_col * first_row - second_col * second_row
            full = jnp.where(rows_full == k + 1, left_over, rest)
        pivots = jnp.sum(jnp.where(lane32 == row32, full, 0.0), axis=1, keepdims=True)
        full = full / jnp.sqrt(pivots)
        upper = jnp.where((lane32 < order) & (lane32 >= row32), full, 0.0)
        lower_inv = left_by(full, order)
        lower_inv = jnp.where(lane32 < small, lower_inv, 0.0)[:small]
        hess = inv * nt_dot(pltpu.roll(lower_inv, blk, 1), upper)
        row_h = lax.broadcasted_iota(jnp.int32, (small, order), 0)
        col_h = lax.broadcasted_iota(jnp.int32, (small, order), 1)
        hess = hess + jnp.where(row_h == col_h, CENTRE, 0.0)
        hess_ref[...] = jnp.where(col_h // blk <= row_h // blk + 1, hess, 0.0)

    def spread():
        for u in range(blk):
            columns[u] = jnp.broadcast_to(normal[:, small + u:small + u + 1], (small, 128))
        for k in range(small):
            for u in range(blk):
                splat[k * blk + u] = jnp.broadcast_to(columns[u, k:k + 1], (8, 128))

    SC("splat", spread)

    def combine(dst, first_layer, count, row_start, height, sources, low=0, high=None):
        tiles = height // 8

        def run(i, carry):
            layer, t = first_layer + i // tiles, i % tiles
            at = pl.multiple_of(row_start + t * 8, 8)
            for lane_at in range(low, nx if high is None else high, 128):
                cols = pl.ds(lane_at, 128)
                vals = []
                for ref, l_at, base in sources:
                    first_row = pl.multiple_of(base + t * 8, 8)
                    vals += [
                        ref[v, pl.ds(first_row, 8), cols] if l_at is None
                        else ref[v, l_at + layer, pl.ds(first_row, 8), cols]
                        for v in range(blk)
                    ]
                for u in range(blk):
                    total = splat[u] * vals[0]
                    for k in range(1, small):
                        total = total + splat[k * blk + u] * vals[k]
                    dst[u, layer, pl.ds(at, 8), cols] = total
            return carry

        lax.fori_loop(0, count * tiles, run, 0)

    def send_late():
        for layer, start, count, lane_at, sem in late_parts:
            for first in range(start, start + count, 8):
                combine(
                    held, layer, 1, first, 8,
                    [(k, 1 + theirs_at, theirs_out + first) for k in basis[:ITERS]], lane_at,
                )
                late_copy(layer, hs + theirs_out, first, 8, lane_at, sem).start()

    SC("comb_late", send_late)
    for ch in range(2):
        SC(f"deepen#{ch}", lambda: deepen(ch))
    SC("comb_own", lambda: combine(
        out_ref, 0, lay, hs, half, ((r_ref, 0, hs), (k1, 1 + mine_at, 0), (k2, 1 + mine_at, 0))
    ))
    SC("deepen#2", lambda: deepen(2))
    SC("factor", factor)

    def back_wait():
        for layer in range(lay):
            all_back(layer).wait()

    SC("back_wait", back_wait)

    def rest():
        for layer in range(lay):
            combine(
                out_ref, layer, 1, os + mine_out, early[layer],
                (
                    (r_ref, 0, os + mine_out),
                    (ret.at[0, layer], None, 0), (ret.at[1, layer], None, 0),
                ),
                0, width[layer],
            )

    SC("comb_other", rest)
    SC("deepen#3", lambda: deepen(3))
    for ch in range(4, CHUNKS):
        SC(f"deepen#{ch}", lambda: deepen(ch))

    def finish_inner():
        for slot, layer in ((0, far), (1, near_l)):
            combine(
                out_ref, layer, 1, inner_at, inner,
                ((r_ref, 0, inner_at), (kd1.at[slot], None, 0), (kd2.at[slot], None, 0)),
            )

    SC("comb_inner", finish_inner)

    def drain():
        whole = r_ref.at[:, :, pl.ds(os, half)]
        remote(whole, whole, x_s, x_r.at[0, 0], (partner, gy)).wait_send()
        for direction, there in ((0, below), (1, above)):
            @pl.when(there)
            def _():
                every = k0.at[:, pl.ds(0, ITERS)]
                remote(
                    every, every, z_s.at[direction], z_r.at[0, 0], (partner, gy)
                ).wait_send()

        for side, there in ((0, before), (1, after)):
            first = has(0, side)

            @pl.when(first)
            def _():
                every = ys.at[:, side]
                remote(every, every, y_s.at[side], y_r.at[0, 0], (partner, gy)).wait_send()

            @pl.when(there & jnp.logical_not(first))
            def _():
                every = ys.at[pl.ds(1, ITERS - 1), side]
                remote(every, every, y_s.at[side], y_r.at[0, 0], (partner, gy)).wait_send()

        diag_copy.wait_send()
        every = deep.at[pl.ds(2, 2)]
        remote(every, every, q_s, q_r.at[0], (partner, gy)).wait_send()
        ghost_copies[0].wait_send()
        ghost_diag.wait_send()

        @pl.when(onward)
        def _():
            remote(every, every, qz_s, qz_r.at[0], (partner, gy)).wait_send()
            for copy in ghost_relays:
                copy.wait_send()

    SC("drain", drain)

    def late_wait():
        for layer, start, count, lane_at, sem in late_parts:
            late_copy(layer, hs + theirs_out, start, count, lane_at, sem).wait_send()
            late_copy(layer, os + mine_out, start, count, lane_at, sem).wait_recv()

    SC("late_wait", late_wait)


def store(x_ref, h_ref, x_out, h_out, sems):
    copies = (
        pltpu.make_async_copy(x_ref, x_out, sems.at[0]),
        pltpu.make_async_copy(h_ref, h_out, sems.at[1]),
    )
    for copy in copies:
        copy.start()
    for copy in copies:
        copy.wait()


def body(right_side, diagonal):
    blk, lay, rows, nx = right_side.shape
    half, group_lay = rows // 2, 2 * lay
    inner = half // 2
    outer = half - inner
    early = [outer * EARLY[layer % len(EARLY)] // 16 * 8 for layer in range(lay)]
    n_z, n_y = lax.axis_size("gz"), lax.axis_size("gy")
    vmem = lambda *shape: pltpu.VMEM(shape, jnp.float32)
    dma = lambda *shape: pltpu.SemaphoreType.DMA(shape) if shape else pltpu.SemaphoreType.DMA
    small, order = ITERS * blk, (ITERS + 1) * blk
    in_hbm = lambda x: pltpu.with_memory_space_constraint(x, pltpu.HBM)
    x, h = pl.pallas_call(
        kernel,
        out_shape=(vmem(*right_side.shape), vmem(small, order)),
        in_specs=[pl.BlockSpec(memory_space=pltpu.HBM)] * 2,
        out_specs=(pl.BlockSpec(memory_space=pltpu.VMEM),) * 2,
        scratch_shapes=[
            vmem(*right_side.shape),
            vmem(*diagonal.shape),
            vmem(blk, group_lay + 2, half, nx),
            vmem(blk, group_lay + 2, half, nx),
            vmem(blk, group_lay + 2, half, nx),
            vmem(blk, group_lay, half, nx),
            vmem(group_lay, half, nx),
            vmem(ITERS - 1, lay, blk, max(early), nx),
            vmem(blk, lay, outer, nx),
            vmem(ITERS, 2, blk, group_lay, nx),
            vmem(ITERS, 2, blk, group_lay, nx),
            vmem(blk, lay + 1, 1, nx),
            vmem(blk, lay + 1, 1, nx),
            vmem(4, blk, inner, nx),
            vmem(3, inner, nx),
            vmem(blk, 2, 1, nx),
            vmem(blk, 3, 1, nx),
            vmem(2, blk, inner, nx),
            vmem(2, blk, inner, nx),
            vmem(8 * blk * blk, 128),
            vmem(4, 128),
            vmem(n_z * n_y, 4, 128),
            vmem(small * blk, 8, 128),
            vmem(blk, small, 128),
            dma(CHUNKS + 1), pltpu.SemaphoreType.REGULAR((4,)),
            dma(), dma(2, CHUNKS),
            dma(), dma(),
            dma(2), dma(2, CHUNKS),
            dma(2), dma(2, CHUNKS),
            dma(), dma(),
            dma(lay), dma(lay), dma(2 * lay), dma(2 * lay),
            dma(), dma(),
            dma(), dma(CHUNKS), dma(), dma(CHUNKS), dma(4), dma(4),
        ],
        compiler_params=pltpu.CompilerParams(
            collective_id=0, has_side_effects=True, vmem_limit_bytes=40 * 1024 * 1024
        ),
        name="gmres",
    )(in_hbm(right_side), in_hbm(diagonal))
    in_vmem = lambda x: pltpu.with_memory_space_constraint(x, pltpu.VMEM)
    return pl.pallas_call(
        store,
        out_shape=(
            jax.ShapeDtypeStruct(x.shape, jnp.float32), jax.ShapeDtypeStruct(h.shape, jnp.float32),
        ),
        in_specs=[pl.BlockSpec(memory_space=pltpu.VMEM)] * 2,
        out_specs=(pl.BlockSpec(memory_space=pltpu.HBM),) * 2,
        scratch_shapes=[dma(2)],
        compiler_params=pltpu.CompilerParams(vmem_limit_bytes=4 * 1024 * 1024),
        name="store",
    )(in_vmem(x), in_vmem(h))


def solution(mesh):
    in_specs = (P(None, "gz", "gy", None), P("gz", "gy", None))
    out_specs = (P(None, "gz", "gy", None), P())
    return jax.shard_map(body, mesh=mesh, in_specs=in_specs, out_specs=out_specs, check_vma=False)
```

```python
import functools

import jax
import jax.numpy as jnp
from jax import lax
from jax.experimental import pallas as pl
from jax.experimental.pallas import tpu as pltpu
from jax.sharding import PartitionSpec as P

ITERS = 3
CENTRE = 7.5
SCALE = 0.25
CUTS = (0, 1, 3, 5, 7, 8)
CHUNKS = len(CUTS) - 1
EARLY = (1, 1)
WIDE = (4, 4)
BACK = {(0, 2): ((0, 0),), (0, 3): ((0, 1),), (0, 4): ((0, 2),), (1, 2): ((0, 3),), (1, 4): ("ghost", (0, 4), (1, 0)), (2, 0): ((1, 1),), (2, 1): ((1, 2),), "reduce": ((1, 3), (1, 4), (2, 0), (2, 1), (2, 2), (2, 3), (2, 4))}
RELAY = {"reduce": (0, 1, 2, 3, 4)}
MESH = pl.DeviceIdType.MESH
HIGH = lax.Precision.HIGHEST


def SC(name, f):
    with jax.named_scope(name):
        return f()


def nt_dot(left, right):
    return lax.dot_general(
        left, right, (((1,), (1,)), ((), ())), precision=HIGH, preferred_element_type=jnp.float32
    )


def dot(left, right):
    return jnp.dot(left, right, precision=HIGH, preferred_element_type=jnp.float32)


def kernel(
    r_hbm, d_hbm, out_ref, hess_ref,
    r_ref, d_ref, k0, k1, k2, k3, diag, ret, held, ys, yh, rows_out, rows_in,
    deep, d_deep, g_out, g_in, kd1, kd2,
    acc, mine, slots, splat, columns, i_s, met,
    x_s, x_r, d_s, d_r, z_s, z_r, y_s, y_r, e_s, e_r, b_s, b_r, l_s, l_r, g_s, g_r,
    q_s, q_r, qz_s, qz_r, w_s, w_r,
):
    blk, lay, rows, nx = r_ref.shape
    half, group_lay = rows // 2, 2 * lay
    starts = [blk * cut // CUTS[-1] for cut in CUTS]
    part = lambda ch: pl.ds(starts[ch], starts[ch + 1] - starts[ch])
    n_z, n_y = lax.axis_size("gz"), lax.axis_size("gy")
    gz, gy = lax.axis_index("gz"), lax.axis_index("gy")
    n_dev = n_z * n_y
    me = gz * n_y + gy
    p, group = gz % 2, gz // 2
    h = (p + gy) % 2
    partner = gz + 1 - 2 * p
    hs = pl.multiple_of(h * half, half)
    os = pl.multiple_of((1 - h) * half, half)
    mine_at = p * lay
    theirs_at = (1 - p) * lay
    below, above = group > 0, group < n_z // 2 - 1
    place = 2 * gy + h
    before, after = place > 0, place < 2 * n_y - 1
    prev_dev = (gz + h * (partner - gz), gy - (1 - h))
    next_dev = (gz + (1 - h) * (partner - gz), gy + h)
    basis = (k0, k1, k2, k3)
    edge = (lay - 1) * p
    inner = half // 2
    outer = half - inner
    early = [outer * EARLY[layer % len(EARLY)] // 16 * 8 for layer in range(lay)]
    late = [outer - e for e in early]
    width = [nx * WIDE[layer % len(WIDE)] // 4 for layer in range(lay)]
    theirs_out = pl.multiple_of(h * inner, 8)
    mine_out = pl.multiple_of((1 - h) * inner, 8)
    inner_at = pl.multiple_of(os + h * outer, 8)
    far, near_l = (lay - 1) * p, (lay - 1) * (1 - p)
    beyond = jnp.where(p == 0, below, above)
    onward = jnp.where(p == 0, above, below)
    onward_dev = (gz + 2 - 4 * p, gy)

    def remote(src, dst, send, recv, dev):
        return pltpu.make_async_remote_copy(
            src_ref=src, dst_ref=dst, send_sem=send, recv_sem=recv, device_id=dev,
            device_id_type=MESH,
        )

    def device(i):
        return (i // n_y, i % n_y)

    def load_r(ch):
        vs = part(ch)
        return pltpu.make_async_copy(r_hbm.at[vs], r_ref.at[vs], i_s.at[ch])

    load_d = pltpu.make_async_copy(d_hbm, d_ref, i_s.at[CHUNKS])
    for ch in range(CHUNKS):
        load_r(ch).start()
    load_d.start()

    def signal(semaphore, dev):
        pl.semaphore_signal(semaphore, inc=1, device_id=dev, device_id_type=MESH)

    barrier = pltpu.get_barrier_semaphore()
    left, right = gy > 0, gy < n_y - 1
    sides = (
        (below, (gz - 2, gy)), (above, (gz + 2, gy)), (left, (gz, gy - 1)), (right, (gz, gy + 1)),
    )
    signal(barrier, (partner, gy))
    for there, dev in sides:
        @pl.when(there)
        def _():
            signal(barrier, dev)

    def wave(which):
        there, back = sides[which], sides[which ^ 1]

        @pl.when(back[0])
        def _():
            pl.semaphore_wait(met.at[which], 1)

        @pl.when(there[0])
        def _():
            signal(met.at[which], there[1])

    @pl.when(jnp.logical_not(below))
    def _():
        for k in (k0, k1, k2):
            k[:, 0] = jnp.zeros((blk, half, nx), jnp.float32)

    @pl.when(jnp.logical_not(above))
    def _():
        for k in (k0, k1, k2):
            k[:, group_lay + 1] = jnp.zeros((blk, half, nx), jnp.float32)

    @pl.when(jnp.logical_not(before))
    def _():
        yh[:, 0] = jnp.zeros((ITERS,) + yh.shape[2:], jnp.float32)

    @pl.when(jnp.logical_not(after))
    def _():
        yh[:, 1] = jnp.zeros((ITERS,) + yh.shape[2:], jnp.float32)

    @pl.when(jnp.logical_not(beyond))
    def _():
        deep[0:2] = jnp.zeros((2,) + deep.shape[1:], jnp.float32)
        d_deep[0] = jnp.zeros(d_deep.shape[1:], jnp.float32)
        g_in[:, 0] = jnp.zeros((blk, 1, nx), jnp.float32)

    load_r(0).wait()
    SC("barrier", lambda: pl.semaphore_wait(
        barrier, 1 + sum(jnp.where(there, 1, 0) for there, _ in sides)
    ))
    rows_copy = remote(rows_out, rows_in, e_s, e_r, (partner, gy))

    def exchange(which, ch):
        layer = edge + which * (1 - 2 * p)
        vs = part(ch)
        return remote(
            r_ref.at[vs, pl.ds(layer, 1), pl.ds(os, half)],
            k0.at[vs, pl.ds(1 + mine_at + layer, 1)],
            x_s, x_r.at[which, ch], (partner, gy),
        )

    def z_from_rhs(ch, direction):
        vs = part(ch)
        if direction == 0:
            dst, dev = k0.at[vs, pl.ds(group_lay + 1, 1)], (gz - 2, gy)
        else:
            dst, dev = k0.at[vs, pl.ds(0, 1)], (gz + 2, gy)
        return remote(
            r_ref.at[vs, pl.ds(edge, 1), pl.ds(hs, half)], dst,
            z_s.at[direction], z_r.at[0, ch], dev,
        )

    def z_copy(j, ch, direction):
        vs = part(ch)
        k = basis[j]
        if direction == 0:
            src, dst, dev = k.at[vs, pl.ds(1, 1)], k.at[vs, pl.ds(group_lay + 1, 1)], (gz - 2, gy)
        else:
            src, dst, dev = k.at[vs, pl.ds(group_lay, 1)], k.at[vs, pl.ds(0, 1)], (gz + 2, gy)
        return remote(src, dst, z_s.at[direction], z_r.at[j % 2, ch], dev)

    def y_copy(j, ch, side):
        vs = part(ch)
        dev = prev_dev if side == 0 else next_dev
        return remote(
            ys.at[j, side, vs], yh.at[j, 1 - side, vs],
            y_s.at[side], y_r.at[j % 2, ch], dev,
        )

    def has(j, side):
        if side == 0:
            return before if j else before & (h == 0)
        return after if j else after & (h == 1)

    def back_copy(j, ch):
        vs = part(ch)
        return [
            remote(
                basis[j].at[vs, 1 + theirs_at + layer, pl.ds(theirs_out, early[layer]), pl.ds(0, width[layer])],
                ret.at[j - 1, layer, vs, pl.ds(0, early[layer]), pl.ds(0, width[layer])],
                b_s.at[layer], b_r.at[layer], (partner, gy),
            )
            for layer in range(lay)
        ]

    def all_back(layer):
        every = ret.at[:, layer, :, pl.ds(0, early[layer]), pl.ds(0, width[layer])]
        return remote(every, every, b_s.at[layer], b_r.at[layer], (partner, gy))

    def late_copy(layer, at, first, count, lane_at, sem):
        cols = pl.ds(lane_at, nx - lane_at)
        return remote(
            held.at[:, pl.ds(layer, 1), pl.ds(first, count), cols],
            out_ref.at[:, pl.ds(layer, 1), pl.ds(pl.multiple_of(at + first, 8), count), cols],
            l_s.at[sem], l_r.at[sem], (partner, gy),
        )

    late_parts = [
        (layer, 0, early[layer], width[layer], lay + layer)
        for layer in range(lay) if width[layer] < nx
    ] + [(layer, early[layer], late[layer], 0, layer) for layer in range(lay) if late[layer]]

    give_at = pl.multiple_of(hs + (1 - h) * outer, 8)

    def deep_copy(ch):
        vs = part(ch)
        return [
            remote(
                r_ref.at[vs, layer, pl.ds(give_at, inner)], deep.at[slot, vs],
                q_s, q_r, (partner, gy),
            )
            for slot, layer in ((2, near_l), (3, far))
        ]

    every_deep = deep.at[pl.ds(2, 2)]
    all_deep = remote(every_deep, every_deep, q_s, q_r, (partner, gy))

    def deep_relay(ch):
        vs = part(ch)
        return remote(
            deep.at[pl.ds(2, 2), vs], deep.at[pl.ds(0, 2), vs], qz_s, qz_r.at[ch], onward_dev
        )

    ghost_copies = [
        remote(g_out, g_in.at[:, pl.ds(1, 2)], w_s.at[0], w_r.at[0], (partner, gy))
    ] + [
        remote(
            d_ref.at[layer, pl.ds(give_at, inner)], d_deep.at[slot], w_s.at[1], w_r.at[1],
            (partner, gy),
        )
        for slot, layer in ((1, near_l), (2, far))
    ]
    both_diag = d_deep.at[pl.ds(1, 2)]
    ghost_diag = remote(both_diag, both_diag, w_s.at[1], w_r.at[1], (partner, gy))
    ghost_relays = (
        remote(g_in.at[:, pl.ds(2, 1)], g_in.at[:, pl.ds(0, 1)], w_s.at[2], w_r.at[2], onward_dev),
        remote(d_deep.at[pl.ds(2, 1)], d_deep.at[pl.ds(0, 1)], w_s.at[3], w_r.at[3], onward_dev),
    )

    def issue(items):
        for item in items:
            if item == "ghost":
                copies = ghost_copies
            else:
                copies = back_copy(*item) if item[0] else deep_copy(item[1])
            for copy in copies:
                copy.start()

    def relay_deep(ch):
        if ch == 0:
            all_deep.wait_recv()
            ghost_copies[0].wait_recv()
            ghost_diag.wait_recv()

        @pl.when(onward)
        def _():
            deep_relay(ch).start()
            if ch == 0:
                for copy in ghost_relays:
                    copy.start()

    diag_copy = remote(
        d_ref.at[:, pl.ds(os, half)], diag.at[pl.ds(mine_at, lay)], d_s, d_r, (partner, gy)
    )

    for ch in range(CHUNKS):
        if ch:
            load_r(ch).wait()
        exchange(0, ch).start()

        @pl.when((p == 0) & below)
        def _():
            z_from_rhs(ch, 0).start()

        @pl.when((p == 1) & above)
        def _():
            z_from_rhs(ch, 1).start()

    for v in range(blk):
        rows_out[v, :lay] = jnp.where(
            h == 0, r_ref[v, :, half - 1:half], r_ref[v, :, half:half + 1]
        )
        rows_out[v, lay] = jnp.where(
            h == 0, r_ref[v, near_l, rows - 1:rows], r_ref[v, near_l, 0:1]
        )
        for slot, layer in ((0, near_l), (1, far)):
            g_out[v, slot] = jnp.where(
                h == 0, r_ref[v, layer, outer - 1:outer], r_ref[v, layer, half + inner:half + inner + 1]
            )
    load_d.wait()
    rows_copy.start()
    diag_copy.start()
    for ch in range(CHUNKS):
        exchange(1, ch).start()

    def own(v, carry):
        k0[v, pl.ds(1 + mine_at, lay)] = r_ref[v, :, pl.ds(hs, half)]
        return carry

    lax.fori_loop(0, blk, own, 0)
    diag[pl.ds(mine_at, lay)] = d_ref[:, pl.ds(hs, half)]

    lanes = nx // 128

    def add_up(sums, tiles):
        def run(i, carry):
            layer, at = i // tiles, pl.multiple_of((i % tiles) * 8, 8)
            for lane in range(lanes):
                carry = sums(carry, layer, at, pl.ds(lane * 128, 128))
            return carry
        return run

    known = (2 * ITERS - 1) * blk * blk
    split = acc.shape[0] - 2 * blk * blk

    def keep_sum(moment, a, b, s):
        line = jnp.sum(s, axis=0, keepdims=True)
        first = moment * blk * blk + (split - known if moment >= 2 * ITERS - 1 else 0)
        at = first + a * blk + b
        acc[at:at + 1] = line
        if a != b:
            at = first + b * blk + a
            acc[at:at + 1] = line

    zero = jnp.zeros((8, 128), jnp.float32)

    def gram_rhs():
        pairs = [(a, b) for a in range(blk) for b in range(a, blk)]

        def body(sums, layer, at, cols):
            x = [r_ref[v, layer, pl.ds(at, 8), cols] for v in range(blk)]
            return tuple(s + x[a] * x[b] for s, (a, b) in zip(sums, pairs))

        sums = lax.fori_loop(
            0, lay * (rows // 8), add_up(body, rows // 8), (zero,) * len(pairs)
        )
        for s, (a, b) in zip(sums, pairs):
            keep_sum(0, a, b, s)

    def gram(j, ch):
        src, dst = basis[j], basis[j + 1]
        shift = 0 if j == ITERS - 1 else 1
        top = starts[ch + 1]
        pairs = [(a, b) for b in range(starts[ch], top) for a in range(b + 1)]

        def body(sums, layer, at, cols):
            x = [src[v, 1 + layer, pl.ds(at, 8), cols] for v in range(top)]
            y = [dst[v, shift + layer, pl.ds(at, 8), cols] for v in range(top)]
            first, second = sums[:len(pairs)], sums[len(pairs):]
            first = tuple(s + x[a] * y[b] for s, (a, b) in zip(first, pairs))
            second = tuple(s + y[a] * y[b] for s, (a, b) in zip(second, pairs))
            return first + second

        sums = lax.fori_loop(
            0, group_lay * (half // 8), add_up(body, half // 8), (zero,) * (2 * len(pairs))
        )
        for i, (a, b) in enumerate(pairs):
            keep_sum(2 * j + 1, a, b, sums[i])
            keep_sum(2 * j + 2, a, b, sums[len(pairs) + i])

    acc[known:split] = jnp.zeros((split - known, 128), jnp.float32)
    SC("gram0", gram_rhs)

    def relay(ch):
        remote(
            r_ref.at[part(ch), pl.ds(0, 1), pl.ds(os, half)],
            k0.at[part(ch), pl.ds(1 + (group_lay - 1) * (1 - p), 1)],
            x_s, x_r.at[0, ch], (partner, gy),
        ).wait_recv()

        @pl.when((p == 0) & above)
        def _():
            z_copy(0, ch, 1).start()

        @pl.when((p == 1) & below)
        def _():
            z_copy(0, ch, 0).start()

    def stage_rows(j, v, layer, value):
        ys[j, 0, v, layer:layer + 1] = value[:1]
        ys[j, 1, v, layer:layer + 1] = value[half - 1:]

    def start_rows(j, ch):
        for side in range(2):
            @pl.when(has(j, side))
            def _():
                y_copy(j, ch, side).start()

    def arrived(ch):
        remote(
            r_ref.at[part(ch), pl.ds(0, 1), pl.ds(os, half)],
            k0.at[part(ch), pl.ds(1 + lay - p, 1)],
            x_s, x_r.at[1, ch], (partner, gy),
        ).wait_recv()

    for ch in range(CHUNKS):
        if ch < len(sides):
            SC(f"wave#{ch}", lambda: wave(ch))
        SC(f"relay#{ch}", lambda: relay(ch))

    def rows_arrived():
        rows_copy.wait()
        for v in range(blk):
            near = jnp.where(
                h == 0, r_ref[v, :, half:half + 1], r_ref[v, :, half - 1:half]
            ).reshape(lay, nx)
            own_row = jnp.where(
                h == 0, r_ref[v, :, 0:1], r_ref[v, :, rows - 1:rows]
            ).reshape(lay, nx)
            both = lambda own, other: jnp.where(
                p == 0,
                jnp.concatenate([own, other], axis=0),
                jnp.concatenate([other, own], axis=0),
            )
            yh[0, 1 - h, v] = both(near, rows_in[v, :lay].reshape(lay, nx))
            last = 1 + (group_lay - 1) * (1 - p)
            edge_row = jnp.where(h == 0, k0[v, last, 0:1], k0[v, last, half - 1:half])
            next_row = rows_in[v, lay]
            ys[0, h, v] = both(own_row, jnp.where(
                p == 0,
                jnp.concatenate([next_row, edge_row], axis=0),
                jnp.concatenate([edge_row, next_row], axis=0),
            ))
        for ch in range(CHUNKS):
            start_rows(0, ch)
        remote(
            d_ref.at[:, pl.ds(os, half)], diag.at[pl.ds(theirs_at, lay)], d_s, d_r, (partner, gy)
        ).wait_recv()

    SC("rows_diag", rows_arrived)

    row_at = lax.broadcasted_iota(jnp.int32, (half, nx), 0)
    col_at = lax.broadcasted_iota(jnp.int32, (half, nx), 1)

    def apply(j, ch):
        src, dst = basis[j], basis[j + 1]
        shift = 0 if j == ITERS - 1 else 1
        vs = part(ch)

        def take(there, every, semaphore):
            for count in (1, 2):
                @pl.when(there[0].astype(jnp.int32) + there[1].astype(jnp.int32) == count)
                def _():
                    ref = every(count)
                    remote(ref, ref, z_s.at[0], semaphore, (partner, gy)).wait_recv()

        def waits():
            take((below, above), lambda n: src.at[vs, pl.ds(0, n)], z_r.at[j % 2, ch])

        def row_waits():
            take((has(j, 0), has(j, 1)), lambda n: yh.at[j, pl.ds(0, n), vs], y_r.at[j % 2, ch])

        for which in RELAY.get((j, ch), ()):
            SC(f"drelay#{which}", lambda: relay_deep(which))
        SC(f"z_wait{j}#{ch}", waits)
        SC(f"y_wait{j}#{ch}", row_waits)

        def run(v, carry):
            for layer in range(group_lay):
                here = src[v, 1 + layer]
                near = src[v, layer] + src[v, 2 + layer]
                up = jnp.where(
                    row_at == 0, yh[j, 0, v, layer:layer + 1], pltpu.roll(here, 1, 0)
                )
                down = jnp.where(
                    row_at == half - 1, yh[j, 1, v, layer:layer + 1],
                    pltpu.roll(here, half - 1, 0),
                )
                left = jnp.where(col_at == 0, 0.0, pltpu.roll(here, 1, 1))
                right = jnp.where(col_at == nx - 1, 0.0, pltpu.roll(here, nx - 1, 1))
                near = near + (up + down) + (left + right)
                centre = (6.0 - CENTRE) + diag[layer]
                value = SCALE * (centre * here - near)
                dst[v, shift + layer] = value
                if j < ITERS - 1:
                    stage_rows(j + 1, v, layer, value)
            return carry

        SC(f"apply{j}#{ch}", lambda: lax.fori_loop(starts[ch], starts[ch + 1], run, 0))
        if j < ITERS - 1:
            @pl.when(below)
            def _():
                z_copy(j + 1, ch, 0).start()

            @pl.when(above)
            def _():
                z_copy(j + 1, ch, 1).start()

            start_rows(j + 1, ch)
        issue(BACK.get((j, ch), ()))
        SC(f"gram{j}#{ch}", lambda: gram(j, ch))

    def gather(first, last, skip):
        count = last - first
        sums = nt_dot(jnp.ones((8, 128), jnp.float32), acc[first:last])
        lane_q = lax.broadcasted_iota(jnp.int32, (8, count), 1)
        row_q = lax.broadcasted_iota(jnp.int32, (8, count), 0)
        q = lax.broadcasted_iota(jnp.int32, (count, 128), 0) + (first - skip)
        c = lax.broadcasted_iota(jnp.int32, (count, 128), 1)
        pick = (q // (blk * blk) == c // blk) & (q % blk == c % blk)
        kept = jnp.where((lane_q // blk) % blk == row_q, sums, 0.0)
        return dot(kept, jnp.where(pick, 1.0, 0.0))

    row_d = lax.broadcasted_iota(jnp.int32, (inner, nx), 0)
    col_d = lax.broadcasted_iota(jnp.int32, (inner, nx), 1)

    def sideways(here, col):
        return jnp.where(col == 0, 0.0, pltpu.roll(here, 1, 1)) + jnp.where(
            col == nx - 1, 0.0, pltpu.roll(here, nx - 1, 1)
        )

    def deepen(ch):
        @pl.when(beyond)
        def _():
            every = deep.at[pl.ds(0, 2), part(ch)]
            remote(every, every, qz_s, qz_r.at[ch], (partner, gy)).wait_recv()
            if ch == 0:
                for slot, ref in ((2, g_in.at[:, pl.ds(0, 1)]), (3, d_deep.at[pl.ds(0, 1)])):
                    remote(ref, ref, w_s.at[slot], w_r.at[slot], (partner, gy)).wait_recv()

        edge_of = lambda ref, v, slot: jnp.where(
            h == 0, ref[v, slot, half - 1:half], ref[v, slot, 0:1]
        )
        ghost_of = lambda row: jnp.where(
            h == 0, row(half + inner), row(outer - 1)
        )
        after_of = lambda row: jnp.where(
            h == 0, row(half + inner + 1), row(outer - 2)
        )
        slots = {
            "beyond": (group_lay + 1) * p, "far": 1 + (group_lay - 1) * p,
            "near": lay + p, "next": lay + 1 - p,
        }
        d_far, d_near = d_ref[far, pl.ds(inner_at, inner)], d_ref[near_l, pl.ds(inner_at, inner)]
        g_far = ghost_of(lambda i: d_ref[far, i:i + 1])
        g_near = ghost_of(lambda i: d_ref[near_l, i:i + 1])
        exists = jnp.where(beyond, 1.0, 0.0)
        one_col = lax.broadcasted_iota(jnp.int32, (1, nx), 1)

        def block(here, below_z, above_z, edge_row, ghost_row, extra):
            up = jnp.where(
                row_d == 0, jnp.where(h == 0, edge_row, ghost_row), pltpu.roll(here, 1, 0)
            )
            down = jnp.where(
                row_d == inner - 1, jnp.where(h == 0, ghost_row, edge_row),
                pltpu.roll(here, inner - 1, 0),
            )
            near = (below_z + above_z) + (up + down) + sideways(here, col_d)
            return SCALE * (((6.0 - CENTRE) + extra) * here - near)

        def run(v, carry):
            r_far = r_ref[v, far, pl.ds(inner_at, inner)]
            r_near = r_ref[v, near_l, pl.ds(inner_at, inner)]
            two, one, nxt, last = deep[0, v], deep[1, v], deep[2, v], deep[3, v]
            ghost_far = ghost_of(lambda i: r_ref[v, far, i:i + 1])
            ghost_near = ghost_of(lambda i: r_ref[v, near_l, i:i + 1])
            ghost_one, ghost_next = g_in[v, 0], g_in[v, 1]
            rows_of = lambda which: edge_of(k0, v, slots[which])
            k_one = exists * block(one, two, r_far, rows_of("beyond"), ghost_one, d_deep[0])
            k_far = block(r_far, one, r_near, rows_of("far"), ghost_far, d_far)
            k_near = block(r_near, r_far, nxt, rows_of("near"), ghost_near, d_near)
            k_next = block(nxt, r_near, last, rows_of("next"), ghost_next, d_deep[1])

            def line(here, inside, layer, beside, extra):
                outside = after_of(lambda i: r_ref[v, layer, i:i + 1])
                within = jnp.where(h == 0, inside[inner - 1:inner], inside[0:1])
                near = beside + (outside + within) + sideways(here, one_col)
                return SCALE * (((6.0 - CENTRE) + extra) * here - near)

            line_far = line(ghost_far, r_far, far, ghost_one + ghost_near, g_far)
            line_near = line(ghost_near, r_near, near_l, ghost_far + ghost_next, g_near)
            kd1[0, v], kd1[1, v] = k_far, k_near
            kd2[0, v] = block(
                k_far, k_one, k_near, edge_of(k1, v, slots["far"]), line_far, d_far
            )
            kd2[1, v] = block(
                k_near, k_far, k_next, edge_of(k1, v, slots["near"]), line_near, d_near
            )
            return carry

        lax.fori_loop(starts[ch], starts[ch + 1], run, 0)

    for ch in range(CHUNKS):
        SC(f"arrived#{ch}", lambda: arrived(ch))
        apply(0, ch)
    for ch in range(CHUNKS):
        apply(1, ch)

    def early_sums():
        local = gather(0, split, 0)
        mine[...] = local[:4] + pltpu.roll(local, 64, 1)[4:]

    SC("early_sums", early_sums)
    for ch in range(CHUNKS):
        apply(2, ch)

    def reduce():
        lane_s = lax.broadcasted_iota(jnp.int32, (8, 128), 1)
        local = jnp.zeros((8, 128), jnp.float32)
        for i in range(2 * blk):
            column = jnp.sum(acc[split + i * blk:split + (i + 1) * blk], axis=1, keepdims=True)
            local = local + jnp.where(lane_s == known // blk + i, column, 0.0)
        packed = mine[...] + local[:4] + pltpu.roll(local, 64, 1)[4:]
        mine[...] = packed
        slots[me] = packed

        def send(i, carry):
            to = jnp.where(2 * gz < n_z, n_dev - 1 - i, i)

            @pl.when(to != me)
            def _():
                remote(mine, slots.at[me], g_s, g_r, device(to)).start()

            return carry

        lax.fori_loop(0, n_dev, send, 0)
        issue(BACK.get("reduce", ()))
        for which in RELAY.get("reduce", ()):
            relay_deep(which)

    SC("red_send", reduce)

    def collect():
        others = slots.at[pl.ds(0, n_dev - 1)]
        remote(others, others, g_s, g_r, (partner, gy)).wait()

    SC("red_wait", collect)
    packed = jnp.sum(slots[...], axis=0)

    lane = lax.broadcasted_iota(jnp.int32, (8, 128), 1)
    keep = lambda x, low, high: jnp.where((lane >= low) & (lane < high), x, 0.0)
    left_by = lambda x, n: x if n == 0 else pltpu.roll(x, 128 - n, 1)
    moments = keep(
        jnp.concatenate([packed, pltpu.roll(packed, 64, 1)], axis=0), 0, 64
    )
    small, order = ITERS * blk, (ITERS + 1) * blk
    inv = 1.0 / SCALE

    wide = lambda x: jnp.broadcast_to(x, (1, 128))

    def solve():
        second = (
            (inv * inv) * left_by(moments, 2 * blk)
            + (2.0 * CENTRE * inv) * left_by(moments, blk)
            + (CENTRE * CENTRE) * moments
        )
        target = inv * left_by(moments, blk) + CENTRE * moments
        normal = jnp.concatenate(
            [
                keep(left_by(second, blk * i), 0, small)
                + keep(pltpu.roll(target, small - blk * i, 1) if i < ITERS else target, small, order)
                for i in range(ITERS)
            ],
            axis=0,
        )
        rows_small = lax.broadcasted_iota(jnp.int32, (small, 1), 0)
        for k in range(0, small, 2):
            top, low = normal[k:k + 1], normal[k + 1:k + 2]
            top_k, top_l = wide(top[:, k:k + 1]), wide(top[:, k + 1:k + 2])
            low_k, low_l = wide(low[:, k:k + 1]), wide(low[:, k + 1:k + 2])
            inv_top = 1.0 / top_k
            ratio = low_k * inv_top
            inv_low = 1.0 / (low_l - ratio * top_l)
            second_row = (low - ratio * top) * inv_low
            first_row = (top - top_l * second_row) * inv_top
            pair = (rows_small == k) | (rows_small == k + 1)
            first_col = jnp.where(pair, 0.0, normal[:, k:k + 1])
            second_col = jnp.where(pair, 0.0, normal[:, k + 1:k + 2])
            rest = normal - first_col * first_row - second_col * second_row
            normal = jnp.where(
                rows_small == k, first_row, jnp.where(rows_small == k + 1, second_row, rest)
            )
        return normal

    normal = SC("solve", solve)

    def factor():
        lane32 = lax.broadcasted_iota(jnp.int32, (order, 128), 1)
        row32 = lax.broadcasted_iota(jnp.int32, (order, 128), 0)
        full = jnp.concatenate(
            [keep(left_by(moments, blk * i), 0, order) for i in range(ITERS + 1)], axis=0
        )
        full = full + jnp.where(lane32 == row32 + order, 1.0, 0.0)
        rows_full = lax.broadcasted_iota(jnp.int32, (order, 1), 0)
        for k in range(0, order, 2):
            top, low = full[k:k + 1], full[k + 1:k + 2]
            top_k, top_l = wide(top[:, k:k + 1]), wide(top[:, k + 1:k + 2])
            low_k, low_l = wide(low[:, k:k + 1]), wide(low[:, k + 1:k + 2])
            inv_top = 1.0 / top_k
            ratio = low_k * inv_top
            left_over = low - ratio * top
            second_row = left_over * (1.0 / (low_l - ratio * top_l))
            first_row = (top - top_l * second_row) * inv_top
            done = rows_full <= k + 1
            first_col = jnp.where(done, 0.0, full[:, k:k + 1])
            second_col = jnp.where(done, 0.0, full[:, k + 1:k + 2])
            rest = full - first_col * first_row - second_col * second_row
            full = jnp.where(rows_full == k + 1, left_over, rest)
        pivots = jnp.sum(jnp.where(lane32 == row32, full, 0.0), axis=1, keepdims=True)
        full = full / jnp.sqrt(pivots)
        upper = jnp.where((lane32 < order) & (lane32 >= row32), full, 0.0)
        lower_inv = left_by(full, order)
        lower_inv = jnp.where(lane32 < small, lower_inv, 0.0)[:small]
        hess = inv * nt_dot(pltpu.roll(lower_inv, blk, 1), upper)
        row_h = lax.broadcasted_iota(jnp.int32, (small, order), 0)
        col_h = lax.broadcasted_iota(jnp.int32, (small, order), 1)
        hess = hess + jnp.where(row_h == col_h, CENTRE, 0.0)
        hess_ref[...] = jnp.where(col_h // blk <= row_h // blk + 1, hess, 0.0)

    def spread():
        for u in range(blk):
            columns[u] = jnp.broadcast_to(normal[:, small + u:small + u + 1], (small, 128))
        for k in range(small):
            for u in range(blk):
                splat[k * blk + u] = jnp.broadcast_to(columns[u, k:k + 1], (8, 128))

    SC("splat", spread)

    def combine(dst, first_layer, count, row_start, height, sources, low=0, high=None):
        tiles = height // 8

        def run(i, carry):
            layer, t = first_layer + i // tiles, i % tiles
            at = pl.multiple_of(row_start + t * 8, 8)
            for lane_at in range(low, nx if high is None else high, 128):
                cols = pl.ds(lane_at, 128)
                vals = []
                for ref, l_at, base in sources:
                    first_row = pl.multiple_of(base + t * 8, 8)
                    vals += [
                        ref[v, pl.ds(first_row, 8), cols] if l_at is None
                        else ref[v, l_at + layer, pl.ds(first_row, 8), cols]
                        for v in range(blk)
                    ]
                for u in range(blk):
                    total = splat[u] * vals[0]
                    for k in range(1, small):
                        total = total + splat[k * blk + u] * vals[k]
                    dst[u, layer, pl.ds(at, 8), cols] = total
            return carry

        lax.fori_loop(0, count * tiles, run, 0)

    def send_late():
        for layer, start, count, lane_at, sem in late_parts:
            for first in range(start, start + count, 8):
                combine(
                    held, layer, 1, first, 8,
                    [(k, 1 + theirs_at, theirs_out + first) for k in basis[:ITERS]], lane_at,
                )
                late_copy(layer, hs + theirs_out, first, 8, lane_at, sem).start()

    SC("comb_late", send_late)
    for ch in range(2):
        SC(f"deepen#{ch}", lambda: deepen(ch))
    SC("comb_own", lambda: combine(
        out_ref, 0, lay, hs, half, ((r_ref, 0, hs), (k1, 1 + mine_at, 0), (k2, 1 + mine_at, 0))
    ))
    SC("deepen#2", lambda: deepen(2))
    SC("factor", factor)

    def back_wait():
        for layer in range(lay):
            all_back(layer).wait()

    SC("back_wait", back_wait)

    def rest():
        for layer in range(lay):
            combine(
                out_ref, layer, 1, os + mine_out, early[layer],
                (
                    (r_ref, 0, os + mine_out),
                    (ret.at[0, layer], None, 0), (ret.at[1, layer], None, 0),
                ),
                0, width[layer],
            )

    SC("comb_other", rest)
    SC("deepen#3", lambda: deepen(3))
    for ch in range(4, CHUNKS):
        SC(f"deepen#{ch}", lambda: deepen(ch))

    def finish_inner():
        for slot, layer in ((0, far), (1, near_l)):
            combine(
                out_ref, layer, 1, inner_at, inner,
                ((r_ref, 0, inner_at), (kd1.at[slot], None, 0), (kd2.at[slot], None, 0)),
            )

    SC("comb_inner", finish_inner)

    def drain():
        whole = r_ref.at[:, :, pl.ds(os, half)]
        remote(whole, whole, x_s, x_r.at[0, 0], (partner, gy)).wait_send()
        for direction, there in ((0, below), (1, above)):
            @pl.when(there)
            def _():
                every = k0.at[:, pl.ds(0, ITERS)]
                remote(
                    every, every, z_s.at[direction], z_r.at[0, 0], (partner, gy)
                ).wait_send()

        for side, there in ((0, before), (1, after)):
            first = has(0, side)

            @pl.when(first)
            def _():
                every = ys.at[:, side]
                remote(every, every, y_s.at[side], y_r.at[0, 0], (partner, gy)).wait_send()

            @pl.when(there & jnp.logical_not(first))
            def _():
                every = ys.at[pl.ds(1, ITERS - 1), side]
                remote(every, every, y_s.at[side], y_r.at[0, 0], (partner, gy)).wait_send()

        diag_copy.wait_send()
        every = deep.at[pl.ds(2, 2)]
        all_deep.wait_send()
        ghost_copies[0].wait_send()
        ghost_diag.wait_send()

        @pl.when(onward)
        def _():
            remote(every, every, qz_s, qz_r.at[0], (partner, gy)).wait_send()
            for copy in ghost_relays:
                copy.wait_send()

    SC("drain", drain)

    def late_wait():
        for layer, start, count, lane_at, sem in late_parts:
            late_copy(layer, hs + theirs_out, start, count, lane_at, sem).wait_send()
            late_copy(layer, os + mine_out, start, count, lane_at, sem).wait_recv()

    SC("late_wait", late_wait)


def store(x_ref, h_ref, x_out, h_out, sems):
    copies = (
        pltpu.make_async_copy(x_ref, x_out, sems.at[0]),
        pltpu.make_async_copy(h_ref, h_out, sems.at[1]),
    )
    for copy in copies:
        copy.start()
    for copy in copies:
        copy.wait()


def body(right_side, diagonal):
    blk, lay, rows, nx = right_side.shape
    half, group_lay = rows // 2, 2 * lay
    inner = half // 2
    outer = half - inner
    early = [outer * EARLY[layer % len(EARLY)] // 16 * 8 for layer in range(lay)]
    n_z, n_y = lax.axis_size("gz"), lax.axis_size("gy")
    parts = 2 * lay if min(WIDE) < 4 else lay
    vmem = lambda *shape: pltpu.VMEM(shape, jnp.float32)
    dma = lambda *shape: pltpu.SemaphoreType.DMA(shape) if shape else pltpu.SemaphoreType.DMA
    small, order = ITERS * blk, (ITERS + 1) * blk
    in_hbm = lambda x: pltpu.with_memory_space_constraint(x, pltpu.HBM)
    x, h = pl.pallas_call(
        kernel,
        out_shape=(vmem(*right_side.shape), vmem(small, order)),
        in_specs=[pl.BlockSpec(memory_space=pltpu.HBM)] * 2,
        out_specs=(pl.BlockSpec(memory_space=pltpu.VMEM),) * 2,
        scratch_shapes=[
            vmem(*right_side.shape),
            vmem(*diagonal.shape),
            vmem(blk, group_lay + 2, half, nx),
            vmem(blk, group_lay + 2, half, nx),
            vmem(blk, group_lay + 2, half, nx),
            vmem(blk, group_lay, half, nx),
            vmem(group_lay, half, nx),
            vmem(ITERS - 1, lay, blk, max(early), nx),
            vmem(blk, lay, outer, nx),
            vmem(ITERS, 2, blk, group_lay, nx),
            vmem(ITERS, 2, blk, group_lay, nx),
            vmem(blk, lay + 1, 1, nx),
            vmem(blk, lay + 1, 1, nx),
            vmem(4, blk, inner, nx),
            vmem(3, inner, nx),
            vmem(blk, 2, 1, nx),
            vmem(blk, 3, 1, nx),
            vmem(2, blk, inner, nx),
            vmem(2, blk, inner, nx),
            vmem(8 * blk * blk, 128),
            vmem(4, 128),
            vmem(n_z * n_y, 4, 128),
            vmem(small * blk, 8, 128),
            vmem(blk, small, 128),
            dma(CHUNKS + 1), pltpu.SemaphoreType.REGULAR((4,)),
            dma(), dma(2, CHUNKS),
            dma(), dma(),
            dma(2), dma(2, CHUNKS),
            dma(2), dma(2, CHUNKS),
            dma(), dma(),
            dma(lay), dma(lay), dma(parts), dma(parts),
            dma(), dma(),
            dma(), dma(), dma(), dma(CHUNKS), dma(4), dma(4),
        ],
        compiler_params=pltpu.CompilerParams(
            collective_id=0, has_side_effects=True, vmem_limit_bytes=40 * 1024 * 1024
        ),
        name="gmres",
    )(in_hbm(right_side), in_hbm(diagonal))
    in_vmem = lambda x: pltpu.with_memory_space_constraint(x, pltpu.VMEM)
    return pl.pallas_call(
        store,
        out_shape=(
            jax.ShapeDtypeStruct(x.shape, jnp.float32), jax.ShapeDtypeStruct(h.shape, jnp.float32),
        ),
        in_specs=[pl.BlockSpec(memory_space=pltpu.VMEM)] * 2,
        out_specs=(pl.BlockSpec(memory_space=pltpu.HBM),) * 2,
        scratch_shapes=[dma(2)],
        compiler_params=pltpu.CompilerParams(vmem_limit_bytes=4 * 1024 * 1024),
        name="store",
    )(in_vmem(x), in_vmem(h))


def solution(mesh):
    in_specs = (P(None, "gz", "gy", None), P("gz", "gy", None))
    out_specs = (P(None, "gz", "gy", None), P())
    return jax.shard_map(body, mesh=mesh, in_specs=in_specs, out_specs=out_specs, check_vma=False)
```
